8 devices in a mesh: dp: 1 (over z), tp: 8 (over y, x, core).
Axes of the slice: x: 2, y: 2, z: 1, core: 2. Of those that a mesh axis runs over, the one named last changes fastest.
Arguments:
- x_rows: bfloat16 [8192, 2304], P(('dp', 'tp'))
- norm_gain: float32 [2304], replicated
- w_q: bfloat16 [2304, 8, 256], P(None, 'tp')
- w_k: bfloat16 [2304, 1024], P(None, 'tp')
- w_v: bfloat16 [2304, 1024], P(None, 'tp')
Outputs:
- output 1: bfloat16 [8192, 8, 256], P('dp', 'tp')
- output 2: bfloat16 [8192, 8, 256], P('dp', 'tp')
- output 3: bfloat16 [8192, 8, 256], P('dp', 'tp')
All inputs are finite; a program needn't handle non-finite values.
Results may differ from the reference program's by a relative error of at most 0.001.
Values are sent between devices in bfloat16 or wider.
A program may use at most 1 GiB of HBM per device.

```python
import jax
import jax.numpy as jnp
from jax import lax

TOKENS = 8192
D_MODEL = 2304
Q_HEADS = 8
KV_COUNT = 4
HEAD_DIM = 256
GROUP_SIZE = 8
EPSILON = 1e-6


def setup_inputs(seed: int = 0, part: int = 0) -> dict:
    key = jax.random.key(seed)
    shared_key, rows_key = jax.random.split(key)
    part_key = jax.random.fold_in(rows_key, part)
    x_rows = jax.random.normal(part_key, (TOKENS, D_MODEL), jnp.float32).astype(jnp.bfloat16)
    gain_key, q_key, k_key, v_key = jax.random.split(shared_key, 4)
    norm_gain = jax.random.uniform(gain_key, (D_MODEL,), jnp.float32, 0.4, 1.6)
    weight_scale = D_MODEL ** -0.5
    w_q = (jax.random.normal(q_key, (D_MODEL, Q_HEADS, HEAD_DIM), jnp.float32) * weight_scale).astype(jnp.bfloat16)
    w_k = (jax.random.normal(k_key, (D_MODEL, KV_COUNT * HEAD_DIM), jnp.float32) * weight_scale).astype(jnp.bfloat16)
    w_v = (jax.random.normal(v_key, (D_MODEL, KV_COUNT * HEAD_DIM), jnp.float32) * weight_scale).astype(jnp.bfloat16)
    return {"x_rows": x_rows, "norm_gain": norm_gain, "w_q": w_q, "w_k": w_k, "w_v": w_v}


def reference(x_rows, norm_gain, w_q, w_k, w_v):
    x_wide = x_rows.astype(jnp.float32)
    mean_sq = jnp.mean(x_wide * x_wide, axis=-1, keepdims=True)
    normed = (x_wide * lax.rsqrt(mean_sq + EPSILON) * norm_gain).astype(jnp.bfloat16)
    q_flat = jnp.dot(normed, w_q.reshape(D_MODEL, Q_HEADS * HEAD_DIM), preferred_element_type=jnp.float32)
    q_out = q_flat.astype(jnp.bfloat16).reshape(TOKENS, Q_HEADS, HEAD_DIM)
    head_share = GROUP_SIZE // KV_COUNT
    k_flat = jnp.dot(normed, w_k, preferred_element_type=jnp.float32).astype(jnp.bfloat16)
    v_flat = jnp.dot(normed, w_v, preferred_element_type=jnp.float32).astype(jnp.bfloat16)
    k_out = jnp.repeat(k_flat.reshape(TOKENS, KV_COUNT, HEAD_DIM), head_share, axis=1)
    v_out = jnp.repeat(v_flat.reshape(TOKENS, KV_COUNT, HEAD_DIM), head_share, axis=1)
    return (q_out, k_out, v_out)
```

```python
import jax
import jax.numpy as jnp
from jax import lax
from jax.experimental import pallas as pl
from jax.experimental.pallas import tpu as pltpu
from jax.sharding import PartitionSpec as P

EPSILON = 1e-6
CHUNK = 256
PIECE = 16


def kernel(x_hbm, gain, wq_hbm, wk_hbm, wv_hbm, q_out, k_out, v_out,
           x_own, x_side, w_own, w_far, far_out, mate_q,
           load_x, load_w, mw_send, mw_recv, fw_send, fw_recv, rw_send, rw_recv,
           x_send, x_recv, m_send, m_recv, f_send, fq_recv, fkv_recv, r_send, r_recv):
    rows, width = x_hbm.shape
    head = wq_hbm.shape[1]
    part = wk_hbm.shape[1]
    chunks = rows // CHUNK

    me = lax.axis_index("tp")
    core = lax.rem(me, 2)
    mate = me + 1 - 2 * core
    side = me + 2 - 4 * lax.rem(me // 2, 2)
    far = me + 4 - 8 * (me // 4)
    far_mate = far + 1 - 2 * core
    far_chip = far - core

    barrier = pltpu.get_barrier_semaphore()
    for peer in (mate, side, far, far_mate):
        pl.semaphore_signal(barrier, inc=1, device_id={"tp": peer})

    def send(src, dst, send_sem, recv_sem, to):
        return pltpu.make_async_remote_copy(src_ref=src, dst_ref=dst, send_sem=send_sem, recv_sem=recv_sem, device_id={"tp": to})

    q_cols = pl.ds(pl.multiple_of(core * head, head), head)
    k_cols = pl.ds(pl.multiple_of(2 * head + core * part, part), part)
    v_cols = pl.ds(pl.multiple_of(3 * head + core * part, part), part)
    mine = ((wk_hbm, k_cols), (wv_hbm, v_cols), (wq_hbm, q_cols))

    local_w = [pltpu.make_async_copy(src, w_own.at[:, cols], load_w.at[i]) for i, (src, cols) in enumerate(mine)]
    mate_w = [send(src, w_own.at[:, cols], mw_send.at[i], mw_recv.at[i], mate) for i, (src, cols) in enumerate(mine)]
    far_w = [send(src, w_far.at[:, cols], fw_send.at[i], fw_recv.at[i], far) for i, (src, cols) in enumerate(mine)]
    relay_w = [send(w_far.at[:, cols], w_far.at[:, cols], rw_send.at[i], rw_recv.at[i], mate) for i, (src, cols) in enumerate(mine)]

    def chunk_rows(i):
        return pl.ds(pl.multiple_of(i * CHUNK, CHUNK), CHUNK)

    def load_chunk(i):
        return pltpu.make_async_copy(x_hbm.at[chunk_rows(i), :], x_own.at[chunk_rows(i), :], load_x.at[i])

    def side_chunk(i):
        return send(x_hbm.at[chunk_rows(i), :], x_side.at[chunk_rows(i), :], x_send.at[i], x_recv.at[i], side)

    for i in range(chunks):
        load_chunk(i).start()
    for copy in local_w:
        copy.start()

    pl.semaphore_wait(barrier, 4)
    for i in range(3):
        far_w[i].start()
    side_chunk(0).start()
    for i in range(3):
        mate_w[i].start()
    for i in range(1, chunks):
        side_chunk(i).start()

    def normalise(ref, i):
        def piece(p, carry):
            at = pl.ds(pl.multiple_of(i * CHUNK + p * PIECE, PIECE), PIECE)
            x_wide = ref[at, :].astype(jnp.float32)
            mean_sq = jnp.mean(x_wide * x_wide, axis=-1, keepdims=True)
            ref[at, :] = (x_wide * lax.rsqrt(mean_sq + EPSILON) * gain[...]).astype(jnp.bfloat16)
            return carry

        lax.fori_loop(0, CHUNK // PIECE, piece, 0, unroll=2)

    def product(ref, i, w, start):
        return jnp.dot(ref[chunk_rows(i), :], w[:, start], preferred_element_type=jnp.float32).astype(jnp.bfloat16)

    def columns(block):
        if isinstance(block, int):
            return slice(block * head, (block + 1) * head)
        return pl.ds(pl.multiple_of(block * head, head), head)

    def out_rows(device, i):
        return pl.ds(pl.multiple_of(device * rows + i * CHUNK, CHUNK), CHUNK)

    def source(device, n):
        across = device + 2 - 4 * lax.rem(device // 2, 2)
        return jnp.where(n < chunks, device, across), lax.rem(n, chunks)

    def slot_rows(device, n):
        return out_rows(*source(device, n))

    def stage_rows(n):
        return pl.ds(pl.multiple_of(n * CHUNK, CHUNK), CHUNK)

    def mate_copies(n):
        at = slot_rows(me, n)
        return [
            send(k_out.at[at, :], k_out.at[at, :], m_send.at[0, n], m_recv.at[0, n], mate),
            send(v_out.at[at, :], v_out.at[at, :], m_send.at[1, n], m_recv.at[1, n], mate),
            send(mate_q.at[stage_rows(n), :], q_out.at[at, :], m_send.at[2, n], m_recv.at[2, n], mate),
        ]

    def far_kv(n):
        at = slot_rows(me, n)
        return [
            send(far_out.at[2, stage_rows(n), :], k_out.at[at, :], f_send.at[2, n], fkv_recv.at[0, n], far),
            send(far_out.at[3, stage_rows(n), :], v_out.at[at, :], f_send.at[3, n], fkv_recv.at[1, n], far),
        ]

    def far_q(n):
        at = slot_rows(me, n)
        return [
            send(far_out.at[j, stage_rows(n), :], q_out.at[at, :], f_send.at[j, n], fq_recv.at[core, n], far_chip + j)
            for j in range(2)
        ]

    def relay_copies(n):
        at = slot_rows(far, n)
        return [
            send(ref.at[at, :], ref.at[at, :], r_send.at[j, n], r_recv.at[j, n], mate)
            for j, ref in enumerate((k_out, v_out))
        ]

    def near_products(ref, i, n):
        at = slot_rows(me, n)
        k_out[at, :] = product(ref, i, w_own, columns(2))
        v_out[at, :] = product(ref, i, w_own, columns(3))
        q_out[at, :] = product(ref, i, w_own, columns(core))
        mate_q[stage_rows(n), :] = product(ref, i, w_own, columns(1 - core))
        for copy in mate_copies(n):
            copy.start()

    def far_kv_products(ref, i, n):
        for block in (2, 3):
            far_out[block, stage_rows(n), :] = product(ref, i, w_far, columns(block))
        for copy in far_kv(n):
            copy.start()

    def far_q_products(ref, i, n):
        for block in (0, 1):
            far_out[block, stage_rows(n), :] = product(ref, i, w_far, columns(block))
        for copy in far_q(n):
            copy.start()

    def loop(count, body):
        def step(i, carry):
            body(i)
            return carry

        lax.fori_loop(0, count, step, 0)

    def own_norm(i):
        load_chunk(i).wait()
        normalise(x_own, i)

    loop(chunks, own_norm)
    for i in range(3):
        local_w[i].wait()
        mate_w[i].wait_recv()
    loop(chunks, lambda i: near_products(x_own, i, i))

    for i in (0, 1):
        far_w[i].wait_recv()
        relay_w[i].start()
    for i in (0, 1):
        relay_w[i].wait_recv()
    loop(chunks, lambda i: far_kv_products(x_own, i, i))
    far_w[2].wait_recv()
    relay_w[2].start()
    relay_w[2].wait_recv()
    loop(chunks, lambda i: far_q_products(x_own, i, i))

    def side_step(i):
        side_chunk(i).wait_recv()
        normalise(x_side, i)
        far_kv_products(x_side, i, chunks + i)
        far_q_products(x_side, i, chunks + i)
        near_products(x_side, i, chunks + i)

    loop(chunks, side_step)

    def relay_step(n):
        for arrived, onward in zip(far_kv(n), relay_copies(n)):
            arrived.wait_recv()
            onward.start()

    loop(2 * chunks, relay_step)

    def drain(n):
        for copy in mate_copies(n):
            copy.wait_send()
            copy.wait_recv()
        for copy in far_kv(n):
            copy.wait_send()
        for j, copy in enumerate(far_q(n)):
            copy.wait_send()
            pltpu.make_async_remote_copy(
                src_ref=far_out.at[j, stage_rows(n), :], dst_ref=q_out.at[slot_rows(me, n), :], send_sem=f_send.at[j, n],
                recv_sem=fq_recv.at[j, n], device_id={"tp": far},
            ).wait_recv()
        for copy in relay_copies(n):
            copy.wait_send()
            copy.wait_recv()

    loop(2 * chunks, drain)
    for copies in (mate_w, far_w, relay_w):
        for copy in copies:
            copy.wait_send()
    loop(chunks, lambda i: side_chunk(i).wait_send())


def solution(mesh):
    group_size = mesh.shape["tp"]

    def local_step(x_rows, norm_gain, w_q, w_k, w_v):
        rows, width = x_rows.shape
        head = w_q.shape[2]
        slots = 2 * (rows // CHUNK)
        chunks = rows // CHUNK
        dma = pltpu.SemaphoreType.DMA
        any_space = pl.BlockSpec(memory_space=pl.ANY)
        vmem = pl.BlockSpec(memory_space=pltpu.VMEM)
        outs = pl.pallas_call(
            kernel,
            out_shape=[pltpu.VMEM((group_size * rows, head), jnp.bfloat16)] * 3,
            in_specs=[any_space, vmem, any_space, any_space, any_space],
            out_specs=[vmem] * 3,
            scratch_shapes=[
                pltpu.VMEM((rows, width), jnp.bfloat16),
                pltpu.VMEM((rows, width), jnp.bfloat16),
                pltpu.VMEM((width, 4 * head), jnp.bfloat16),
                pltpu.VMEM((width, 4 * head), jnp.bfloat16),
                pltpu.VMEM((4, 2 * rows, head), jnp.bfloat16),
                pltpu.VMEM((2 * rows, head), jnp.bfloat16),
                dma((chunks,)), dma((3,)), dma((3,)), dma((3,)), dma((3,)), dma((3,)), dma((3,)), dma((3,)),
                dma((chunks,)), dma((chunks,)), dma((3, slots)), dma((3, slots)), dma((4, slots)), dma((2, slots)),
                dma((2, slots)), dma((2, slots)), dma((2, slots)),
            ],
            compiler_params=pltpu.CompilerParams(collective_id=0, has_side_effects=True, vmem_limit_bytes=44 * 1024 * 1024),
        )(x_rows, norm_gain.reshape(1, width), w_q.reshape(width, head), w_k, w_v)
        return tuple(out[:, None, :] for out in outs)

    return jax.shard_map(local_step, mesh=mesh, in_specs=(P(("dp", "tp"), None), P(None), P(None, "tp", None), P(None, "tp"), P(None, "tp")), out_specs=(P("dp", "tp", None), P("dp", "tp", None), P("dp", "tp", None)), check_vma=False)
```

```python
import jax
import jax.numpy as jnp
from jax import lax
from jax.experimental import pallas as pl
from jax.experimental.pallas import tpu as pltpu
from jax.sharding import PartitionSpec as P

EPSILON = 1e-6
CHUNK = 256
PIECE = 16
STORES = 4


def kernel(x_hbm, gain_hbm, wq_hbm, wk_hbm, wv_hbm, q_out, k_out, v_out,
           x_own, x_side, w_own, w_far, far_out, mate_q, gain,
           load_gain, load_x, load_w, mw_send, mw_recv, fw_send, fw_recv, rw_send, rw_recv,
           x_send, x_recv, m_send, m_recv, f_send, fq_recv, fkv_recv, r_send, r_recv):
    rows, width = x_hbm.shape
    head = wq_hbm.shape[1]
    part = wk_hbm.shape[1]
    chunks = rows // CHUNK

    me = lax.axis_index("tp")
    core = lax.rem(me, 2)
    mate = me + 1 - 2 * core
    side = me + 2 - 4 * lax.rem(me // 2, 2)
    far = me + 4 - 8 * (me // 4)
    far_mate = far + 1 - 2 * core
    far_chip = far - core

    barrier = pltpu.get_barrier_semaphore()
    for peer in (mate, side, far, far_mate):
        pl.semaphore_signal(barrier, inc=1, device_id={"tp": peer})

    def send(src, dst, send_sem, recv_sem, to):
        return pltpu.make_async_remote_copy(src_ref=src, dst_ref=dst, send_sem=send_sem, recv_sem=recv_sem, device_id={"tp": to})

    q_cols = pl.ds(pl.multiple_of(core * head, head), head)
    k_cols = pl.ds(pl.multiple_of(2 * head + core * part, part), part)
    v_cols = pl.ds(pl.multiple_of(3 * head + core * part, part), part)
    mine = ((wk_hbm, k_cols), (wv_hbm, v_cols), (wq_hbm, q_cols))

    local_w = [pltpu.make_async_copy(src, w_own.at[:, cols], load_w.at[i]) for i, (src, cols) in enumerate(mine)]
    mate_w = [send(src, w_own.at[:, cols], mw_send.at[i], mw_recv.at[i], mate) for i, (src, cols) in enumerate(mine)]
    far_w = [send(src, w_far.at[:, cols], fw_send.at[i], fw_recv.at[i], far) for i, (src, cols) in enumerate(mine)]
    relay_w = [send(w_far.at[:, cols], w_far.at[:, cols], rw_send.at[i], rw_recv.at[i], mate) for i, (src, cols) in enumerate(mine)]

    def chunk_rows(i):
        return pl.ds(pl.multiple_of(i * CHUNK, CHUNK), CHUNK)

    def load_chunk(i):
        return pltpu.make_async_copy(x_hbm.at[chunk_rows(i), :], x_own.at[chunk_rows(i), :], load_x.at[i])

    def side_chunk(i):
        return send(x_hbm.at[chunk_rows(i), :], x_side.at[chunk_rows(i), :], x_send.at[i], x_recv.at[i], side)

    gain_copy = pltpu.make_async_copy(gain_hbm, gain, load_gain)
    gain_copy.start()
    for i in range(chunks):
        load_chunk(i).start()
    for copy in local_w:
        copy.start()

    pl.semaphore_wait(barrier, 4)
    for i in range(3):
        far_w[i].start()
    side_chunk(0).start()
    for i in range(3):
        mate_w[i].start()
    for i in range(1, chunks):
        side_chunk(i).start()

    def normalise(ref, i):
        def piece(p, carry):
            at = pl.ds(pl.multiple_of(i * CHUNK + p * PIECE, PIECE), PIECE)
            x_wide = ref[at, :].astype(jnp.float32)
            mean_sq = jnp.mean(x_wide * x_wide, axis=-1, keepdims=True)
            ref[at, :] = (x_wide * lax.rsqrt(mean_sq + EPSILON) * gain[...].reshape(1, width)).astype(jnp.bfloat16)
            return carry

        lax.fori_loop(0, CHUNK // PIECE, piece, 0, unroll=2)

    def product(ref, i, w, start):
        return jnp.dot(ref[chunk_rows(i), :], w[:, start], preferred_element_type=jnp.float32).astype(jnp.bfloat16)

    def columns(block):
        if isinstance(block, int):
            return slice(block * head, (block + 1) * head)
        return pl.ds(pl.multiple_of(block * head, head), head)

    def out_rows(device, i):
        return pl.ds(pl.multiple_of(device * rows + i * CHUNK, CHUNK), CHUNK)

    def source(device, n):
        across = device + 2 - 4 * lax.rem(device // 2, 2)
        return jnp.where(n < chunks, device, across), lax.rem(n, chunks)

    def slot_rows(device, n):
        return out_rows(*source(device, n))

    def stage_rows(n):
        return pl.ds(pl.multiple_of(n * CHUNK, CHUNK), CHUNK)

    def mate_copies(n):
        at = slot_rows(me, n)
        return [
            send(k_out.at[at, :], k_out.at[at, :], m_send.at[0, n], m_recv.at[0, n], mate),
            send(v_out.at[at, :], v_out.at[at, :], m_send.at[1, n], m_recv.at[1, n], mate),
            send(mate_q.at[stage_rows(n), :], q_out.at[at, :], m_send.at[2, n], m_recv.at[2, n], mate),
        ]

    def far_kv(n):
        at = slot_rows(me, n)
        return [
            send(far_out.at[2, stage_rows(n), :], k_out.at[at, :], f_send.at[2, n], fkv_recv.at[0, n], far),
            send(far_out.at[3, stage_rows(n), :], v_out.at[at, :], f_send.at[3, n], fkv_recv.at[1, n], far),
        ]

    def far_q(n):
        at = slot_rows(me, n)
        return [
            send(far_out.at[j, stage_rows(n), :], q_out.at[at, :], f_send.at[j, n], fq_recv.at[core, n], far_chip + j)
            for j in range(2)
        ]

    def relay_copies(n):
        at = slot_rows(far, n)
        return [
            send(ref.at[at, :], ref.at[at, :], r_send.at[j, n], r_recv.at[j, n], mate)
            for j, ref in enumerate((k_out, v_out))
        ]

    def near_products(ref, i, n):
        at = slot_rows(me, n)
        k_out[at, :] = product(ref, i, w_own, columns(2))
        v_out[at, :] = product(ref, i, w_own, columns(3))
        q_out[at, :] = product(ref, i, w_own, columns(core))
        mate_q[stage_rows(n), :] = product(ref, i, w_own, columns(1 - core))
        for copy in mate_copies(n):
            copy.start()

    def far_kv_products(ref, i, n):
        for block in (2, 3):
            far_out[block, stage_rows(n), :] = product(ref, i, w_far, columns(block))
        for copy in far_kv(n):
            copy.start()

    def far_q_products(ref, i, n):
        for block in (0, 1):
            far_out[block, stage_rows(n), :] = product(ref, i, w_far, columns(block))
        for copy in far_q(n):
            copy.start()

    def loop(count, body):
        def step(i, carry):
            body(i)
            return carry

        lax.fori_loop(0, count, step, 0)

    def own_norm(i):
        load_chunk(i).wait()
        normalise(x_own, i)

    gain_copy.wait()
    loop(chunks, own_norm)
    for i in range(3):
        local_w[i].wait()
        mate_w[i].wait_recv()
    loop(chunks, lambda i: near_products(x_own, i, i))

    for i in (0, 1):
        far_w[i].wait_recv()
        relay_w[i].start()
    for i in (0, 1):
        relay_w[i].wait_recv()
    loop(chunks, lambda i: far_kv_products(x_own, i, i))
    far_w[2].wait_recv()
    relay_w[2].start()
    relay_w[2].wait_recv()
    loop(chunks, lambda i: far_q_products(x_own, i, i))

    def side_step(i):
        side_chunk(i).wait_recv()
        normalise(x_side, i)
        far_kv_products(x_side, i, chunks + i)
        far_q_products(x_side, i, chunks + i)
        near_products(x_side, i, chunks + i)

    loop(chunks, side_step)

    def drain(n):
        for copy in mate_copies(n):
            copy.wait_send()
            copy.wait_recv()
        for copy in relay_copies(n):
            copy.wait_send()
            copy.wait_recv()
        for copy in far_kv(n):
            copy.wait_send()
        for j, copy in enumerate(far_q(n)):
            copy.wait_send()
            send(far_out.at[j, stage_rows(n), :], q_out.at[slot_rows(me, n), :], f_send.at[j, n], fq_recv.at[j, n], far).wait_recv()

    for copies in (mate_w, far_w, relay_w):
        for copy in copies:
            copy.wait_send()
    loop(chunks, lambda i: side_chunk(i).wait_send())

    def relay_step(n):
        for arrived, onward in zip(far_kv(n), relay_copies(n)):
            arrived.wait_recv()
            onward.start()

        @pl.when(n > 0)
        def _():
            drain(n - 1)

    loop(2 * chunks, relay_step)
    drain(2 * chunks - 1)


def store(*refs):
    count = len(refs) // 2
    sources, targets, sems = refs[:count], refs[count:2 * count], refs[2 * count]
    size = sources[0].shape[0] // STORES
    copies = [
        pltpu.make_async_copy(source.at[pl.ds(i * size, size), :], target.at[pl.ds(i * size, size), :], sems.at[o, i])
        for o, (source, target) in enumerate(zip(sources, targets))
        for i in range(STORES)
    ]
    for copy in copies:
        copy.start()
    for copy in copies:
        copy.wait()


def solution(mesh):
    group_size = mesh.shape["tp"]

    def local_step(x_rows, norm_gain, w_q, w_k, w_v):
        rows, width = x_rows.shape
        head = w_q.shape[2]
        slots = 2 * (rows // CHUNK)
        chunks = rows // CHUNK
        dma = pltpu.SemaphoreType.DMA
        any_space = pl.BlockSpec(memory_space=pl.ANY)
        vmem = pl.BlockSpec(memory_space=pltpu.VMEM)
        outs = pl.pallas_call(
            kernel,
            out_shape=[pltpu.VMEM((group_size * rows, head), jnp.bfloat16)] * 3,
            in_specs=[any_space] * 5,
            out_specs=[vmem] * 3,
            scratch_shapes=[
                pltpu.VMEM((rows, width), jnp.bfloat16),
                pltpu.VMEM((rows, width), jnp.bfloat16),
                pltpu.VMEM((width, 4 * head), jnp.bfloat16),
                pltpu.VMEM((width, 4 * head), jnp.bfloat16),
                pltpu.VMEM((4, 2 * rows, head), jnp.bfloat16),
                pltpu.VMEM((2 * rows, head), jnp.bfloat16),
                pltpu.VMEM((width,), jnp.float32),
                dma(()), dma((chunks,)), dma((3,)), dma((3,)), dma((3,)), dma((3,)), dma((3,)), dma((3,)), dma((3,)),
                dma((chunks,)), dma((chunks,)), dma((3, slots)), dma((3, slots)), dma((4, slots)), dma((2, slots)),
                dma((2, slots)), dma((2, slots)), dma((2, slots)),
            ],
            compiler_params=pltpu.CompilerParams(collective_id=0, has_side_effects=True, vmem_limit_bytes=44 * 1024 * 1024),
        )(x_rows, norm_gain, w_q.reshape(width, head), w_k, w_v)
        outs = pl.pallas_call(
            store,
            out_shape=[pltpu.HBM((group_size * rows, head), jnp.bfloat16)] * 3,
            in_specs=[vmem] * 3,
            out_specs=[pl.BlockSpec(memory_space=pltpu.HBM)] * 3,
            scratch_shapes=[dma((3, STORES))],
            compiler_params=pltpu.CompilerParams(vmem_limit_bytes=1024 * 1024),
        )(*(pltpu.with_memory_space_constraint(out, pltpu.VMEM) for out in outs))
        return tuple(out[:, None, :] for out in outs)

    return jax.shard_map(local_step, mesh=mesh, in_specs=(P(("dp", "tp"), None), P(None), P(None, "tp", None), P(None, "tp"), P(None, "tp")), out_specs=(P("dp", "tp", None), P("dp", "tp", None), P("dp", "tp", None)), check_vma=False)
```

```python
import jax
import jax.numpy as jnp
from jax import lax
from jax.experimental import pallas as pl
from jax.experimental.pallas import tpu as pltpu
from jax.sharding import PartitionSpec as P

EPSILON = 1e-6
CHUNK = 256
PIECE = 16
STORES = 4


def kernel(x_hbm, gain_hbm, wq_hbm, wk_hbm, wv_hbm, q_out, k_out, v_out,
           x_own, x_side, w_own, w_far, far_out, mate_q, gain,
           answer, load_gain, load_x, load_w, mw_send, mw_recv, fw_send, fw_recv, rw_send, rw_recv,
           x_send, x_recv, m_send, m_recv, f_send, fq_recv, fkv_recv, r_send, r_recv):
    rows, width = x_hbm.shape
    head = wq_hbm.shape[1]
    part = wk_hbm.shape[1]
    chunks = rows // CHUNK

    me = lax.axis_index("tp")
    core = lax.rem(me, 2)
    mate = me + 1 - 2 * core
    row = me // 4
    side = me + 4 - 8 * row
    far = me + 2 - 4 * lax.rem(me // 2, 2)
    far_mate = far + 1 - 2 * core
    far_chip = far - core

    barrier = pltpu.get_barrier_semaphore()
    for peer in (mate, far, far_mate):
        pl.semaphore_signal(barrier, inc=1, device_id={"tp": peer})

    @pl.when(row == 0)
    def _():
        pl.semaphore_signal(barrier, inc=1, device_id={"tp": side})

    def send(src, dst, send_sem, recv_sem, to):
        return pltpu.make_async_remote_copy(src_ref=src, dst_ref=dst, send_sem=send_sem, recv_sem=recv_sem, device_id={"tp": to})

    q_cols = pl.ds(pl.multiple_of(core * head, head), head)
    k_cols = pl.ds(pl.multiple_of(2 * head + core * part, part), part)
    v_cols = pl.ds(pl.multiple_of(3 * head + core * part, part), part)
    mine = ((wk_hbm, k_cols), (wv_hbm, v_cols), (wq_hbm, q_cols))

    local_w = [pltpu.make_async_copy(src, w_own.at[:, cols], load_w.at[i]) for i, (src, cols) in enumerate(mine)]
    mate_w = [send(src, w_own.at[:, cols], mw_send.at[i], mw_recv.at[i], mate) for i, (src, cols) in enumerate(mine)]
    far_w = [send(src, w_far.at[:, cols], fw_send.at[i], fw_recv.at[i], far) for i, (src, cols) in enumerate(mine)]
    relay_w = [send(w_far.at[:, cols], w_far.at[:, cols], rw_send.at[i], rw_recv.at[i], mate) for i, (src, cols) in enumerate(mine)]

    def chunk_rows(i):
        return pl.ds(pl.multiple_of(i * CHUNK, CHUNK), CHUNK)

    def load_chunk(i):
        return pltpu.make_async_copy(x_hbm.at[chunk_rows(i), :], x_own.at[chunk_rows(i), :], load_x.at[i])

    def side_chunk(i):
        return send(x_hbm.at[chunk_rows(i), :], x_side.at[chunk_rows(i), :], x_send.at[i], x_recv.at[i], side)

    gain_copy = pltpu.make_async_copy(gain_hbm, gain, load_gain)
    gain_copy.start()
    for i in range(chunks):
        load_chunk(i).start()
    for copy in local_w:
        copy.start()

    pl.semaphore_wait(barrier, 3 + row)
    for i in range(3):
        far_w[i].start()

    @pl.when(row == 1)
    def _():
        pl.semaphore_signal(answer, inc=1, device_id={"tp": side})

    for i in range(3):
        mate_w[i].start()

    @pl.when(row == 0)
    def _():
        pl.semaphore_wait(answer, 1)

    for i in range(chunks):
        side_chunk(i).start()

    def normalise(ref, i):
        def piece(p, carry):
            at = pl.ds(pl.multiple_of(i * CHUNK + p * PIECE, PIECE), PIECE)
            x_wide = ref[at, :].astype(jnp.float32)
            mean_sq = jnp.mean(x_wide * x_wide, axis=-1, keepdims=True)
            ref[at, :] = (x_wide * lax.rsqrt(mean_sq + EPSILON) * gain[...].reshape(1, width)).astype(jnp.bfloat16)
            return carry

        lax.fori_loop(0, CHUNK // PIECE, piece, 0, unroll=2)

    def product(ref, i, w, start):
        return jnp.dot(ref[chunk_rows(i), :], w[:, start], preferred_element_type=jnp.float32).astype(jnp.bfloat16)

    def columns(block):
        if isinstance(block, int):
            return slice(block * head, (block + 1) * head)
        return pl.ds(pl.multiple_of(block * head, head), head)

    def out_rows(device, i):
        return pl.ds(pl.multiple_of(device * rows + i * CHUNK, CHUNK), CHUNK)

    def source(device, n):
        across = device + 4 - 8 * (device // 4)
        return jnp.where(n < chunks, device, across), lax.rem(n, chunks)

    def slot_rows(device, n):
        return out_rows(*source(device, n))

    def stage_rows(n):
        return pl.ds(pl.multiple_of(n * CHUNK, CHUNK), CHUNK)

    def mate_copies(n):
        at = slot_rows(me, n)
        return [
            send(k_out.at[at, :], k_out.at[at, :], m_send.at[0, n], m_recv.at[0, n], mate),
            send(v_out.at[at, :], v_out.at[at, :], m_send.at[1, n], m_recv.at[1, n], mate),
            send(mate_q.at[stage_rows(n), :], q_out.at[at, :], m_send.at[2, n], m_recv.at[2, n], mate),
        ]

    def far_kv(n):
        at = slot_rows(me, n)
        return [
            send(far_out.at[2, stage_rows(n), :], k_out.at[at, :], f_send.at[2, n], fkv_recv.at[0, n], far),
            send(far_out.at[3, stage_rows(n), :], v_out.at[at, :], f_send.at[3, n], fkv_recv.at[1, n], far),
        ]

    def far_q(n):
        at = slot_rows(me, n)
        return [
            send(far_out.at[j, stage_rows(n), :], q_out.at[at, :], f_send.at[j, n], fq_recv.at[core, n], far_chip + j)
            for j in range(2)
        ]

    def relay_copies(n):
        at = slot_rows(far, n)
        return [
            send(ref.at[at, :], ref.at[at, :], r_send.at[j, n], r_recv.at[j, n], mate)
            for j, ref in enumerate((k_out, v_out))
        ]

    def near_products(ref, i, n):
        at = slot_rows(me, n)
        k_out[at, :] = product(ref, i, w_own, columns(2))
        v_out[at, :] = product(ref, i, w_own, columns(3))
        q_out[at, :] = product(ref, i, w_own, columns(core))
        mate_q[stage_rows(n), :] = product(ref, i, w_own, columns(1 - core))
        for copy in mate_copies(n):
            copy.start()

    def far_kv_products(ref, i, n):
        for block in (2, 3):
            far_out[block, stage_rows(n), :] = product(ref, i, w_far, columns(block))
        for copy in far_kv(n):
            copy.start()

    def far_q_products(ref, i, n):
        for block in (0, 1):
            far_out[block, stage_rows(n), :] = product(ref, i, w_far, columns(block))
        for copy in far_q(n):
            copy.start()

    def loop(count, body):
        def step(i, carry):
            body(i)
            return carry

        lax.fori_loop(0, count, step, 0)

    def own_norm(i):
        load_chunk(i).wait()
        normalise(x_own, i)

    gain_copy.wait()
    loop(chunks, own_norm)
    for i in range(3):
        local_w[i].wait()
        mate_w[i].wait_recv()
    loop(chunks, lambda i: near_products(x_own, i, i))

    for i in (0, 1):
        far_w[i].wait_recv()
        relay_w[i].start()
    for i in (0, 1):
        relay_w[i].wait_recv()
    loop(chunks, lambda i: far_kv_products(x_own, i, i))
    far_w[2].wait_recv()
    relay_w[2].start()
    relay_w[2].wait_recv()
    loop(chunks, lambda i: far_q_products(x_own, i, i))

    def side_step(i):
        side_chunk(i).wait_recv()
        normalise(x_side, i)
        far_kv_products(x_side, i, chunks + i)
        far_q_products(x_side, i, chunks + i)
        near_products(x_side, i, chunks + i)

    loop(chunks, side_step)

    def drain(n):
        for copy in mate_copies(n):
            copy.wait_send()
            copy.wait_recv()
        for copy in relay_copies(n):
            copy.wait_send()
            copy.wait_recv()
        for copy in far_kv(n):
            copy.wait_send()
        for j, copy in enumerate(far_q(n)):
            copy.wait_send()
            send(far_out.at[j, stage_rows(n), :], q_out.at[slot_rows(me, n), :], f_send.at[j, n], fq_recv.at[j, n], far).wait_recv()

    for copies in (mate_w, far_w, relay_w):
        for copy in copies:
            copy.wait_send()
    loop(chunks, lambda i: side_chunk(i).wait_send())

    def relay_step(n):
        for arrived, onward in zip(far_kv(n), relay_copies(n)):
            arrived.wait_recv()
            onward.start()

        @pl.when(n > 0)
        def _():
            drain(n - 1)

    loop(2 * chunks, relay_step)
    drain(2 * chunks - 1)


def store(*refs):
    count = len(refs) // 2
    sources, targets, sems = refs[:count], refs[count:2 * count], refs[2 * count]
    size = sources[0].shape[0] // STORES
    copies = [
        pltpu.make_async_copy(source.at[pl.ds(i * size, size), :], target.at[pl.ds(i * size, size), :], sems.at[o, i])
        for o, (source, target) in enumerate(zip(sources, targets))
        for i in range(STORES)
    ]
    for copy in copies:
        copy.start()
    for copy in copies:
        copy.wait()


def solution(mesh):
    group_size = mesh.shape["tp"]

    def local_step(x_rows, norm_gain, w_q, w_k, w_v):
        rows, width = x_rows.shape
        head = w_q.shape[2]
        slots = 2 * (rows // CHUNK)
        chunks = rows // CHUNK
        dma = pltpu.SemaphoreType.DMA
        any_space = pl.BlockSpec(memory_space=pl.ANY)
        vmem = pl.BlockSpec(memory_space=pltpu.VMEM)
        outs = pl.pallas_call(
            kernel,
            out_shape=[pltpu.VMEM((group_size * rows, head), jnp.bfloat16)] * 3,
            in_specs=[any_space] * 5,
            out_specs=[vmem] * 3,
            scratch_shapes=[
                pltpu.VMEM((rows, width), jnp.bfloat16),
                pltpu.VMEM((rows, width), jnp.bfloat16),
                pltpu.VMEM((width, 4 * head), jnp.bfloat16),
                pltpu.VMEM((width, 4 * head), jnp.bfloat16),
                pltpu.VMEM((4, 2 * rows, head), jnp.bfloat16),
                pltpu.VMEM((2 * rows, head), jnp.bfloat16),
                pltpu.VMEM((width,), jnp.float32),
                pltpu.SemaphoreType.REGULAR, dma(()), dma((chunks,)), dma((3,)), dma((3,)), dma((3,)), dma((3,)), dma((3,)), dma((3,)), dma((3,)),
                dma((chunks,)), dma((chunks,)), dma((3, slots)), dma((3, slots)), dma((4, slots)), dma((2, slots)),
                dma((2, slots)), dma((2, slots)), dma((2, slots)),
            ],
            compiler_params=pltpu.CompilerParams(collective_id=0, has_side_effects=True, vmem_limit_bytes=44 * 1024 * 1024),
        )(x_rows, norm_gain, w_q.reshape(width, head), w_k, w_v)
        outs = pl.pallas_call(
            store,
            out_shape=[pltpu.HBM((group_size * rows, head), jnp.bfloat16)] * 3,
            in_specs=[vmem] * 3,
            out_specs=[pl.BlockSpec(memory_space=pltpu.HBM)] * 3,
            scratch_shapes=[dma((3, STORES))],
            compiler_params=pltpu.CompilerParams(vmem_limit_bytes=1024 * 1024),
        )(*(pltpu.with_memory_space_constraint(out, pltpu.VMEM) for out in outs))
        return tuple(out[:, None, :] for out in outs)

    return jax.shard_map(local_step, mesh=mesh, in_specs=(P(("dp", "tp"), None), P(None), P(None, "tp", None), P(None, "tp"), P(None, "tp")), out_specs=(P("dp", "tp", None), P("dp", "tp", None), P("dp", "tp", None)), check_vma=False)
```

```python
import functools

import jax
import jax.numpy as jnp
from jax import lax
from jax.experimental import pallas as pl
from jax.experimental.pallas import tpu as pltpu
from jax.sharding import PartitionSpec as P

EPSILON = 1e-6
CHUNK = 256
PIECE = 16

OWN, SIDE, MATE, MATE_SIDE, FAR, FAR_MATE = range(6)
LATE_FAR, LATE_FAR_MATE = range(2)
K, V, Q_SAME, Q_OTHER = range(4)


class Place:
    def __init__(self):
        self.me = lax.axis_index("tp")
        self.core = lax.rem(self.me, 2)
        self.row = self.me // 4
        self.mate = self.me + 1 - 2 * self.core
        self.side = self.across(self.me)
        self.far = self.me + 2 - 4 * lax.rem(self.me // 2, 2)
        self.far_mate = self.far + 1 - 2 * self.core
        self.first = 1 + 2 * self.core
        self.first_other = 3 - 2 * self.core

    def across(self, device):
        return device + 4 - 8 * (device // 4)


def send(src, dst, send_sem, recv_sem, to):
    return pltpu.make_async_remote_copy(src_ref=src, dst_ref=dst, send_sem=send_sem, recv_sem=recv_sem, device_id={"tp": to})


def signal(sem, to):
    pl.semaphore_signal(sem, inc=1, device_id={"tp": to})


def loop(start, stop, body):
    def step(i, carry):
        body(i)
        return carry

    lax.fori_loop(start, stop, step, 0)


def chunk_rows(i, base=0):
    return pl.ds(pl.multiple_of(base + i * CHUNK, CHUNK), CHUNK)


def gather(x_hbm, gain_hbm, wq_hbm, wk_hbm, wv_hbm, q_early, k_early, v_early, q_late, k_late, v_late, far_late,
           x_own, x_side, w_own, w_far, far_own, mate_q, gain,
           answer, load_gain, load_x, load_w, mw_send, mw_recv, fw_send, fw_recv, rw_send, rw_recv,
           x_send, x_recv, m_send, m_recv, f_send, f_recv, r_send, r_recv):
    rows, width = x_hbm.shape
    head = wq_hbm.shape[1]
    part = wk_hbm.shape[1]
    chunks = rows // CHUNK
    at = Place()
    core = at.core

    barrier = pltpu.get_barrier_semaphore()
    for peer in (at.mate, at.far, at.far_mate):
        signal(barrier, peer)

    @pl.when(at.row == 0)
    def _():
        signal(barrier, at.side)

    q_cols = pl.ds(pl.multiple_of(core * head, head), head)
    k_cols = pl.ds(pl.multiple_of(2 * head + core * part, part), part)
    v_cols = pl.ds(pl.multiple_of(3 * head + core * part, part), part)
    mine = ((wk_hbm, k_cols), (wv_hbm, v_cols), (wq_hbm, q_cols))
    local_w = [pltpu.make_async_copy(src, w_own.at[:, cols], load_w.at[i]) for i, (src, cols) in enumerate(mine)]
    mate_w = [send(w_own.at[:, cols], w_own.at[:, cols], mw_send.at[i], mw_recv.at[i], at.mate) for i, (src, cols) in enumerate(mine)]
    far_w = [send(w_own.at[:, cols], w_far.at[:, cols], fw_send.at[i], fw_recv.at[i], at.far) for i, (src, cols) in enumerate(mine)]
    relay_w = [send(w_far.at[:, cols], w_far.at[:, cols], rw_send.at[i], rw_recv.at[i], at.mate) for i, (src, cols) in enumerate(mine)]

    def load_chunk(i):
        return pltpu.make_async_copy(x_hbm.at[chunk_rows(i), :], x_own.at[chunk_rows(i), :], load_x.at[i])

    def side_chunk(i):
        return send(x_hbm.at[chunk_rows(i), :], x_side.at[chunk_rows(i), :], x_send.at[i], x_recv.at[i], at.side)

    for copy in local_w:
        copy.start()
    gain_copy = pltpu.make_async_copy(gain_hbm, gain, load_gain)
    gain_copy.start()
    for i in range(chunks):
        load_chunk(i).start()

    pl.semaphore_wait(barrier, 3 + at.row)
    for i in range(3):
        local_w[i].wait()
        far_w[i].start()

    @pl.when(at.row == 1)
    def _():
        signal(answer, at.side)

    for copy in mate_w:
        copy.start()

    @pl.when(at.row == 0)
    def _():
        pl.semaphore_wait(answer, 1)

    for i in range(chunks):
        side_chunk(i).start()

    def normalise(ref, i):
        def piece(p, carry):
            here = pl.ds(pl.multiple_of(i * CHUNK + p * PIECE, PIECE), PIECE)
            x_wide = ref[here, :].astype(jnp.float32)
            mean_sq = jnp.mean(x_wide * x_wide, axis=-1, keepdims=True)
            ref[here, :] = (x_wide * lax.rsqrt(mean_sq + EPSILON) * gain[...].reshape(1, width)).astype(jnp.bfloat16)
            return carry

        lax.fori_loop(0, CHUNK // PIECE, piece, 0, unroll=2)

    def product(ref, i, w, block):
        cols = slice(block * head, (block + 1) * head) if isinstance(block, int) else pl.ds(pl.multiple_of(block * head, head), head)
        return jnp.dot(ref[chunk_rows(i), :], w[:, cols], preferred_element_type=jnp.float32).astype(jnp.bfloat16)

    far_columns = {K: 2, V: 3, Q_SAME: core, Q_OTHER: 1 - core}

    def mate_copies(block, i):
        n = block * chunks + i
        here, there = chunk_rows(i, block * rows), chunk_rows(i, (MATE + block) * rows)
        sources = (k_early.at[here, :], v_early.at[here, :], mate_q.at[here, :])
        return [send(src, dst.at[there, :], m_send.at[j, n], m_recv.at[j, n], at.mate)
                for j, (src, dst) in enumerate(zip(sources, (k_early, v_early, q_early)))]

    def near_products(ref, block, i):
        here = chunk_rows(i, block * rows)
        k_early[here, :] = product(ref, i, w_own, 2)
        v_early[here, :] = product(ref, i, w_own, 3)
        q_early[here, :] = product(ref, i, w_own, core)
        mate_q[here, :] = product(ref, i, w_own, 1 - core)
        for copy in mate_copies(block, i):
            copy.start()

    def far_products(ref, stage, kinds, i):
        for kind in kinds:
            stage[kind, chunk_rows(i), :] = product(ref, i, w_far, far_columns[kind])

    def own_message(kind, i):
        dst = {K: k_early, V: v_early, Q_SAME: q_early, Q_OTHER: q_early}[kind]
        there = chunk_rows(i, (FAR_MATE if kind == Q_OTHER else FAR) * rows)
        return send(far_own.at[kind, chunk_rows(i), :], dst.at[there, :], f_send.at[kind, i], f_recv.at[kind, i],
                    at.far_mate if kind == Q_OTHER else at.far)

    side_message = functools.partial(late_message, at, rows, chunks, far_late, (k_late, v_late, q_late, q_late), f_send, f_recv)

    def relay(j, i):
        ref = (k_early, v_early)[j]
        return send(ref.at[chunk_rows(i, FAR * rows), :], ref.at[chunk_rows(i, FAR_MATE * rows), :], r_send.at[j, i], r_recv.at[j, i], at.mate)

    def own_norm(i):
        load_chunk(i).wait()
        normalise(x_own, i)

    gain_copy.wait()
    loop(0, chunks, own_norm)
    for copy in mate_w:
        copy.wait_recv()
    loop(0, chunks, lambda i: near_products(x_own, OWN, i))

    def far_step(kinds, i):
        far_products(x_own, far_own, kinds, i)
        for kind in kinds:
            own_message(kind, i).start()

    for i in (0, 1):
        far_w[i].wait_recv()
        relay_w[i].start()
    for i in (0, 1):
        relay_w[i].wait_recv()
    loop(0, chunks, functools.partial(far_step, (K, V)))
    far_w[2].wait_recv()
    relay_w[2].start()
    relay_w[2].wait_recv()
    loop(0, chunks, functools.partial(far_step, (Q_SAME, Q_OTHER)))

    def side_step(i):
        side_chunk(i).wait_recv()
        normalise(x_side, i)
        far_products(x_side, far_late, (Q_OTHER, K, V, Q_SAME), i)

        @pl.when(i < at.first)
        def _():
            side_message(Q_OTHER, i).start()

        @pl.when(i == at.first - 1)
        def _():
            loop(0, at.first, start_same)

        near_products(x_side, SIDE, i)

    def start_same(i):
        for kind in (K, V, Q_SAME):
            side_message(kind, i).start()

    loop(0, chunks, side_step)

    def relay_step(i):
        for j, kind in enumerate((K, V)):
            own_message(kind, i).wait_recv()
            relay(j, i).start()

    loop(0, chunks, relay_step)

    for copies in (mate_w, far_w, relay_w):
        for copy in copies:
            copy.wait_send()

    def drain(i):
        side_chunk(i).wait_send()
        for block in (OWN, SIDE):
            for copy in mate_copies(block, i):
                copy.wait_send()
                copy.wait_recv()
        for kind in (Q_SAME, Q_OTHER):
            own_message(kind, i).wait_recv()
        for kind in (K, V, Q_SAME, Q_OTHER):
            own_message(kind, i).wait_send()
        for j in range(2):
            relay(j, i).wait_send()
            relay(j, i).wait_recv()

    loop(0, chunks, drain)
    loop(0, at.first_other, lambda i: side_message(Q_OTHER, i).wait_recv())

    def drain_side(i):
        side_message(Q_OTHER, i).wait_send()
        for kind in (K, V, Q_SAME):
            side_message(kind, i).wait_send()
            side_message(kind, i).wait_recv()

    loop(0, at.first, drain_side)


def late_message(at, rows, chunks, stage, targets, f_send, f_recv, kind, i):
    there = chunk_rows(i, (LATE_FAR_MATE if kind == Q_OTHER else LATE_FAR) * rows)
    n = chunks + i
    return send(stage.at[kind, chunk_rows(i), :], targets[kind].at[there, :], f_send.at[kind, n], f_recv.at[kind, n],
                at.far_mate if kind == Q_OTHER else at.far)


def finish(k_held, v_held, far_late, token, q_late, k_late, v_late, answer, f_send, f_recv, r_send, r_recv):
    rows = far_late.shape[1]
    chunks = rows // CHUNK
    at = Place()
    barrier = pltpu.get_barrier_semaphore()
    signal(barrier, at.far)

    @pl.when(at.core == 0)
    def _():
        signal(barrier, at.mate)
        signal(barrier, at.far_mate)

    pl.semaphore_wait(barrier, 1 + 2 * at.core)

    @pl.when(at.core == 1)
    def _():
        signal(answer, at.mate)
        signal(answer, at.far_mate)

    message = functools.partial(late_message, at, rows, 0, far_late, (k_late, v_late, q_late, q_late), f_send, f_recv)

    def relay(j, i, sources=(k_late, v_late)):
        return send(sources[j].at[chunk_rows(i, LATE_FAR * rows), :], (k_late, v_late)[j].at[chunk_rows(i, LATE_FAR_MATE * rows), :],
                    r_send.at[j, i], r_recv.at[j, i], at.mate)

    def start_same(i):
        for kind in (K, V, Q_SAME):
            message(kind, i).start()

    loop(at.first, chunks, start_same)

    @pl.when(at.core == 0)
    def _():
        pl.semaphore_wait(answer, 2)

    loop(at.first, chunks, lambda i: message(Q_OTHER, i).start())

    def relay_held(i):
        for j in range(2):
            relay(j, i, (k_held, v_held)).start()

    loop(0, at.first, relay_held)

    def relay_step(i):
        for j, kind in enumerate((K, V)):
            message(kind, i).wait_recv()
            relay(j, i).start()

    loop(at.first, chunks, relay_step)

    def drain(i):
        message(Q_SAME, i).wait_recv()
        for kind in (K, V, Q_SAME, Q_OTHER):
            message(kind, i).wait_send()

    def drain_relay(i):
        for j in range(2):
            relay(j, i).wait_send()
            relay(j, i).wait_recv()

    loop(0, chunks, drain_relay)
    loop(at.first_other, chunks, lambda i: message(Q_OTHER, i).wait_recv())
    loop(at.first, chunks, drain)


def store_early(q_early, k_early, v_early, q_out, k_out, v_out, token, sems):
    at = Place()
    owners = (at.me, at.side, at.mate, at.across(at.mate), at.far, at.far_mate)
    rows = q_early.shape[0] // len(owners)
    copies = [
        pltpu.make_async_copy(source.at[pl.ds(block * rows, rows), :], target.at[pl.ds(pl.multiple_of(owner * rows, rows), rows), :], sems.at[o, block])
        for o, (source, target) in enumerate(((q_early, q_out), (k_early, k_out), (v_early, v_out)))
        for block, owner in enumerate(owners)
    ]
    for copy in copies:
        copy.start()
    for copy in copies:
        copy.wait()


def store_late(q_held, k_held, v_held, q_late, k_late, v_late, q_in, k_in, v_in, q_out, k_out, v_out, sems):
    at = Place()
    rows = q_late.shape[0] // 2
    held, late, outs = (q_held, k_held, v_held), (q_late, k_late, v_late), (q_out, k_out, v_out)

    def copy(o, block, part, sources):
        first, count = ((0, CHUNK), (CHUNK, rows - 2 * CHUNK), (rows - CHUNK, CHUNK))[part]
        owner = at.across((at.far, at.far_mate)[block])
        return pltpu.make_async_copy(
            sources[o].at[pl.ds(block * rows + first, count), :],
            outs[o].at[pl.ds(pl.multiple_of(owner * rows + first, CHUNK), count), :],
            sems.at[o, block, part],
        )

    for o in range(3):
        for block in range(2):
            relayed = block == LATE_FAR_MATE and o > 0
            copy(o, block, 0, late if relayed else held).start()
            copy(o, block, 2, late).start()
            if relayed:
                copy(o, block, 1, late).start()

    for core in range(2):
        @pl.when(at.core == core)
        def _():
            for o in range(3):
                copy(o, LATE_FAR, 1, held if core else late).start()
            copy(0, LATE_FAR_MATE, 1, late if core else held).start()

    for o in range(3):
        for block in range(2):
            for part in range(3):
                copy(o, block, part, late).wait()


def in_vmem(*arrays):
    return tuple(pltpu.with_memory_space_constraint(array, pltpu.VMEM) for array in arrays)


def solution(mesh):
    group_size = mesh.shape["tp"]

    def local_step(x_rows, norm_gain, w_q, w_k, w_v):
        rows, width = x_rows.shape
        head = w_q.shape[2]
        chunks = rows // CHUNK
        dma = pltpu.SemaphoreType.DMA
        any_space = pl.BlockSpec(memory_space=pl.ANY)
        vmem = pl.BlockSpec(memory_space=pltpu.VMEM)
        hbm = pl.BlockSpec(memory_space=pltpu.HBM)

        def small(**settings):
            return pltpu.CompilerParams(vmem_limit_bytes=1024 * 1024, **settings)

        early = [pltpu.VMEM((6 * rows, head), jnp.bfloat16)] * 3
        late = [pltpu.VMEM((2 * rows, head), jnp.bfloat16)] * 3
        final = [pltpu.HBM((group_size * rows, head), jnp.bfloat16)] * 3

        *gathered, far_late = pl.pallas_call(
            gather,
            out_shape=early + late + [pltpu.VMEM((4, rows, head), jnp.bfloat16)],
            in_specs=[any_space] * 5,
            out_specs=[vmem] * 7,
            scratch_shapes=[
                pltpu.VMEM((rows, width), jnp.bfloat16),
                pltpu.VMEM((rows, width), jnp.bfloat16),
                pltpu.VMEM((width, 4 * head), jnp.bfloat16),
                pltpu.VMEM((width, 4 * head), jnp.bfloat16),
                pltpu.VMEM((4, rows, head), jnp.bfloat16),
                pltpu.VMEM((2 * rows, head), jnp.bfloat16),
                pltpu.VMEM((width,), jnp.float32),
                pltpu.SemaphoreType.REGULAR, dma(()), dma((chunks,)),
                dma((3,)), dma((3,)), dma((3,)), dma((3,)), dma((3,)), dma((3,)), dma((3,)),
                dma((chunks,)), dma((chunks,)), dma((3, 2 * chunks)), dma((3, 2 * chunks)),
                dma((4, 2 * chunks)), dma((4, 2 * chunks)), dma((2, chunks)), dma((2, chunks)),
            ],
            compiler_params=pltpu.CompilerParams(collective_id=0, has_side_effects=True, vmem_limit_bytes=40 * 1024 * 1024),
            name="gather",
        )(x_rows, norm_gain, w_q.reshape(width, head), w_k, w_v)
        *stored, token = pl.pallas_call(
            store_early,
            out_shape=final + [pltpu.HBM((8, 128), jnp.float32)],
            in_specs=[vmem] * 3,
            out_specs=[hbm] * 4,
            scratch_shapes=[dma((3, 6))],
            compiler_params=small(),
            name="store_early",
        )(*in_vmem(*gathered[:3]))
        held = in_vmem(*gathered[3:])
        finished = pl.pallas_call(
            finish,
            out_shape=late,
            in_specs=[vmem] * 3 + [hbm],
            out_specs=[vmem] * 3,
            scratch_shapes=[
                pltpu.SemaphoreType.REGULAR, dma((4, chunks)), dma((4, chunks)), dma((2, chunks)), dma((2, chunks)),
            ],
            compiler_params=small(collective_id=1, has_side_effects=True),
            name="finish",
        )(*held[1:], *in_vmem(far_late), pltpu.with_memory_space_constraint(token, pltpu.HBM))
        outs = pl.pallas_call(
            store_late,
            out_shape=final,
            in_specs=[vmem] * 6 + [hbm] * 3,
            out_specs=[hbm] * 3,
            input_output_aliases={6: 0, 7: 1, 8: 2},
            scratch_shapes=[dma((3, 2, 3))],
            compiler_params=small(),
            name="store_late",
        )(*held, *in_vmem(*finished), *stored)
        return tuple(out[:, None, :] for out in outs)

    return jax.shard_map(local_step, mesh=mesh, in_specs=(P(("dp", "tp"), None), P(None), P(None, "tp", None), P(None, "tp"), P(None, "tp")), out_specs=(P("dp", "tp", None), P("dp", "tp", None), P("dp", "tp", None)), check_vma=False)
```

```python
import functools

import jax
import jax.numpy as jnp
from jax import lax
from jax.experimental import pallas as pl
from jax.experimental.pallas import tpu as pltpu
from jax.sharding import PartitionSpec as P

EPSILON = 1e-6
CHUNK = 256
SIDE_CHUNK = 128
PIECE = 16

K, V, Q = range(3)
KV, KVQ = pl.ds(0, 2), pl.ds(0, 3)
Q_SAME, Q_OTHER = 2, 3
OWN, SIDE, MATE, MATE_SIDE, FAR, FAR_MATE = range(6)
LATE_FAR, LATE_FAR_MATE = range(2)


class Place:
    def __init__(self):
        self.me = lax.axis_index("tp")
        self.core = lax.rem(self.me, 2)
        self.row = self.me // 4
        self.mate = self.me + 1 - 2 * self.core
        self.side = self.across(self.me)
        self.far = self.me + 2 - 4 * lax.rem(self.me // 2, 2)
        self.far_mate = self.far + 1 - 2 * self.core
        self.first = 1 + 2 * self.core
        self.first_other = 3 - 2 * self.core

    def across(self, device):
        return device + 4 - 8 * (device // 4)


def send(src, dst, send_sem, recv_sem, to):
    return pltpu.make_async_remote_copy(src_ref=src, dst_ref=dst, send_sem=send_sem, recv_sem=recv_sem, device_id={"tp": to})


def signal(sem, to):
    pl.semaphore_signal(sem, inc=1, device_id={"tp": to})


def loop(start, stop, body):
    def step(i, carry):
        body(i)
        return carry

    lax.fori_loop(start, stop, step, 0)


def span(i, size, base=0):
    return pl.ds(pl.multiple_of(base + i * size, size), size)


def side_messages(at, rows, stage, target, send_sems, recv_sems, i):
    return (
        send(stage.at[KVQ, span(i, CHUNK), :], target.at[KVQ, span(i, CHUNK, LATE_FAR * rows), :],
             send_sems.at[0, i], recv_sems.at[0, i], at.far),
        send(stage.at[Q_OTHER, span(i, CHUNK), :], target.at[Q, span(i, CHUNK, LATE_FAR_MATE * rows), :],
             send_sems.at[1, i], recv_sems.at[1, i], at.far_mate),
    )


def gather(x_hbm, gain_hbm, wq_hbm, wk_hbm, wv_hbm, early, late, far_late,
           x_own, x_side, w_own, w_far, far_own, mate_q, gain,
           answer, load_gain, load_x, load_w, mw_send, mw_recv, fw_send, fw_recv, rw_send, rw_recv,
           x_send, x_recv, mo_send, mo_recv, ms_send, ms_recv, fo_send, fo_recv, fs_send, fs_recv, r_send, r_recv):
    rows, width = x_hbm.shape
    head = wq_hbm.shape[1]
    part = wk_hbm.shape[1]
    chunks = rows // CHUNK
    side_chunks = rows // SIDE_CHUNK
    at = Place()
    core = at.core

    barrier = pltpu.get_barrier_semaphore()
    for peer in (at.mate, at.far, at.far_mate):
        signal(barrier, peer)

    @pl.when(at.row == 0)
    def _():
        signal(barrier, at.side)

    q_cols = pl.ds(pl.multiple_of(core * head, head), head)
    k_cols = pl.ds(pl.multiple_of(2 * head + core * part, part), part)
    v_cols = pl.ds(pl.multiple_of(3 * head + core * part, part), part)
    mine = ((wk_hbm, k_cols), (wv_hbm, v_cols), (wq_hbm, q_cols))
    local_w = [pltpu.make_async_copy(src, w_own.at[:, cols], load_w.at[i]) for i, (src, cols) in enumerate(mine)]
    mate_w = [send(w_own.at[:, cols], w_own.at[:, cols], mw_send.at[i], mw_recv.at[i], at.mate) for i, (src, cols) in enumerate(mine)]
    far_w = [send(w_own.at[:, cols], w_far.at[:, cols], fw_send.at[i], fw_recv.at[i], at.far) for i, (src, cols) in enumerate(mine)]
    relay_w = [send(w_far.at[:, cols], w_far.at[:, cols], rw_send.at[i], rw_recv.at[i], at.mate) for i, (src, cols) in enumerate(mine)]

    def load_chunk(i):
        return pltpu.make_async_copy(x_hbm.at[span(i, CHUNK), :], x_own.at[span(i, CHUNK), :], load_x.at[i])

    def side_chunk(i):
        return send(x_hbm.at[span(i, SIDE_CHUNK), :], x_side.at[span(i, SIDE_CHUNK), :], x_send.at[i], x_recv.at[i], at.side)

    for copy in local_w:
        copy.start()
    gain_copy = pltpu.make_async_copy(gain_hbm, gain, load_gain)
    gain_copy.start()
    for i in range(chunks):
        load_chunk(i).start()

    pl.semaphore_wait(barrier, 3 + at.row)
    for i in range(3):
        local_w[i].wait()
        far_w[i].start()

    @pl.when(at.row == 1)
    def _():
        signal(answer, at.side)

    for copy in mate_w:
        copy.start()

    @pl.when(at.row == 0)
    def _():
        pl.semaphore_wait(answer, 1)

    loop(0, side_chunks, lambda i: side_chunk(i).start())

    def normalise(ref, i, size):
        def piece(p, carry):
            here = pl.ds(pl.multiple_of(i * size + p * PIECE, PIECE), PIECE)
            x_wide = ref[here, :].astype(jnp.float32)
            mean_sq = jnp.mean(x_wide * x_wide, axis=-1, keepdims=True)
            ref[here, :] = (x_wide * lax.rsqrt(mean_sq + EPSILON) * gain[...].reshape(1, width)).astype(jnp.bfloat16)
            return carry

        lax.fori_loop(0, size // PIECE, piece, 0, unroll=4)

    def product(ref, here, w, block):
        cols = slice(block * head, (block + 1) * head) if isinstance(block, int) else pl.ds(pl.multiple_of(block * head, head), head)
        return jnp.dot(ref[here, :], w[:, cols], preferred_element_type=jnp.float32).astype(jnp.bfloat16)

    def mate_copies(block, i):
        size, sends, recvs = (SIDE_CHUNK, ms_send, ms_recv) if block == SIDE else (CHUNK, mo_send, mo_recv)
        here, there = span(i, size, block * rows), span(i, size, (MATE + block) * rows)
        return (
            send(early.at[KV, here, :], early.at[KV, there, :], sends.at[0, i], recvs.at[0, i], at.mate),
            send(mate_q.at[here, :], early.at[Q, there, :], sends.at[1, i], recvs.at[1, i], at.mate),
        )

    def near_products(ref, block, i):
        size = SIDE_CHUNK if block == SIDE else CHUNK
        here, source = span(i, size, block * rows), span(i, size)
        early[K, here, :] = product(ref, source, w_own, 2)
        early[V, here, :] = product(ref, source, w_own, 3)
        early[Q, here, :] = product(ref, source, w_own, core)
        mate_q[here, :] = product(ref, source, w_own, 1 - core)
        for copy in mate_copies(block, i):
            copy.start()

    far_columns = {K: 2, V: 3, Q_SAME: core, Q_OTHER: 1 - core}

    def far_products(ref, here, stage, kinds):
        for kind in kinds:
            stage[kind, here, :] = product(ref, here, w_far, far_columns[kind])

    def own_messages(i):
        there = span(i, CHUNK, FAR * rows)
        sources = ((KV, KV, there, at.far), (Q_SAME, Q, there, at.far), (Q_OTHER, Q, span(i, CHUNK, FAR_MATE * rows), at.far_mate))
        return [send(far_own.at[src, span(i, CHUNK), :], early.at[dst, to, :], fo_send.at[j, i], fo_recv.at[j, i], peer)
                for j, (src, dst, to, peer) in enumerate(sources)]

    messages = functools.partial(side_messages, at, rows, far_late, late, fs_send, fs_recv)

    def relay(i):
        return send(early.at[KV, span(i, CHUNK, FAR * rows), :], early.at[KV, span(i, CHUNK, FAR_MATE * rows), :], r_send.at[i], r_recv.at[i], at.mate)

    def own_norm(i):
        load_chunk(i).wait()
        normalise(x_own, i, CHUNK)

    gain_copy.wait()
    loop(0, chunks, own_norm)
    for copy in mate_w:
        copy.wait_recv()
    loop(0, chunks, lambda i: near_products(x_own, OWN, i))

    for i in (0, 1):
        far_w[i].wait_recv()
        relay_w[i].start()
    for i in (0, 1):
        relay_w[i].wait_recv()

    def far_kv_step(i):
        far_products(x_own, span(i, CHUNK), far_own, (K, V))
        own_messages(i)[0].start()

    loop(0, chunks, far_kv_step)
    far_w[2].wait_recv()
    relay_w[2].start()
    relay_w[2].wait_recv()

    def far_q_step(i):
        far_products(x_own, span(i, CHUNK), far_own, (Q_SAME, Q_OTHER))
        for message in own_messages(i)[1:]:
            message.start()

    loop(0, chunks, far_q_step)

    def side_step(i):
        side_chunk(i).wait_recv()
        normalise(x_side, i, SIDE_CHUNK)
        near_products(x_side, SIDE, i)
        far_products(x_side, span(i, SIDE_CHUNK), far_late, (Q_OTHER, K, V, Q_SAME))
        done = lax.rem(i + 1, CHUNK // SIDE_CHUNK) == 0
        n = i // (CHUNK // SIDE_CHUNK)

        @pl.when(done & (n < at.first))
        def _():
            messages(n)[1].start()

        @pl.when(done & (n == at.first - 1))
        def _():
            loop(0, at.first, lambda j: messages(j)[0].start())

    loop(0, side_chunks - 1, side_step)

    def relay_step(i):
        own_messages(i)[0].wait_recv()
        relay(i).start()

    loop(0, chunks, relay_step)

    def drain_own(i):
        for copy in mate_copies(OWN, i):
            copy.wait_send()
            copy.wait_recv()
        for j, message in enumerate(own_messages(i)):
            message.wait_send()
            if j:
                message.wait_recv()
        relay(i).wait_send()
        relay(i).wait_recv()

    loop(0, chunks, drain_own)
    for copies in (mate_w, far_w, relay_w):
        for copy in copies:
            copy.wait_send()

    side_step(side_chunks - 1)

    def drain_side(i):
        side_chunk(i).wait_send()
        for copy in mate_copies(SIDE, i):
            copy.wait_send()
            copy.wait_recv()

    def drain_same(i):
        same, other = messages(i)
        same.wait_send()
        same.wait_recv()
        other.wait_send()

    loop(0, side_chunks, drain_side)
    loop(0, at.first_other, lambda i: messages(i)[1].wait_recv())
    loop(0, at.first, drain_same)


def finish(held, far_late, token, late, answer, fs_send, fs_recv, r_send, r_recv):
    rows = far_late.shape[1]
    chunks = rows // CHUNK
    at = Place()
    barrier = pltpu.get_barrier_semaphore()
    signal(barrier, at.far)

    @pl.when(at.core == 0)
    def _():
        signal(barrier, at.mate)
        signal(barrier, at.far_mate)

    pl.semaphore_wait(barrier, 1 + 2 * at.core)
    messages = functools.partial(side_messages, at, rows, far_late, late, fs_send, fs_recv)
    loop(at.first, chunks, lambda i: messages(i)[0].start())

    @pl.when(at.core == 1)
    def _():
        signal(answer, at.mate)
        signal(answer, at.far_mate)

    @pl.when(at.core == 0)
    def _():
        pl.semaphore_wait(answer, 2)

    loop(at.first, chunks, lambda i: messages(i)[1].start())

    def relay(i, source):
        return send(source.at[KV, span(i, CHUNK, LATE_FAR * rows), :], late.at[KV, span(i, CHUNK, LATE_FAR_MATE * rows), :],
                    r_send.at[i], r_recv.at[i], at.mate)

    loop(0, at.first, lambda i: relay(i, held).start())

    def relay_step(i):
        messages(i)[0].wait_recv()
        relay(i, late).start()

    loop(at.first, chunks, relay_step)

    def drain_relay(i):
        relay(i, late).wait_send()
        relay(i, late).wait_recv()

    def drain(i):
        for message in messages(i):
            message.wait_send()

    loop(0, chunks, drain_relay)
    loop(at.first_other, chunks, lambda i: messages(i)[1].wait_recv())
    loop(at.first, chunks, drain)


def store_early(early, q_out, k_out, v_out, token, sems):
    at = Place()
    owners = (at.me, at.side, at.mate, at.across(at.mate), at.far, at.far_mate)
    rows = early.shape[1] // len(owners)
    copies = [
        pltpu.make_async_copy(early.at[o, pl.ds(block * rows, rows), :], out.at[span(owner, rows), :], sems.at[o, block])
        for o, out in enumerate((k_out, v_out, q_out))
        for block, owner in enumerate(owners)
    ]
    for copy in copies:
        copy.start()
    for copy in copies:
        copy.wait()


def store_late(held, late, q_in, k_in, v_in, q_out, k_out, v_out, sems):
    at = Place()
    rows = late.shape[1] // 2
    outs = (k_out, v_out, q_out)

    def copy(o, block, part, source):
        first, count = ((0, CHUNK), (CHUNK, rows - 2 * CHUNK), (rows - CHUNK, CHUNK))[part]
        owner = at.across((at.far, at.far_mate)[block])
        return pltpu.make_async_copy(
            source.at[o, pl.ds(block * rows + first, count), :],
            outs[o].at[pl.ds(pl.multiple_of(owner * rows + first, CHUNK), count), :],
            sems.at[o, block, part],
        )

    for o in range(3):
        for block in range(2):
            relayed = block == LATE_FAR_MATE and o != Q
            copy(o, block, 0, late if relayed else held).start()
            copy(o, block, 2, late).start()
            if relayed:
                copy(o, block, 1, late).start()

    for core in range(2):
        @pl.when(at.core == core)
        def _():
            for o in range(3):
                copy(o, LATE_FAR, 1, held if core else late).start()
            copy(Q, LATE_FAR_MATE, 1, late if core else held).start()

    for o in range(3):
        for block in range(2):
            for part in range(3):
                copy(o, block, part, late).wait()


def in_vmem(*arrays):
    return tuple(pltpu.with_memory_space_constraint(array, pltpu.VMEM) for array in arrays)


def solution(mesh):
    group_size = mesh.shape["tp"]

    def local_step(x_rows, norm_gain, w_q, w_k, w_v):
        rows, width = x_rows.shape
        head = w_q.shape[2]
        chunks = rows // CHUNK
        dma = pltpu.SemaphoreType.DMA
        any_space = pl.BlockSpec(memory_space=pl.ANY)
        vmem = pl.BlockSpec(memory_space=pltpu.VMEM)
        hbm = pl.BlockSpec(memory_space=pltpu.HBM)

        def small(**settings):
            return pltpu.CompilerParams(vmem_limit_bytes=1024 * 1024, **settings)

        early = pltpu.VMEM((3, 6 * rows, head), jnp.bfloat16)
        late = pltpu.VMEM((3, 2 * rows, head), jnp.bfloat16)
        final = [pltpu.HBM((group_size * rows, head), jnp.bfloat16)] * 3
        side_chunks = rows // SIDE_CHUNK

        gathered, held, far_late = in_vmem(*pl.pallas_call(
            gather,
            out_shape=[early, late, pltpu.VMEM((4, rows, head), jnp.bfloat16)],
            in_specs=[any_space] * 5,
            out_specs=[vmem] * 3,
            scratch_shapes=[
                pltpu.VMEM((rows, width), jnp.bfloat16),
                pltpu.VMEM((rows, width), jnp.bfloat16),
                pltpu.VMEM((width, 4 * head), jnp.bfloat16),
                pltpu.VMEM((width, 4 * head), jnp.bfloat16),
                pltpu.VMEM((4, rows, head), jnp.bfloat16),
                pltpu.VMEM((2 * rows, head), jnp.bfloat16),
                pltpu.VMEM((width,), jnp.float32),
                pltpu.SemaphoreType.REGULAR, dma(()), dma((chunks,)),
                dma((3,)), dma((3,)), dma((3,)), dma((3,)), dma((3,)), dma((3,)), dma((3,)),
                dma((side_chunks,)), dma((side_chunks,)), dma((2, chunks)), dma((2, chunks)), dma((2, side_chunks)), dma((2, side_chunks)),
                dma((3, chunks)), dma((3, chunks)), dma((2, chunks)), dma((2, chunks)), dma((chunks,)), dma((chunks,)),
            ],
            compiler_params=pltpu.CompilerParams(collective_id=0, has_side_effects=True, vmem_limit_bytes=40 * 1024 * 1024),
            name="gather",
        )(x_rows, norm_gain, w_q.reshape(width, head), w_k, w_v))
        *stored, token = pl.pallas_call(
            store_early,
            out_shape=final + [pltpu.HBM((8, 128), jnp.float32)],
            in_specs=[vmem],
            out_specs=[hbm] * 4,
            scratch_shapes=[dma((3, 6))],
            compiler_params=small(),
            name="store_early",
        )(gathered)
        finished = pl.pallas_call(
            finish,
            out_shape=late,
            in_specs=[vmem] * 2 + [hbm],
            out_specs=vmem,
            scratch_shapes=[pltpu.SemaphoreType.REGULAR, dma((2, chunks)), dma((2, chunks)), dma((chunks,)), dma((chunks,))],
            compiler_params=small(collective_id=1, has_side_effects=True),
            name="finish",
        )(held, far_late, pltpu.with_memory_space_constraint(token, pltpu.HBM))
        outs = pl.pallas_call(
            store_late,
            out_shape=final,
            in_specs=[vmem] * 2 + [hbm] * 3,
            out_specs=[hbm] * 3,
            input_output_aliases={2: 0, 3: 1, 4: 2},
            scratch_shapes=[dma((3, 2, 3))],
            compiler_params=small(),
            name="store_late",
        )(held, *in_vmem(finished), *stored)
        return tuple(out[:, None, :] for out in outs)

    return jax.shard_map(local_step, mesh=mesh, in_specs=(P(("dp", "tp"), None), P(None), P(None, "tp", None), P(None, "tp"), P(None, "tp")), out_specs=(P("dp", "tp", None), P("dp", "tp", None), P("dp", "tp", None)), check_vma=False)
```

```python
import functools

import jax
import jax.numpy as jnp
from jax import lax
from jax.experimental import pallas as pl
from jax.experimental.pallas import tpu as pltpu
from jax.sharding import PartitionSpec as P

EPSILON = 1e-6
CHUNK = 256
SIDE_CHUNK = 128
PIECE = 16

K, V, Q = range(3)
KV, KVQ = pl.ds(0, 2), pl.ds(0, 3)
Q_SAME, Q_OTHER = 2, 3
OWN, SIDE, MATE, MATE_SIDE, FAR, FAR_MATE = range(6)
LATE_FAR, LATE_FAR_MATE = range(2)


class Place:
    def __init__(self):
        self.me = lax.axis_index("tp")
        self.core = lax.rem(self.me, 2)
        self.row = self.me // 4
        self.mate = self.me + 1 - 2 * self.core
        self.side = self.across(self.me)
        self.far = self.me + 2 - 4 * lax.rem(self.me // 2, 2)
        self.far_mate = self.far + 1 - 2 * self.core
        self.first = 1 + 2 * self.core
        self.first_other = 3 - 2 * self.core

    def across(self, device):
        return device + 4 - 8 * (device // 4)


def send(src, dst, send_sem, recv_sem, to):
    return pltpu.make_async_remote_copy(src_ref=src, dst_ref=dst, send_sem=send_sem, recv_sem=recv_sem, device_id={"tp": to})


def signal(sem, to):
    pl.semaphore_signal(sem, inc=1, device_id={"tp": to})


def loop(start, stop, body):
    def step(i, carry):
        body(i)
        return carry

    lax.fori_loop(start, stop, step, 0)


def span(i, size, base=0):
    return pl.ds(pl.multiple_of(base + i * size, size), size)


SAME, OTHER = range(2)


def side_message(at, rows, stage, target, send_sems, recv_sems, kind, i):
    src, dst, block, peer = ((KVQ, KVQ, LATE_FAR, at.far), (Q_OTHER, Q, LATE_FAR_MATE, at.far_mate))[kind]
    return send(stage.at[src, span(i, CHUNK), :], target.at[dst, span(i, CHUNK, block * rows), :], send_sems.at[kind, i], recv_sems.at[kind, i], peer)


def late_relay(at, rows, source, target, send_sems, recv_sems, i):
    return send(source.at[KV, span(i, CHUNK, LATE_FAR * rows), :], target.at[KV, span(i, CHUNK, LATE_FAR_MATE * rows), :],
                send_sems.at[i], recv_sems.at[i], at.mate)


def gather(x_hbm, gain_hbm, wq_hbm, wk_hbm, wv_hbm, early, late, far_late,
           x_own, x_side, w_own, w_far, far_own, mate_q, gain,
           mate_answer, side_answer, far_answer, load_gain, load_x, load_w, mw_send, mw_recv, fw_send, fw_recv, rw_send, rw_recv,
           x_send, x_recv, mo_send, mo_recv, ms_send, ms_recv, fo_send, fo_recv, fs_send, fs_recv, r_send, r_recv, lr_send, lr_recv):
    rows, width = x_hbm.shape
    head = wq_hbm.shape[1]
    part = wk_hbm.shape[1]
    chunks = rows // CHUNK
    side_chunks = rows // SIDE_CHUNK
    at = Place()
    core = at.core

    barrier = pltpu.get_barrier_semaphore()
    signal(barrier, at.far)

    @pl.when(core == 1)
    def _():
        signal(barrier, at.mate)

    @pl.when(at.row == 0)
    def _():
        signal(barrier, at.side)

    q_cols = pl.ds(pl.multiple_of(core * head, head), head)
    k_cols = pl.ds(pl.multiple_of(2 * head + core * part, part), part)
    v_cols = pl.ds(pl.multiple_of(3 * head + core * part, part), part)
    mine = ((wk_hbm, k_cols), (wv_hbm, v_cols), (wq_hbm, q_cols))
    local_w = [pltpu.make_async_copy(src, w_own.at[:, cols], load_w.at[i]) for i, (src, cols) in enumerate(mine)]
    mate_w = [send(w_own.at[:, cols], w_own.at[:, cols], mw_send.at[i], mw_recv.at[i], at.mate) for i, (src, cols) in enumerate(mine)]
    far_w = [send(w_own.at[:, cols], w_far.at[:, cols], fw_send.at[i], fw_recv.at[i], at.far) for i, (src, cols) in enumerate(mine)]
    relay_w = [send(w_far.at[:, cols], w_far.at[:, cols], rw_send.at[i], rw_recv.at[i], at.mate) for i, (src, cols) in enumerate(mine)]

    def load_chunk(i):
        return pltpu.make_async_copy(x_hbm.at[span(i, CHUNK), :], x_own.at[span(i, CHUNK), :], load_x.at[i])

    def side_chunk(i):
        return send(x_hbm.at[span(i, SIDE_CHUNK), :], x_side.at[span(i, SIDE_CHUNK), :], x_send.at[i], x_recv.at[i], at.side)

    for copy in local_w:
        copy.start()
    gain_copy = pltpu.make_async_copy(gain_hbm, gain, load_gain)
    gain_copy.start()
    for i in range(chunks):
        load_chunk(i).start()

    pl.semaphore_wait(barrier, 2 - core + at.row)
    for i in range(3):
        local_w[i].wait()
        far_w[i].start()

    @pl.when(core == 0)
    def _():
        signal(mate_answer, at.mate)

    @pl.when(at.row == 1)
    def _():
        signal(side_answer, at.side)

    @pl.when(core == 1)
    def _():
        pl.semaphore_wait(mate_answer, 1)

    signal(far_answer, at.far)
    for copy in mate_w:
        copy.start()

    @pl.when(at.row == 0)
    def _():
        pl.semaphore_wait(side_answer, 1)

    loop(0, side_chunks, lambda i: side_chunk(i).start())

    def normalise(ref, i, size):
        def piece(p, carry):
            here = pl.ds(pl.multiple_of(i * size + p * PIECE, PIECE), PIECE)
            x_wide = ref[here, :].astype(jnp.float32)
            mean_sq = jnp.mean(x_wide * x_wide, axis=-1, keepdims=True)
            ref[here, :] = (x_wide * lax.rsqrt(mean_sq + EPSILON) * gain[...].reshape(1, width)).astype(jnp.bfloat16)
            return carry

        lax.fori_loop(0, size // PIECE, piece, 0, unroll=4)

    def product(ref, here, w, block):
        cols = slice(block * head, (block + 1) * head) if isinstance(block, int) else pl.ds(pl.multiple_of(block * head, head), head)
        return jnp.dot(ref[here, :], w[:, cols], preferred_element_type=jnp.float32).astype(jnp.bfloat16)

    def mate_copies(block, i):
        size, sends, recvs = (SIDE_CHUNK, ms_send, ms_recv) if block == SIDE else (CHUNK, mo_send, mo_recv)
        here, there = span(i, size, block * rows), span(i, size, (MATE + block) * rows)
        return (
            send(early.at[KV, here, :], early.at[KV, there, :], sends.at[0, i], recvs.at[0, i], at.mate),
            send(mate_q.at[here, :], early.at[Q, there, :], sends.at[1, i], recvs.at[1, i], at.mate),
        )

    def near_products(ref, block, i):
        size = SIDE_CHUNK if block == SIDE else CHUNK
        here, source = span(i, size, block * rows), span(i, size)
        early[K, here, :] = product(ref, source, w_own, 2)
        early[V, here, :] = product(ref, source, w_own, 3)
        early[Q, here, :] = product(ref, source, w_own, core)
        mate_q[here, :] = product(ref, source, w_own, 1 - core)
        for copy in mate_copies(block, i):
            copy.start()

    far_columns = {K: 2, V: 3, Q_SAME: core, Q_OTHER: 1 - core}

    def far_products(ref, here, stage, kinds):
        for kind in kinds:
            stage[kind, here, :] = product(ref, here, w_far, far_columns[kind])

    def own_message(j, i):
        src, dst, block, peer = ((KV, KV, FAR, at.far), (Q_SAME, Q, FAR, at.far), (Q_OTHER, Q, FAR_MATE, at.far_mate))[j]
        return send(far_own.at[src, span(i, CHUNK), :], early.at[dst, span(i, CHUNK, block * rows), :], fo_send.at[j, i], fo_recv.at[j, i], peer)

    message = functools.partial(side_message, at, rows, far_late, late, fs_send, fs_recv)

    def relay(i):
        return send(early.at[KV, span(i, CHUNK, FAR * rows), :], early.at[KV, span(i, CHUNK, FAR_MATE * rows), :], r_send.at[i], r_recv.at[i], at.mate)

    def own_norm(i):
        load_chunk(i).wait()
        normalise(x_own, i, CHUNK)

    gain_copy.wait()
    loop(0, chunks, own_norm)
    for copy in mate_w:
        copy.wait_recv()
    loop(0, chunks, lambda i: near_products(x_own, OWN, i))

    for i in (0, 1):
        far_w[i].wait_recv()
        relay_w[i].start()
    for i in (0, 1):
        relay_w[i].wait_recv()

    def far_kv_step(i):
        far_products(x_own, span(i, CHUNK), far_own, (K, V))
        own_message(0, i).start()

    loop(0, chunks, far_kv_step)
    far_w[2].wait_recv()
    relay_w[2].start()
    relay_w[2].wait_recv()
    pl.semaphore_wait(far_answer, 1)

    def far_q_step(i):
        far_products(x_own, span(i, CHUNK), far_own, (Q_SAME, Q_OTHER))
        own_message(1, i).start()
        own_message(2, i).start()

    loop(0, chunks, far_q_step)

    def side_step(i):
        side_chunk(i).wait_recv()
        normalise(x_side, i, SIDE_CHUNK)
        near_products(x_side, SIDE, i)
        far_products(x_side, span(i, SIDE_CHUNK), far_late, (Q_OTHER, K, V, Q_SAME))
        done = lax.rem(i + 1, CHUNK // SIDE_CHUNK) == 0
        n = i // (CHUNK // SIDE_CHUNK)

        @pl.when(done & (n < at.first))
        def _():
            message(OTHER, n).start()

        @pl.when(done & (n == at.first - 1))
        def _():
            loop(0, at.first, lambda j: message(SAME, j).start())

    loop(0, side_chunks - 1, side_step)

    def relay_step(i):
        own_message(0, i).wait_recv()
        relay(i).start()

    loop(0, chunks, relay_step)

    def drain_own(i):
        for copy in mate_copies(OWN, i):
            copy.wait_send()
            copy.wait_recv()
        for j in range(3):
            own_message(j, i).wait_send()
        for j in (1, 2):
            own_message(j, i).wait_recv()
        relay(i).wait_send()
        relay(i).wait_recv()

    loop(0, chunks, drain_own)
    for copies in (mate_w, far_w, relay_w):
        for copy in copies:
            copy.wait_send()

    side_step(side_chunks - 1)

    def drain_side(i):
        side_chunk(i).wait_send()
        for copy in mate_copies(SIDE, i):
            copy.wait_send()
            copy.wait_recv()

    def drain_same(i):
        message(SAME, i).wait_send()
        message(SAME, i).wait_recv()
        message(OTHER, i).wait_send()

    loop(0, side_chunks, drain_side)
    loop(0, at.first_other, lambda i: message(OTHER, i).wait_recv())
    loop(0, at.first, drain_same)

    first_relay = late_relay(at, rows, late, late, lr_send, lr_recv, 0)

    @pl.when(core == 0)
    def _():
        first_relay.start()
        first_relay.wait_send()

    @pl.when(core == 1)
    def _():
        first_relay.wait_recv()


def finish(held, far_late, token, late, answer, fs_send, fs_recv, r_send, r_recv):
    rows = far_late.shape[1]
    chunks = rows // CHUNK
    at = Place()
    barrier = pltpu.get_barrier_semaphore()
    signal(barrier, at.far)

    @pl.when(at.core == 0)
    def _():
        signal(barrier, at.mate)
        signal(barrier, at.far_mate)

    pl.semaphore_wait(barrier, 1 + 2 * at.core)
    message = functools.partial(side_message, at, rows, far_late, late, fs_send, fs_recv)
    loop(at.first, chunks, lambda i: message(SAME, i).start())

    @pl.when(at.core == 1)
    def _():
        signal(answer, at.mate)
        signal(answer, at.far_mate)

    @pl.when(at.core == 0)
    def _():
        pl.semaphore_wait(answer, 2)

    loop(at.first, chunks, lambda i: message(OTHER, i).start())

    def relay(i, source=late):
        return late_relay(at, rows, source, late, r_send, r_recv, i)

    loop(1 - at.core, at.first, lambda i: relay(i, held).start())

    def relay_step(i):
        message(SAME, i).wait_recv()
        relay(i).start()

    loop(at.first, chunks, relay_step)
    loop(at.core, chunks, lambda i: relay(i).wait_recv())
    loop(1 - at.core, chunks, lambda i: relay(i).wait_send())
    loop(at.first_other, chunks, lambda i: message(OTHER, i).wait_recv())

    def drain(i):
        message(SAME, i).wait_send()
        message(OTHER, i).wait_send()

    loop(at.first, chunks, drain)


def late_chunks(core, held):
    first, other, relayed = (1, 3, 0) if core == 0 else (3, 1, 1)
    spans = [(o, LATE_FAR, first) for o in (K, V, Q)] + [(Q, LATE_FAR_MATE, other)] + [(o, LATE_FAR_MATE, relayed) for o in (K, V)]
    return [(o, block, 0, n) if held else (o, block, n, None) for o, block, n in spans]


def store_chunks(at, source, outs, sems, core, held):
    rows = source.shape[1] // 2
    owners = tuple(at.across(device) for device in (at.far, at.far_mate))
    copies = []
    for j, (o, block, start, count) in enumerate(late_chunks(core, held)):
        count = (rows // CHUNK - start if count is None else count) * CHUNK
        if count:
            copies.append(pltpu.make_async_copy(
                source.at[o, pl.ds(block * rows + start * CHUNK, count), :],
                outs[o].at[pl.ds(pl.multiple_of(owners[block] * rows + start * CHUNK, CHUNK), count), :],
                sems.at[j],
            ))
    return copies


def run(copies):
    for copy in copies:
        copy.start()
    for copy in copies:
        copy.wait()


def store_early(early, held, q_out, k_out, v_out, token, sems, held_sems):
    at = Place()
    owners = (at.me, at.side, at.mate, at.across(at.mate), at.far, at.far_mate)
    rows = early.shape[1] // len(owners)
    outs = (k_out, v_out, q_out)
    for core in range(2):
        @pl.when(at.core == core)
        def _():
            run([
                pltpu.make_async_copy(early.at[o, pl.ds(block * rows, rows), :], out.at[span(owner, rows), :], sems.at[o, block])
                for o, out in enumerate(outs)
                for block, owner in enumerate(owners)
            ] + store_chunks(at, held, outs, held_sems, core, True))


def store_late(late, q_in, k_in, v_in, q_out, k_out, v_out, sems):
    at = Place()
    for core in range(2):
        @pl.when(at.core == core)
        def _():
            run(store_chunks(at, late, (k_out, v_out, q_out), sems, core, False))


def in_vmem(*arrays):
    return tuple(pltpu.with_memory_space_constraint(array, pltpu.VMEM) for array in arrays)


def solution(mesh):
    group_size = mesh.shape["tp"]

    def local_step(x_rows, norm_gain, w_q, w_k, w_v):
        rows, width = x_rows.shape
        head = w_q.shape[2]
        chunks = rows // CHUNK
        dma = pltpu.SemaphoreType.DMA
        any_space = pl.BlockSpec(memory_space=pl.ANY)
        vmem = pl.BlockSpec(memory_space=pltpu.VMEM)
        hbm = pl.BlockSpec(memory_space=pltpu.HBM)

        def small(**settings):
            return pltpu.CompilerParams(vmem_limit_bytes=1024 * 1024, **settings)

        early = pltpu.VMEM((3, 6 * rows, head), jnp.bfloat16)
        late = pltpu.VMEM((3, 2 * rows, head), jnp.bfloat16)
        final = [pltpu.HBM((group_size * rows, head), jnp.bfloat16)] * 3
        side_chunks = rows // SIDE_CHUNK

        gathered, held, far_late = in_vmem(*pl.pallas_call(
            gather,
            out_shape=[early, late, pltpu.VMEM((4, rows, head), jnp.bfloat16)],
            in_specs=[any_space] * 5,
            out_specs=[vmem] * 3,
            scratch_shapes=[
                pltpu.VMEM((rows, width), jnp.bfloat16),
                pltpu.VMEM((rows, width), jnp.bfloat16),
                pltpu.VMEM((width, 4 * head), jnp.bfloat16),
                pltpu.VMEM((width, 4 * head), jnp.bfloat16),
                pltpu.VMEM((4, rows, head), jnp.bfloat16),
                pltpu.VMEM((2 * rows, head), jnp.bfloat16),
                pltpu.VMEM((width,), jnp.float32),
                *[pltpu.SemaphoreType.REGULAR] * 3, dma(()), dma((chunks,)),
                dma((3,)), dma((3,)), dma((3,)), dma((3,)), dma((3,)), dma((3,)), dma((3,)),
                dma((side_chunks,)), dma((side_chunks,)), dma((2, chunks)), dma((2, chunks)), dma((2, side_chunks)), dma((2, side_chunks)),
                dma((3, chunks)), dma((3, chunks)), dma((2, chunks)), dma((2, chunks)), dma((chunks,)), dma((chunks,)), dma((1,)), dma((1,)),
            ],
            compiler_params=pltpu.CompilerParams(collective_id=0, has_side_effects=True, vmem_limit_bytes=40 * 1024 * 1024),
            name="gather",
        )(x_rows, norm_gain, w_q.reshape(width, head), w_k, w_v))
        *stored, token = pl.pallas_call(
            store_early,
            out_shape=final + [pltpu.HBM((8, 128), jnp.float32)],
            in_specs=[vmem] * 2,
            out_specs=[hbm] * 4,
            scratch_shapes=[dma((3, 6)), dma((6,))],
            compiler_params=small(),
            name="store_early",
        )(gathered, held)
        finished = pl.pallas_call(
            finish,
            out_shape=late,
            in_specs=[vmem] * 2 + [hbm],
            out_specs=vmem,
            scratch_shapes=[pltpu.SemaphoreType.REGULAR, dma((2, chunks)), dma((2, chunks)), dma((chunks,)), dma((chunks,))],
            compiler_params=small(collective_id=1, has_side_effects=True),
            name="finish",
        )(held, far_late, pltpu.with_memory_space_constraint(token, pltpu.HBM))
        outs = pl.pallas_call(
            store_late,
            out_shape=final,
            in_specs=[vmem] + [hbm] * 3,
            out_specs=[hbm] * 3,
            input_output_aliases={1: 0, 2: 1, 3: 2},
            scratch_shapes=[dma((6,))],
            compiler_params=small(),
            name="store_late",
        )(*in_vmem(finished), *stored)
        return tuple(out[:, None, :] for out in outs)

    return jax.shard_map(local_step, mesh=mesh, in_specs=(P(("dp", "tp"), None), P(None), P(None, "tp", None), P(None, "tp"), P(None, "tp")), out_specs=(P("dp", "tp", None), P("dp", "tp", None), P("dp", "tp", None)), check_vma=False)
```

```python
import functools

import jax
import jax.numpy as jnp
from jax import lax
from jax.experimental import pallas as pl
from jax.experimental.pallas import tpu as pltpu
from jax.sharding import PartitionSpec as P

EPSILON = 1e-6
CHUNK = 256
SIDE_CHUNK = 128
PIECE = 16

K, V, Q = range(3)
KV, KVQ = pl.ds(0, 2), pl.ds(0, 3)
Q_SAME, Q_OTHER = 2, 3
OWN, SIDE, MATE, MATE_SIDE, FAR, FAR_MATE = range(6)
LATE_FAR, LATE_FAR_MATE = range(2)


class Place:
    def __init__(self):
        self.me = lax.axis_index("tp")
        self.core = lax.rem(self.me, 2)
        self.row = self.me // 4
        self.mate = self.me + 1 - 2 * self.core
        self.side = self.across(self.me)
        self.far = self.me + 2 - 4 * lax.rem(self.me // 2, 2)
        self.far_mate = self.far + 1 - 2 * self.core
        self.first = 1 + 2 * self.core
        self.first_other = 3 - 2 * self.core

    def across(self, device):
        return device + 4 - 8 * (device // 4)


def send(src, dst, send_sem, recv_sem, to):
    return pltpu.make_async_remote_copy(src_ref=src, dst_ref=dst, send_sem=send_sem, recv_sem=recv_sem, device_id={"tp": to})


def signal(sem, to):
    pl.semaphore_signal(sem, inc=1, device_id={"tp": to})


def loop(start, stop, body):
    def step(i, carry):
        body(i)
        return carry

    lax.fori_loop(start, stop, step, 0)


def span(i, size, base=0):
    return pl.ds(pl.multiple_of(base + i * size, size), size)


SAME, OTHER = range(2)


def side_message(at, rows, stage, target, send_sems, recv_sems, kind, i):
    src, dst, block, peer = ((KVQ, KVQ, LATE_FAR, at.far), (Q_OTHER, Q, LATE_FAR_MATE, at.far_mate))[kind]
    return send(stage.at[src, span(i, CHUNK), :], target.at[dst, span(i, CHUNK, block * rows), :], send_sems.at[kind, i], recv_sems.at[kind, i], peer)


def late_relay(at, rows, source, target, send_sems, recv_sems, i):
    return send(source.at[KV, span(i, CHUNK, LATE_FAR * rows), :], target.at[KV, span(i, CHUNK, LATE_FAR_MATE * rows), :],
                send_sems.at[i], recv_sems.at[i], at.mate)


def gather(x_hbm, gain_hbm, wq_hbm, wk_hbm, wv_hbm, early, late, far_late,
           x_own, x_side, w_own, w_far, far_own, mate_q, gain,
           mate_answer, side_answer, far_answer, load_gain, load_x, lw_sem, mw_send, mw_recv, fw_send, fw_recv, rw_send, rw_recv,
           x_send, x_recv, mo_send, mo_recv, ms_send, ms_recv, fo_send, fo_recv, fs_send, fs_recv, r_send, r_recv, lr_send, lr_recv):
    rows, width = x_hbm.shape
    head = wq_hbm.shape[1]
    part = wk_hbm.shape[1]
    chunks = rows // CHUNK
    side_chunks = rows // SIDE_CHUNK
    at = Place()
    core = at.core

    barrier = pltpu.get_barrier_semaphore()
    signal(barrier, at.far)

    @pl.when(core == 1)
    def _():
        signal(barrier, at.mate)

    @pl.when(at.row == 0)
    def _():
        signal(barrier, at.side)

    q_cols = pl.ds(pl.multiple_of(core * head, head), head)
    k_cols = pl.ds(pl.multiple_of(2 * head + core * part, part), part)
    v_cols = pl.ds(pl.multiple_of(3 * head + core * part, part), part)
    lead = width // 4
    mine = (
        (wk_hbm, pl.ds(0, lead), k_cols),
        (wk_hbm, pl.ds(lead, width - lead), k_cols),
        (wv_hbm, pl.ds(0, width), v_cols),
        (wq_hbm, pl.ds(0, width), q_cols),
    )
    load_w, mate_w, far_w, relay_w = [], [], [], []
    for i, (src, depth, cols) in enumerate(mine):
        near_part, far_part = w_own.at[depth, cols], w_far.at[depth, cols]
        load_w.append(pltpu.make_async_copy(src.at[depth, :], near_part, lw_sem.at[i]))
        mate_w.append(send(near_part, near_part, mw_send.at[i], mw_recv.at[i], at.mate))
        far_w.append(send(near_part, far_part, fw_send.at[i], fw_recv.at[i], at.far))
        relay_w.append(send(far_part, far_part, rw_send.at[i], rw_recv.at[i], at.mate))

    def load_chunk(i):
        return pltpu.make_async_copy(x_hbm.at[span(i, CHUNK), :], x_own.at[span(i, CHUNK), :], load_x.at[i])

    def side_chunk(i):
        return send(x_hbm.at[span(i, SIDE_CHUNK), :], x_side.at[span(i, SIDE_CHUNK), :], x_send.at[i], x_recv.at[i], at.side)

    for copy in load_w:
        copy.start()

    pl.semaphore_wait(barrier, 2 - core + at.row)
    for load, copy in zip(load_w, far_w):
        load.wait()
        copy.start()

    gain_copy = pltpu.make_async_copy(gain_hbm, gain, load_gain)
    gain_copy.start()
    for i in range(chunks):
        load_chunk(i).start()

    @pl.when(core == 0)
    def _():
        signal(mate_answer, at.mate)

    @pl.when(at.row == 1)
    def _():
        signal(side_answer, at.side)

    @pl.when(core == 1)
    def _():
        pl.semaphore_wait(mate_answer, 1)

    signal(far_answer, at.far)
    for copy in mate_w:
        copy.start()

    @pl.when(at.row == 0)
    def _():
        pl.semaphore_wait(side_answer, 1)

    loop(0, side_chunks, lambda i: side_chunk(i).start())

    def normalise(ref, i, size):
        def piece(p, carry):
            here = pl.ds(pl.multiple_of(i * size + p * PIECE, PIECE), PIECE)
            x_wide = ref[here, :].astype(jnp.float32)
            mean_sq = jnp.mean(x_wide * x_wide, axis=-1, keepdims=True)
            ref[here, :] = (x_wide * lax.rsqrt(mean_sq + EPSILON) * gain[...].reshape(1, width)).astype(jnp.bfloat16)
            return carry

        lax.fori_loop(0, size // PIECE, piece, 0, unroll=4)

    def product(ref, here, w, block):
        cols = slice(block * head, (block + 1) * head) if isinstance(block, int) else pl.ds(pl.multiple_of(block * head, head), head)
        return jnp.dot(ref[here, :], w[:, cols], preferred_element_type=jnp.float32).astype(jnp.bfloat16)

    def mate_copies(block, i):
        size, sends, recvs = (SIDE_CHUNK, ms_send, ms_recv) if block == SIDE else (CHUNK, mo_send, mo_recv)
        here, there = span(i, size, block * rows), span(i, size, (MATE + block) * rows)
        return (
            send(early.at[KV, here, :], early.at[KV, there, :], sends.at[0, i], recvs.at[0, i], at.mate),
            send(mate_q.at[here, :], early.at[Q, there, :], sends.at[1, i], recvs.at[1, i], at.mate),
        )

    def near_products(ref, block, i):
        size = SIDE_CHUNK if block == SIDE else CHUNK
        here, source = span(i, size, block * rows), span(i, size)
        early[K, here, :] = product(ref, source, w_own, 2)
        early[V, here, :] = product(ref, source, w_own, 3)
        early[Q, here, :] = product(ref, source, w_own, core)
        mate_q[here, :] = product(ref, source, w_own, 1 - core)
        for copy in mate_copies(block, i):
            copy.start()

    far_columns = {K: 2, V: 3, Q_SAME: core, Q_OTHER: 1 - core}

    def far_products(ref, here, stage, kinds):
        for kind in kinds:
            stage[kind, here, :] = product(ref, here, w_far, far_columns[kind])

    def own_message(j, i):
        src, dst, block, peer = ((KV, KV, FAR, at.far), (Q_SAME, Q, FAR, at.far), (Q_OTHER, Q, FAR_MATE, at.far_mate))[j]
        return send(far_own.at[src, span(i, CHUNK), :], early.at[dst, span(i, CHUNK, block * rows), :], fo_send.at[j, i], fo_recv.at[j, i], peer)

    message = functools.partial(side_message, at, rows, far_late, late, fs_send, fs_recv)

    def relay(i):
        return send(early.at[KV, span(i, CHUNK, FAR * rows), :], early.at[KV, span(i, CHUNK, FAR_MATE * rows), :], r_send.at[i], r_recv.at[i], at.mate)

    def own_norm(i):
        load_chunk(i).wait()
        normalise(x_own, i, CHUNK)

    gain_copy.wait()
    loop(0, chunks, own_norm)
    for copy in mate_w:
        copy.wait_recv()
    loop(0, chunks, lambda i: near_products(x_own, OWN, i))

    for arrived, onward in zip(far_w[:3], relay_w[:3]):
        arrived.wait_recv()
        onward.start()
    for copy in relay_w[:3]:
        copy.wait_recv()

    def far_kv_step(i):
        far_products(x_own, span(i, CHUNK), far_own, (K, V))
        own_message(0, i).start()

    loop(0, chunks, far_kv_step)
    far_w[3].wait_recv()
    relay_w[3].start()
    relay_w[3].wait_recv()
    pl.semaphore_wait(far_answer, 1)

    def far_q_step(i):
        far_products(x_own, span(i, CHUNK), far_own, (Q_SAME, Q_OTHER))
        own_message(1, i).start()
        own_message(2, i).start()

    loop(0, chunks, far_q_step)

    def side_step(i):
        side_chunk(i).wait_recv()
        normalise(x_side, i, SIDE_CHUNK)
        near_products(x_side, SIDE, i)
        far_products(x_side, span(i, SIDE_CHUNK), far_late, (Q_OTHER, K, V, Q_SAME))
        done = lax.rem(i + 1, CHUNK // SIDE_CHUNK) == 0
        n = i // (CHUNK // SIDE_CHUNK)

        @pl.when(done & (n < at.first))
        def _():
            message(OTHER, n).start()

        @pl.when(done & (n == at.first - 1))
        def _():
            loop(0, at.first, lambda j: message(SAME, j).start())

    loop(0, side_chunks - 1, side_step)

    def relay_step(i):
        own_message(0, i).wait_recv()
        relay(i).start()

    loop(0, chunks, relay_step)

    def drain_own(i):
        for copy in mate_copies(OWN, i):
            copy.wait_send()
            copy.wait_recv()
        for j in range(3):
            own_message(j, i).wait_send()
        for j in (1, 2):
            own_message(j, i).wait_recv()
        relay(i).wait_send()
        relay(i).wait_recv()

    loop(0, chunks, drain_own)
    for copies in (mate_w, far_w, relay_w):
        for copy in copies:
            copy.wait_send()

    side_step(side_chunks - 1)

    def drain_side(i):
        side_chunk(i).wait_send()
        for copy in mate_copies(SIDE, i):
            copy.wait_send()
            copy.wait_recv()

    def drain_same(i):
        message(SAME, i).wait_send()
        message(SAME, i).wait_recv()
        message(OTHER, i).wait_send()

    loop(0, side_chunks, drain_side)
    loop(0, at.first_other, lambda i: message(OTHER, i).wait_recv())
    loop(0, at.first, drain_same)

    first_relay = late_relay(at, rows, late, late, lr_send, lr_recv, 0)

    @pl.when(core == 0)
    def _():
        first_relay.start()
        first_relay.wait_send()

    @pl.when(core == 1)
    def _():
        first_relay.wait_recv()


def finish(held, far_late, token, late, answer, fs_send, fs_recv, r_send, r_recv):
    rows = far_late.shape[1]
    chunks = rows // CHUNK
    at = Place()
    barrier = pltpu.get_barrier_semaphore()
    signal(barrier, at.far)

    @pl.when(at.core == 0)
    def _():
        signal(barrier, at.mate)
        signal(barrier, at.far_mate)

    pl.semaphore_wait(barrier, 1 + 2 * at.core)
    message = functools.partial(side_message, at, rows, far_late, late, fs_send, fs_recv)
    loop(at.first, chunks, lambda i: message(SAME, i).start())

    @pl.when(at.core == 1)
    def _():
        signal(answer, at.mate)
        signal(answer, at.far_mate)

    @pl.when(at.core == 0)
    def _():
        pl.semaphore_wait(answer, 2)

    loop(at.first, chunks, lambda i: message(OTHER, i).start())

    def relay(i, source=late):
        return late_relay(at, rows, source, late, r_send, r_recv, i)

    loop(1 - at.core, at.first, lambda i: relay(i, held).start())

    def relay_step(i):
        message(SAME, i).wait_recv()
        relay(i).start()

    loop(at.first, chunks, relay_step)
    loop(at.core, chunks, lambda i: relay(i).wait_recv())
    loop(1 - at.core, chunks, lambda i: relay(i).wait_send())
    loop(at.first_other, chunks, lambda i: message(OTHER, i).wait_recv())

    def drain(i):
        message(SAME, i).wait_send()
        message(OTHER, i).wait_send()

    loop(at.first, chunks, drain)


def late_chunks(core, held):
    first, other, relayed = (1, 3, 0) if core == 0 else (3, 1, 1)
    spans = [(o, LATE_FAR, first) for o in (K, V, Q)] + [(Q, LATE_FAR_MATE, other)] + [(o, LATE_FAR_MATE, relayed) for o in (K, V)]
    return [(o, block, 0, n) if held else (o, block, n, None) for o, block, n in spans]


def store_chunks(at, source, outs, sems, core, held):
    rows = source.shape[1] // 2
    owners = tuple(at.across(device) for device in (at.far, at.far_mate))
    copies = []
    for j, (o, block, start, count) in enumerate(late_chunks(core, held)):
        count = (rows // CHUNK - start if count is None else count) * CHUNK
        if count:
            copies.append(pltpu.make_async_copy(
                source.at[o, pl.ds(block * rows + start * CHUNK, count), :],
                outs[o].at[pl.ds(pl.multiple_of(owners[block] * rows + start * CHUNK, CHUNK), count), :],
                sems.at[j],
            ))
    return copies


def run(copies):
    for copy in copies:
        copy.start()
    for copy in copies:
        copy.wait()


def store_early(early, held, q_out, k_out, v_out, token, sems, held_sems):
    at = Place()
    owners = (at.me, at.side, at.mate, at.across(at.mate), at.far, at.far_mate)
    rows = early.shape[1] // len(owners)
    outs = (k_out, v_out, q_out)
    for core in range(2):
        @pl.when(at.core == core)
        def _():
            run([
                pltpu.make_async_copy(early.at[o, pl.ds(block * rows, rows), :], out.at[span(owner, rows), :], sems.at[o, block])
                for o, out in enumerate(outs)
                for block, owner in enumerate(owners)
            ] + store_chunks(at, held, outs, held_sems, core, True))


def store_late(late, q_in, k_in, v_in, q_out, k_out, v_out, sems):
    at = Place()
    for core in range(2):
        @pl.when(at.core == core)
        def _():
            run(store_chunks(at, late, (k_out, v_out, q_out), sems, core, False))


def in_vmem(*arrays):
    return tuple(pltpu.with_memory_space_constraint(array, pltpu.VMEM) for array in arrays)


def solution(mesh):
    group_size = mesh.shape["tp"]

    def local_step(x_rows, norm_gain, w_q, w_k, w_v):
        rows, width = x_rows.shape
        head = w_q.shape[2]
        chunks = rows // CHUNK
        dma = pltpu.SemaphoreType.DMA
        any_space = pl.BlockSpec(memory_space=pl.ANY)
        vmem = pl.BlockSpec(memory_space=pltpu.VMEM)
        hbm = pl.BlockSpec(memory_space=pltpu.HBM)

        def small(**settings):
            return pltpu.CompilerParams(vmem_limit_bytes=1024 * 1024, **settings)

        early = pltpu.VMEM((3, 6 * rows, head), jnp.bfloat16)
        late = pltpu.VMEM((3, 2 * rows, head), jnp.bfloat16)
        final = [pltpu.HBM((group_size * rows, head), jnp.bfloat16)] * 3
        side_chunks = rows // SIDE_CHUNK

        gathered, held, far_late = in_vmem(*pl.pallas_call(
            gather,
            out_shape=[early, late, pltpu.VMEM((4, rows, head), jnp.bfloat16)],
            in_specs=[any_space] * 5,
            out_specs=[vmem] * 3,
            scratch_shapes=[
                pltpu.VMEM((rows, width), jnp.bfloat16),
                pltpu.VMEM((rows, width), jnp.bfloat16),
                pltpu.VMEM((width, 4 * head), jnp.bfloat16),
                pltpu.VMEM((width, 4 * head), jnp.bfloat16),
                pltpu.VMEM((4, rows, head), jnp.bfloat16),
                pltpu.VMEM((2 * rows, head), jnp.bfloat16),
                pltpu.VMEM((width,), jnp.float32),
                *[pltpu.SemaphoreType.REGULAR] * 3, dma(()), dma((chunks,)),
                *[dma((4,))] * 7,
                dma((side_chunks,)), dma((side_chunks,)), dma((2, chunks)), dma((2, chunks)), dma((2, side_chunks)), dma((2, side_chunks)),
                dma((3, chunks)), dma((3, chunks)), dma((2, chunks)), dma((2, chunks)), dma((chunks,)), dma((chunks,)), dma((1,)), dma((1,)),
            ],
            compiler_params=pltpu.CompilerParams(collective_id=0, has_side_effects=True, vmem_limit_bytes=40 * 1024 * 1024),
            name="gather",
        )(x_rows, norm_gain, w_q.reshape(width, head), w_k, w_v))
        *stored, token = pl.pallas_call(
            store_early,
            out_shape=final + [pltpu.HBM((8, 128), jnp.float32)],
            in_specs=[vmem] * 2,
            out_specs=[hbm] * 4,
            scratch_shapes=[dma((3, 6)), dma((6,))],
            compiler_params=small(),
            name="store_early",
        )(gathered, held)
        finished = pl.pallas_call(
            finish,
            out_shape=late,
            in_specs=[vmem] * 2 + [hbm],
            out_specs=vmem,
            scratch_shapes=[pltpu.SemaphoreType.REGULAR, dma((2, chunks)), dma((2, chunks)), dma((chunks,)), dma((chunks,))],
            compiler_params=small(collective_id=1, has_side_effects=True),
            name="finish",
        )(held, far_late, pltpu.with_memory_space_constraint(token, pltpu.HBM))
        outs = pl.pallas_call(
            store_late,
            out_shape=final,
            in_specs=[vmem] + [hbm] * 3,
            out_specs=[hbm] * 3,
            input_output_aliases={1: 0, 2: 1, 3: 2},
            scratch_shapes=[dma((6,))],
            compiler_params=small(),
            name="store_late",
        )(*in_vmem(finished), *stored)
        return tuple(out[:, None, :] for out in outs)

    return jax.shard_map(local_step, mesh=mesh, in_specs=(P(("dp", "tp"), None), P(None), P(None, "tp", None), P(None, "tp"), P(None, "tp")), out_specs=(P("dp", "tp", None), P("dp", "tp", None), P("dp", "tp", None)), check_vma=False)
```

```python
import functools

import jax
import jax.numpy as jnp
from jax import lax
from jax.experimental import pallas as pl
from jax.experimental.pallas import tpu as pltpu
from jax.sharding import PartitionSpec as P

EPSILON = 1e-6
CHUNK = 256
SIDE_CHUNK = 128
PIECE = 16

K, V, Q = range(3)
KV, KVQ = pl.ds(0, 2), pl.ds(0, 3)
Q_SAME, Q_OTHER = 2, 3
OWN, SIDE, MATE, MATE_SIDE, FAR, FAR_MATE = range(6)
LATE_FAR, LATE_FAR_MATE = range(2)


class Place:
    def __init__(self):
        self.me = lax.axis_index("tp")
        self.core = lax.rem(self.me, 2)
        self.row = self.me // 4
        self.mate = self.me + 1 - 2 * self.core
        self.side = self.across(self.me)
        self.far = self.me + 2 - 4 * lax.rem(self.me // 2, 2)
        self.far_mate = self.far + 1 - 2 * self.core
        self.first = FIRST[0] + (FIRST[1] - FIRST[0]) * self.core
        self.first_other = FIRST[0] + FIRST[1] - self.first

    def across(self, device):
        return device + 4 - 8 * (device // 4)


def send(src, dst, send_sem, recv_sem, to):
    return pltpu.make_async_remote_copy(src_ref=src, dst_ref=dst, send_sem=send_sem, recv_sem=recv_sem, device_id={"tp": to})


def signal(sem, to):
    pl.semaphore_signal(sem, inc=1, device_id={"tp": to})


def loop(start, stop, body):
    def step(i, carry):
        body(i)
        return carry

    lax.fori_loop(start, stop, step, 0)


def span(i, size, base=0, count=1):
    return pl.ds(pl.multiple_of(base + i * size, size), count * size)


def by_core(at, body):
    for core in range(2):
        pl.when(at.core == core)(functools.partial(body, core))


SAME, OTHER = range(2)
FIRST = (1, 3)


def side_message(at, rows, stage, target, send_sems, recv_sems, kind, i, count=1):
    src, dst, block, peer = ((KVQ, KVQ, LATE_FAR, at.far), (Q_OTHER, Q, LATE_FAR_MATE, at.far_mate))[kind]
    return send(stage.at[src, span(i, CHUNK, 0, count), :], target.at[dst, span(i, CHUNK, block * rows, count), :],
                send_sems.at[kind, i], recv_sems.at[kind, i], peer)


def late_relay(at, rows, source, target, send_sems, recv_sems, i, count=1):
    return send(source.at[KV, span(i, CHUNK, LATE_FAR * rows, count), :], target.at[KV, span(i, CHUNK, LATE_FAR_MATE * rows, count), :],
                send_sems.at[i], recv_sems.at[i], at.mate)


def gather(x_hbm, gain_hbm, wq_hbm, wk_hbm, wv_hbm, early, late, far_late,
           x_own, x_side, w_own, w_far, far_own, mate_q, gain,
           mate_answer, side_answer, far_answer, load_gain, load_x, lw_sem, mw_send, mw_recv, fw_send, fw_recv, rw_send, rw_recv,
           x_send, x_recv, mo_send, mo_recv, ms_send, ms_recv, fo_send, fo_recv, fs_send, fs_recv, r_send, r_recv, lr_send, lr_recv):
    rows, width = x_hbm.shape
    head = wq_hbm.shape[1]
    part = wk_hbm.shape[1]
    chunks = rows // CHUNK
    side_chunks = rows // SIDE_CHUNK
    at = Place()
    core = at.core

    barrier = pltpu.get_barrier_semaphore()
    signal(barrier, at.far)

    @pl.when(core == 1)
    def _():
        signal(barrier, at.mate)

    @pl.when(at.row == 0)
    def _():
        signal(barrier, at.side)

    q_cols = pl.ds(pl.multiple_of(core * head, head), head)
    k_cols = pl.ds(pl.multiple_of(2 * head + core * part, part), part)
    v_cols = pl.ds(pl.multiple_of(3 * head + core * part, part), part)
    lead = width // 4
    mine = (
        (wk_hbm, pl.ds(0, lead), k_cols),
        (wk_hbm, pl.ds(lead, width - lead), k_cols),
        (wv_hbm, pl.ds(0, width), v_cols),
        (wq_hbm, pl.ds(0, width), q_cols),
    )
    load_w, mate_w, far_w, relay_w = [], [], [], []
    for i, (src, depth, cols) in enumerate(mine):
        near_part, far_part = w_own.at[depth, cols], w_far.at[depth, cols]
        load_w.append(pltpu.make_async_copy(src.at[depth, :], near_part, lw_sem.at[i]))
        mate_w.append(send(near_part, near_part, mw_send.at[i], mw_recv.at[i], at.mate))
        far_w.append(send(near_part, far_part, fw_send.at[i], fw_recv.at[i], at.far))
        relay_w.append(send(far_part, far_part, rw_send.at[i], rw_recv.at[i], at.mate))

    def load_chunk(i):
        return pltpu.make_async_copy(x_hbm.at[span(i, CHUNK), :], x_own.at[span(i, CHUNK), :], load_x.at[i])

    def side_chunk(i):
        return send(x_hbm.at[span(i, SIDE_CHUNK), :], x_side.at[span(i, SIDE_CHUNK), :], x_send.at[i], x_recv.at[i], at.side)

    for copy in load_w:
        copy.start()

    pl.semaphore_wait(barrier, 2 - core + at.row)
    for load, copy in zip(load_w, far_w):
        load.wait()
        copy.start()

    gain_copy = pltpu.make_async_copy(gain_hbm, gain, load_gain)
    gain_copy.start()
    for i in range(chunks):
        load_chunk(i).start()

    @pl.when(core == 0)
    def _():
        signal(mate_answer, at.mate)

    @pl.when(at.row == 1)
    def _():
        signal(side_answer, at.side)

    @pl.when(core == 1)
    def _():
        pl.semaphore_wait(mate_answer, 1)

    signal(far_answer, at.far)
    for copy in mate_w:
        copy.start()

    @pl.when(at.row == 0)
    def _():
        pl.semaphore_wait(side_answer, 1)

    loop(0, side_chunks, lambda i: side_chunk(i).start())

    def normalise(ref, i, size):
        def piece(p, carry):
            here = pl.ds(pl.multiple_of(i * size + p * PIECE, PIECE), PIECE)
            x_wide = ref[here, :].astype(jnp.float32)
            mean_sq = jnp.mean(x_wide * x_wide, axis=-1, keepdims=True)
            ref[here, :] = (x_wide * lax.rsqrt(mean_sq + EPSILON) * gain[...].reshape(1, width)).astype(jnp.bfloat16)
            return carry

        lax.fori_loop(0, size // PIECE, piece, 0, unroll=4)

    def product(ref, here, w, block):
        cols = slice(block * head, (block + 1) * head) if isinstance(block, int) else pl.ds(pl.multiple_of(block * head, head), head)
        return jnp.dot(ref[here, :], w[:, cols], preferred_element_type=jnp.float32).astype(jnp.bfloat16)

    def mate_copies(block, i):
        size, sends, recvs = (SIDE_CHUNK, ms_send, ms_recv) if block == SIDE else (CHUNK, mo_send, mo_recv)
        here, there = span(i, size, block * rows), span(i, size, (MATE + block) * rows)
        return (
            send(early.at[KV, here, :], early.at[KV, there, :], sends.at[0, i], recvs.at[0, i], at.mate),
            send(mate_q.at[here, :], early.at[Q, there, :], sends.at[1, i], recvs.at[1, i], at.mate),
        )

    def near_products(ref, block, i):
        size = SIDE_CHUNK if block == SIDE else CHUNK
        here, source = span(i, size, block * rows), span(i, size)
        early[K, here, :] = product(ref, source, w_own, 2)
        early[V, here, :] = product(ref, source, w_own, 3)
        early[Q, here, :] = product(ref, source, w_own, core)
        mate_q[here, :] = product(ref, source, w_own, 1 - core)
        for copy in mate_copies(block, i):
            copy.start()

    far_columns = {K: 2, V: 3, Q_SAME: core, Q_OTHER: 1 - core}

    def far_products(ref, here, stage, kinds):
        for kind in kinds:
            stage[kind, here, :] = product(ref, here, w_far, far_columns[kind])

    def own_message(j, i):
        src, dst, block, peer = ((KV, KV, FAR, at.far), (Q_SAME, Q, FAR, at.far), (Q_OTHER, Q, FAR_MATE, at.far_mate))[j]
        return send(far_own.at[src, span(i, CHUNK), :], early.at[dst, span(i, CHUNK, block * rows), :], fo_send.at[j, i], fo_recv.at[j, i], peer)

    message = functools.partial(side_message, at, rows, far_late, late, fs_send, fs_recv)

    def relay(i):
        return send(early.at[KV, span(i, CHUNK, FAR * rows), :], early.at[KV, span(i, CHUNK, FAR_MATE * rows), :], r_send.at[i], r_recv.at[i], at.mate)

    def own_norm(i):
        load_chunk(i).wait()
        normalise(x_own, i, CHUNK)

    gain_copy.wait()
    loop(0, chunks, own_norm)
    for copy in mate_w:
        copy.wait_recv()
    loop(0, chunks, lambda i: near_products(x_own, OWN, i))

    for arrived, onward in zip(far_w[:3], relay_w[:3]):
        arrived.wait_recv()
        onward.start()
    for copy in relay_w[:3]:
        copy.wait_recv()

    def far_kv_step(i):
        far_products(x_own, span(i, CHUNK), far_own, (K, V))
        own_message(0, i).start()

    loop(0, chunks, far_kv_step)
    far_w[3].wait_recv()
    relay_w[3].start()
    relay_w[3].wait_recv()
    pl.semaphore_wait(far_answer, 1)

    def far_q_step(i):
        far_products(x_own, span(i, CHUNK), far_own, (Q_SAME, Q_OTHER))
        own_message(1, i).start()
        own_message(2, i).start()

    loop(0, chunks, far_q_step)

    def side_step(i):
        side_chunk(i).wait_recv()
        normalise(x_side, i, SIDE_CHUNK)
        near_products(x_side, SIDE, i)
        far_products(x_side, span(i, SIDE_CHUNK), far_late, (Q_OTHER, K, V, Q_SAME))
        done = lax.rem(i + 1, CHUNK // SIDE_CHUNK) == 0
        n = i // (CHUNK // SIDE_CHUNK)

        @pl.when(done & (n < at.first))
        def _():
            message(OTHER, n).start()

        @pl.when(done & (n == at.first - 1))
        def _():
            by_core(at, lambda c: message(SAME, 0, FIRST[c]).start())

    loop(0, side_chunks - 1, side_step)

    def relay_step(i):
        own_message(0, i).wait_recv()
        relay(i).start()

    loop(0, chunks, relay_step)

    def drain_own(i):
        for copy in mate_copies(OWN, i):
            copy.wait_send()
            copy.wait_recv()
        for j in range(3):
            own_message(j, i).wait_send()
        for j in (1, 2):
            own_message(j, i).wait_recv()
        relay(i).wait_send()
        relay(i).wait_recv()

    loop(0, chunks, drain_own)
    for copies in (mate_w, far_w, relay_w):
        for copy in copies:
            copy.wait_send()

    side_step(side_chunks - 1)

    def drain_side(i):
        side_chunk(i).wait_send()
        for copy in mate_copies(SIDE, i):
            copy.wait_send()
            copy.wait_recv()

    loop(0, side_chunks, drain_side)
    loop(0, at.first_other, lambda i: message(OTHER, i).wait_recv())
    loop(0, at.first, lambda i: message(OTHER, i).wait_send())

    def close(c):
        same = message(SAME, 0, FIRST[c])
        same.wait_recv()
        onward = late_relay(at, rows, late, late, lr_send, lr_recv, 0, FIRST[0])
        if c == 0:
            onward.start()
            onward.wait_send()
        else:
            onward.wait_recv()
        same.wait_send()

    by_core(at, close)


def finish(held, far_late, token, late, answer, fs_send, fs_recv, r_send, r_recv):
    rows = far_late.shape[1]
    chunks = rows // CHUNK
    at = Place()
    barrier = pltpu.get_barrier_semaphore()
    signal(barrier, at.far)

    @pl.when(at.core == 0)
    def _():
        signal(barrier, at.mate)
        signal(barrier, at.far_mate)

    pl.semaphore_wait(barrier, 1 + 2 * at.core)
    message = functools.partial(side_message, at, rows, far_late, late, fs_send, fs_recv)
    relay = functools.partial(late_relay, at, rows)

    def body(c):
        first, other_first = FIRST[c], FIRST[1 - c]
        same, other = (message(kind, first, chunks - first) for kind in (SAME, OTHER))
        same.start()
        relays = [relay(held, late, r_send, r_recv, 0, first)] if c else []
        if c:
            signal(answer, at.mate)
            signal(answer, at.far_mate)
        else:
            pl.semaphore_wait(answer, 2)
        other.start()
        for copy in relays:
            copy.start()
        same.wait_recv()
        relays.append(relay(late, late, r_send, r_recv, first, chunks - first))
        relays[-1].start()
        if c == 0:
            relay(held, late, r_send, r_recv, 0, other_first).wait_recv()
        relay(late, late, r_send, r_recv, other_first, chunks - other_first).wait_recv()
        for copy in relays:
            copy.wait_send()
        same.wait_send()
        message(OTHER, other_first, chunks - other_first).wait_recv()
        other.wait_send()

    by_core(at, body)


def late_chunks(core, held):
    first, other, relayed = FIRST[core], FIRST[1 - core], core * FIRST[0]
    spans = [(o, LATE_FAR, first) for o in (K, V, Q)] + [(Q, LATE_FAR_MATE, other)] + [(o, LATE_FAR_MATE, relayed) for o in (K, V)]
    return [(o, block, 0, n) if held else (o, block, n, None) for o, block, n in spans]


def store_chunks(at, source, outs, sems, core, held):
    rows = source.shape[1] // 2
    owners = tuple(at.across(device) for device in (at.far, at.far_mate))
    copies = []
    for j, (o, block, start, count) in enumerate(late_chunks(core, held)):
        count = (rows // CHUNK - start if count is None else count) * CHUNK
        if count:
            copies.append(pltpu.make_async_copy(
                source.at[o, pl.ds(block * rows + start * CHUNK, count), :],
                outs[o].at[pl.ds(pl.multiple_of(owners[block] * rows + start * CHUNK, CHUNK), count), :],
                sems.at[j],
            ))
    return copies


def run(copies):
    for copy in copies:
        copy.start()
    for copy in copies:
        copy.wait()


def store_early(early, held, q_out, k_out, v_out, token, sems, held_sems):
    at = Place()
    owners = (at.me, at.side, at.mate, at.across(at.mate), at.far, at.far_mate)
    rows = early.shape[1] // len(owners)
    outs = (k_out, v_out, q_out)
    for core in range(2):
        @pl.when(at.core == core)
        def _():
            run([
                pltpu.make_async_copy(early.at[o, pl.ds(block * rows, rows), :], out.at[span(owner, rows), :], sems.at[o, block])
                for o, out in enumerate(outs)
                for block, owner in enumerate(owners)
            ] + store_chunks(at, held, outs, held_sems, core, True))


def store_late(late, q_in, k_in, v_in, q_out, k_out, v_out, sems):
    at = Place()
    for core in range(2):
        @pl.when(at.core == core)
        def _():
            run(store_chunks(at, late, (k_out, v_out, q_out), sems, core, False))


def in_vmem(*arrays):
    return tuple(pltpu.with_memory_space_constraint(array, pltpu.VMEM) for array in arrays)


def solution(mesh):
    group_size = mesh.shape["tp"]

    def local_step(x_rows, norm_gain, w_q, w_k, w_v):
        rows, width = x_rows.shape
        head = w_q.shape[2]
        chunks = rows // CHUNK
        dma = pltpu.SemaphoreType.DMA
        any_space = pl.BlockSpec(memory_space=pl.ANY)
        vmem = pl.BlockSpec(memory_space=pltpu.VMEM)
        hbm = pl.BlockSpec(memory_space=pltpu.HBM)

        def small(**settings):
            return pltpu.CompilerParams(vmem_limit_bytes=1024 * 1024, **settings)

        early = pltpu.VMEM((3, 6 * rows, head), jnp.bfloat16)
        late = pltpu.VMEM((3, 2 * rows, head), jnp.bfloat16)
        final = [pltpu.HBM((group_size * rows, head), jnp.bfloat16)] * 3
        side_chunks = rows // SIDE_CHUNK

        gathered, held, far_late = in_vmem(*pl.pallas_call(
            gather,
            out_shape=[early, late, pltpu.VMEM((4, rows, head), jnp.bfloat16)],
            in_specs=[any_space] * 5,
            out_specs=[vmem] * 3,
            scratch_shapes=[
                pltpu.VMEM((rows, width), jnp.bfloat16),
                pltpu.VMEM((rows, width), jnp.bfloat16),
                pltpu.VMEM((width, 4 * head), jnp.bfloat16),
                pltpu.VMEM((width, 4 * head), jnp.bfloat16),
                pltpu.VMEM((4, rows, head), jnp.bfloat16),
                pltpu.VMEM((2 * rows, head), jnp.bfloat16),
                pltpu.VMEM((width,), jnp.float32),
                *[pltpu.SemaphoreType.REGULAR] * 3, dma(()), dma((chunks,)),
                *[dma((4,))] * 7,
                dma((side_chunks,)), dma((side_chunks,)), dma((2, chunks)), dma((2, chunks)), dma((2, side_chunks)), dma((2, side_chunks)),
                dma((3, chunks)), dma((3, chunks)), dma((2, chunks)), dma((2, chunks)), dma((chunks,)), dma((chunks,)), dma((1,)), dma((1,)),
            ],
            compiler_params=pltpu.CompilerParams(collective_id=0, has_side_effects=True, vmem_limit_bytes=40 * 1024 * 1024),
            name="gather",
        )(x_rows, norm_gain, w_q.reshape(width, head), w_k, w_v))
        *stored, token = pl.pallas_call(
            store_early,
            out_shape=final + [pltpu.HBM((8, 128), jnp.float32)],
            in_specs=[vmem] * 2,
            out_specs=[hbm] * 4,
            scratch_shapes=[dma((3, 6)), dma((6,))],
            compiler_params=small(),
            name="store_early",
        )(gathered, held)
        finished = pl.pallas_call(
            finish,
            out_shape=late,
            in_specs=[vmem] * 2 + [hbm],
            out_specs=vmem,
            scratch_shapes=[pltpu.SemaphoreType.REGULAR, dma((2, chunks)), dma((2, chunks)), dma((chunks,)), dma((chunks,))],
            compiler_params=small(collective_id=1, has_side_effects=True),
            name="finish",
        )(held, far_late, pltpu.with_memory_space_constraint(token, pltpu.HBM))
        outs = pl.pallas_call(
            store_late,
            out_shape=final,
            in_specs=[vmem] + [hbm] * 3,
            out_specs=[hbm] * 3,
            input_output_aliases={1: 0, 2: 1, 3: 2},
            scratch_shapes=[dma((6,))],
            compiler_params=small(),
            name="store_late",
        )(*in_vmem(finished), *stored)
        return tuple(out[:, None, :] for out in outs)

    return jax.shard_map(local_step, mesh=mesh, in_specs=(P(("dp", "tp"), None), P(None), P(None, "tp", None), P(None, "tp"), P(None, "tp")), out_specs=(P("dp", "tp", None), P("dp", "tp", None), P("dp", "tp", None)), check_vma=False)
```

```python
import functools

import jax
import jax.numpy as jnp
from jax import lax
from jax.experimental import pallas as pl
from jax.experimental.pallas import tpu as pltpu
from jax.sharding import PartitionSpec as P

EPSILON = 1e-6
CHUNK = 256
SIDE_CHUNK = 128
PIECE = 16

K, V, Q = range(3)
KV, KVQ = pl.ds(0, 2), pl.ds(0, 3)
Q_SAME, Q_OTHER = 2, 3
OWN, SIDE, MATE, MATE_SIDE, FAR, FAR_MATE = range(6)
LATE_FAR, LATE_FAR_MATE = range(2)


class Place:
    def __init__(self):
        self.me = lax.axis_index("tp")
        self.core = lax.rem(self.me, 2)
        self.row = self.me // 4
        self.mate = self.me + 1 - 2 * self.core
        self.side = self.across(self.me)
        self.far = self.me + 2 - 4 * lax.rem(self.me // 2, 2)
        self.far_mate = self.far + 1 - 2 * self.core
        self.first = FIRST[0] + (FIRST[1] - FIRST[0]) * self.core
        self.first_other = FIRST[0] + FIRST[1] - self.first

    def across(self, device):
        return device + 4 - 8 * (device // 4)


def send(src, dst, send_sem, recv_sem, to):
    return pltpu.make_async_remote_copy(src_ref=src, dst_ref=dst, send_sem=send_sem, recv_sem=recv_sem, device_id={"tp": to})


def signal(sem, to):
    pl.semaphore_signal(sem, inc=1, device_id={"tp": to})


def loop(start, stop, body):
    def step(i, carry):
        body(i)
        return carry

    lax.fori_loop(start, stop, step, 0)


def span(i, size, base=0, count=1):
    return pl.ds(pl.multiple_of(base + i * size, size), count * size)


def by_core(at, body):
    for core in range(2):
        pl.when(at.core == core)(functools.partial(body, core))


SAME, OTHER, SAME_KV, SAME_Q = range(4)
FIRST = (1, 3)


def side_message(at, rows, stage, target, send_sems, recv_sems, kind, i, count=1):
    src, dst, block, peer = {
        SAME: (KVQ, KVQ, LATE_FAR, at.far),
        SAME_KV: (KV, KV, LATE_FAR, at.far),
        SAME_Q: (Q_SAME, Q, LATE_FAR, at.far),
        OTHER: (Q_OTHER, Q, LATE_FAR_MATE, at.far_mate),
    }[kind]
    return send(stage.at[src, span(i, CHUNK, 0, count), :], target.at[dst, span(i, CHUNK, block * rows, count), :],
                send_sems.at[kind, i], recv_sems.at[kind, i], peer)


def late_relay(at, rows, source, target, send_sems, recv_sems, i, count=1):
    return send(source.at[KV, span(i, CHUNK, LATE_FAR * rows, count), :], target.at[KV, span(i, CHUNK, LATE_FAR_MATE * rows, count), :],
                send_sems.at[i], recv_sems.at[i], at.mate)


def gather(x_hbm, gain_hbm, wq_hbm, wk_hbm, wv_hbm, early, late, far_late,
           x_own, x_side, w_own, w_far, far_own, mate_q, gain,
           mate_answer, side_answer, far_answer, load_gain, load_x, lw_sem, mw_send, mw_recv, fw_send, fw_recv, rw_send, rw_recv,
           x_send, x_recv, mo_send, mo_recv, ms_send, ms_recv, fo_send, fo_recv, fs_send, fs_recv, r_send, r_recv, lr_send, lr_recv):
    rows, width = x_hbm.shape
    head = wq_hbm.shape[1]
    part = wk_hbm.shape[1]
    chunks = rows // CHUNK
    side_chunks = rows // SIDE_CHUNK
    at = Place()
    core = at.core

    barrier = pltpu.get_barrier_semaphore()
    signal(barrier, at.far)

    @pl.when(core == 1)
    def _():
        signal(barrier, at.mate)

    @pl.when(at.row == 0)
    def _():
        signal(barrier, at.side)

    q_cols = pl.ds(pl.multiple_of(core * head, head), head)
    k_cols = pl.ds(pl.multiple_of(2 * head + core * part, part), part)
    v_cols = pl.ds(pl.multiple_of(3 * head + core * part, part), part)
    lead = width // 4
    mine = (
        (wk_hbm, pl.ds(0, lead), k_cols),
        (wk_hbm, pl.ds(lead, width - lead), k_cols),
        (wv_hbm, pl.ds(0, width), v_cols),
        (wq_hbm, pl.ds(0, width), q_cols),
    )
    load_w, mate_w, far_w, relay_w = [], [], [], []
    for i, (src, depth, cols) in enumerate(mine):
        near_part, far_part = w_own.at[depth, cols], w_far.at[depth, cols]
        load_w.append(pltpu.make_async_copy(src.at[depth, :], near_part, lw_sem.at[i]))
        mate_w.append(send(near_part, near_part, mw_send.at[i], mw_recv.at[i], at.mate))
        far_w.append(send(near_part, far_part, fw_send.at[i], fw_recv.at[i], at.far))
        relay_w.append(send(far_part, far_part, rw_send.at[i], rw_recv.at[i], at.mate))

    def load_chunk(i):
        return pltpu.make_async_copy(x_hbm.at[span(i, CHUNK), :], x_own.at[span(i, CHUNK), :], load_x.at[i])

    def side_chunk(i):
        return send(x_hbm.at[span(i, SIDE_CHUNK), :], x_side.at[span(i, SIDE_CHUNK), :], x_send.at[i], x_recv.at[i], at.side)

    for copy in load_w:
        copy.start()

    pl.semaphore_wait(barrier, 2 - core + at.row)
    for load, copy in zip(load_w, far_w):
        load.wait()
        copy.start()

    gain_copy = pltpu.make_async_copy(gain_hbm, gain, load_gain)
    gain_copy.start()
    for i in range(chunks):
        load_chunk(i).start()

    @pl.when(core == 0)
    def _():
        signal(mate_answer, at.mate)

    @pl.when(at.row == 1)
    def _():
        signal(side_answer, at.side)

    @pl.when(core == 1)
    def _():
        pl.semaphore_wait(mate_answer, 1)

    signal(far_answer, at.far)
    for copy in mate_w:
        copy.start()

    @pl.when(at.row == 0)
    def _():
        pl.semaphore_wait(side_answer, 1)

    loop(0, side_chunks, lambda i: side_chunk(i).start())

    def normalise(ref, i, size):
        def piece(p, carry):
            here = pl.ds(pl.multiple_of(i * size + p * PIECE, PIECE), PIECE)
            x_wide = ref[here, :].astype(jnp.float32)
            mean_sq = jnp.mean(x_wide * x_wide, axis=-1, keepdims=True)
            ref[here, :] = (x_wide * lax.rsqrt(mean_sq + EPSILON) * gain[...].reshape(1, width)).astype(jnp.bfloat16)
            return carry

        lax.fori_loop(0, size // PIECE, piece, 0, unroll=4)

    def product(ref, here, w, block):
        cols = slice(block * head, (block + 1) * head) if isinstance(block, int) else pl.ds(pl.multiple_of(block * head, head), head)
        return jnp.dot(ref[here, :], w[:, cols], preferred_element_type=jnp.float32).astype(jnp.bfloat16)

    def mate_copies(block, i):
        size, sends, recvs = (SIDE_CHUNK, ms_send, ms_recv) if block == SIDE else (CHUNK, mo_send, mo_recv)
        here, there = span(i, size, block * rows), span(i, size, (MATE + block) * rows)
        return (
            send(early.at[KV, here, :], early.at[KV, there, :], sends.at[0, i], recvs.at[0, i], at.mate),
            send(mate_q.at[here, :], early.at[Q, there, :], sends.at[1, i], recvs.at[1, i], at.mate),
        )

    def near_products(ref, block, i):
        size = SIDE_CHUNK if block == SIDE else CHUNK
        here, source = span(i, size, block * rows), span(i, size)
        early[K, here, :] = product(ref, source, w_own, 2)
        early[V, here, :] = product(ref, source, w_own, 3)
        early[Q, here, :] = product(ref, source, w_own, core)
        mate_q[here, :] = product(ref, source, w_own, 1 - core)
        for copy in mate_copies(block, i):
            copy.start()

    far_columns = {K: 2, V: 3, Q_SAME: core, Q_OTHER: 1 - core}

    def far_products(ref, here, stage, kinds):
        for kind in kinds:
            stage[kind, here, :] = product(ref, here, w_far, far_columns[kind])

    def own_message(j, i):
        src, dst, block, peer = ((KV, KV, FAR, at.far), (Q_SAME, Q, FAR, at.far), (Q_OTHER, Q, FAR_MATE, at.far_mate))[j]
        return send(far_own.at[src, span(i, CHUNK), :], early.at[dst, span(i, CHUNK, block * rows), :], fo_send.at[j, i], fo_recv.at[j, i], peer)

    message = functools.partial(side_message, at, rows, far_late, late, fs_send, fs_recv)

    def relay(i):
        return send(early.at[KV, span(i, CHUNK, FAR * rows), :], early.at[KV, span(i, CHUNK, FAR_MATE * rows), :], r_send.at[i], r_recv.at[i], at.mate)

    def own_norm(i):
        load_chunk(i).wait()
        normalise(x_own, i, CHUNK)

    gain_copy.wait()
    loop(0, chunks, own_norm)
    for copy in mate_w:
        copy.wait_recv()
    loop(0, chunks, lambda i: near_products(x_own, OWN, i))

    for arrived, onward in zip(far_w[:3], relay_w[:3]):
        arrived.wait_recv()
        onward.start()
    for copy in relay_w[:3]:
        copy.wait_recv()

    def far_kv_step(i):
        far_products(x_own, span(i, CHUNK), far_own, (K, V))
        own_message(0, i).start()

    loop(0, chunks, far_kv_step)
    far_w[3].wait_recv()
    relay_w[3].start()
    relay_w[3].wait_recv()
    pl.semaphore_wait(far_answer, 1)

    def far_q_step(i):
        far_products(x_own, span(i, CHUNK), far_own, (Q_SAME, Q_OTHER))
        own_message(1, i).start()
        own_message(2, i).start()

    loop(0, chunks, far_q_step)

    def side_step(i):
        side_chunk(i).wait_recv()
        normalise(x_side, i, SIDE_CHUNK)
        near_products(x_side, SIDE, i)
        far_products(x_side, span(i, SIDE_CHUNK), far_late, (Q_OTHER, K, V, Q_SAME))
        done = lax.rem(i + 1, CHUNK // SIDE_CHUNK) == 0
        n = i // (CHUNK // SIDE_CHUNK)

        @pl.when(done & (n < at.first))
        def _():
            message(OTHER, n).start()

        @pl.when(done & (n == at.first - 1))
        def _():
            by_core(at, lambda c: message(SAME, 0, FIRST[c]).start())

    loop(0, side_chunks - 1, side_step)

    def relay_step(i):
        own_message(0, i).wait_recv()
        relay(i).start()

    loop(0, chunks, relay_step)

    def drain_own(i):
        for copy in mate_copies(OWN, i):
            copy.wait_send()
            copy.wait_recv()
        for j in range(3):
            own_message(j, i).wait_send()
        for j in (1, 2):
            own_message(j, i).wait_recv()
        relay(i).wait_send()
        relay(i).wait_recv()

    loop(0, chunks, drain_own)
    for copies in (mate_w, far_w, relay_w):
        for copy in copies:
            copy.wait_send()

    side_step(side_chunks - 1)

    def drain_side(i):
        side_chunk(i).wait_send()
        for copy in mate_copies(SIDE, i):
            copy.wait_send()
            copy.wait_recv()

    loop(0, side_chunks, drain_side)
    loop(0, at.first_other, lambda i: message(OTHER, i).wait_recv())
    loop(0, at.first, lambda i: message(OTHER, i).wait_send())

    def close(c):
        same = message(SAME, 0, FIRST[c])
        same.wait_recv()
        onward = late_relay(at, rows, late, late, lr_send, lr_recv, 0, FIRST[0])
        if c == 0:
            onward.start()
            onward.wait_send()
        else:
            onward.wait_recv()
        same.wait_send()

    by_core(at, close)


def finish(held, far_late, token, late, answer, fs_send, fs_recv, r_send, r_recv):
    rows = far_late.shape[1]
    chunks = rows // CHUNK
    at = Place()
    barrier = pltpu.get_barrier_semaphore()
    signal(barrier, at.far)

    @pl.when(at.core == 0)
    def _():
        signal(barrier, at.mate)
        signal(barrier, at.far_mate)

    pl.semaphore_wait(barrier, 1 + 2 * at.core)
    message = functools.partial(side_message, at, rows, far_late, late, fs_send, fs_recv)
    relay = functools.partial(late_relay, at, rows)

    def body(c):
        first, other_first = FIRST[c], FIRST[1 - c]
        here = functools.partial(message, i=first, count=chunks - first)
        if c == 0:
            same = [here(SAME)]
            other = [message(OTHER, first), message(OTHER, first + 1, chunks - first - 1)]
            other_arrives = [message(OTHER, other_first, chunks - other_first)]
            relays = []
            relays_arrive = [relay(held, late, r_send, r_recv, 0, other_first)]
        else:
            same = [here(SAME_KV), here(SAME_Q)]
            other = [here(OTHER)]
            other_arrives = [message(OTHER, other_first), message(OTHER, other_first + 1, chunks - other_first - 1)]
            relays = [relay(held, late, r_send, r_recv, 0, first)]
            relays_arrive = []
        onward = relay(late, late, r_send, r_recv, first, chunks - first)
        relays_arrive.append(relay(late, late, r_send, r_recv, other_first, chunks - other_first))

        same[0].start()
        if c == 0:
            pl.semaphore_wait(answer, 2)
        else:
            signal(answer, at.mate)
            signal(answer, at.far_mate)
        for copy in other + relays:
            copy.start()
        same[0].wait_recv()
        onward.start()
        if c == 1:
            other_arrives[0].wait_recv()
            same[1].start()
        for copy in relays_arrive + other_arrives[c:] + same[1:]:
            copy.wait_recv()
        for copy in relays + [onward] + same + other:
            copy.wait_send()

    by_core(at, body)


def late_chunks(core, held):
    first, other, relayed = FIRST[core], FIRST[1 - core], core * FIRST[0]
    spans = [(o, LATE_FAR, first) for o in (K, V, Q)] + [(Q, LATE_FAR_MATE, other)] + [(o, LATE_FAR_MATE, relayed) for o in (K, V)]
    return [(o, block, 0, n) if held else (o, block, n, None) for o, block, n in spans]


def store_chunks(at, source, outs, sems, core, held):
    rows = source.shape[1] // 2
    owners = tuple(at.across(device) for device in (at.far, at.far_mate))
    copies = []
    for j, (o, block, start, count) in enumerate(late_chunks(core, held)):
        count = (rows // CHUNK - start if count is None else count) * CHUNK
        if count:
            copies.append(pltpu.make_async_copy(
                source.at[o, pl.ds(block * rows + start * CHUNK, count), :],
                outs[o].at[pl.ds(pl.multiple_of(owners[block] * rows + start * CHUNK, CHUNK), count), :],
                sems.at[j],
            ))
    return copies


def run(copies):
    for copy in copies:
        copy.start()
    for copy in copies:
        copy.wait()


def store_early(early, held, q_out, k_out, v_out, token, sems, held_sems):
    at = Place()
    owners = (at.me, at.side, at.mate, at.across(at.mate), at.far, at.far_mate)
    rows = early.shape[1] // len(owners)
    outs = (k_out, v_out, q_out)
    for core in range(2):
        @pl.when(at.core == core)
        def _():
            run([
                pltpu.make_async_copy(early.at[o, pl.ds(block * rows, rows), :], out.at[span(owner, rows), :], sems.at[o, block])
                for o, out in enumerate(outs)
                for block, owner in enumerate(owners)
            ] + store_chunks(at, held, outs, held_sems, core, True))


def store_late(late, q_in, k_in, v_in, q_out, k_out, v_out, sems):
    at = Place()
    for core in range(2):
        @pl.when(at.core == core)
        def _():
            run(store_chunks(at, late, (k_out, v_out, q_out), sems, core, False))


def in_vmem(*arrays):
    return tuple(pltpu.with_memory_space_constraint(array, pltpu.VMEM) for array in arrays)


def solution(mesh):
    group_size = mesh.shape["tp"]

    def local_step(x_rows, norm_gain, w_q, w_k, w_v):
        rows, width = x_rows.shape
        head = w_q.shape[2]
        chunks = rows // CHUNK
        dma = pltpu.SemaphoreType.DMA
        any_space = pl.BlockSpec(memory_space=pl.ANY)
        vmem = pl.BlockSpec(memory_space=pltpu.VMEM)
        hbm = pl.BlockSpec(memory_space=pltpu.HBM)

        def small(**settings):
            return pltpu.CompilerParams(vmem_limit_bytes=1024 * 1024, **settings)

        early = pltpu.VMEM((3, 6 * rows, head), jnp.bfloat16)
        late = pltpu.VMEM((3, 2 * rows, head), jnp.bfloat16)
        final = [pltpu.HBM((group_size * rows, head), jnp.bfloat16)] * 3
        side_chunks = rows // SIDE_CHUNK

        gathered, held, far_late = in_vmem(*pl.pallas_call(
            gather,
            out_shape=[early, late, pltpu.VMEM((4, rows, head), jnp.bfloat16)],
            in_specs=[any_space] * 5,
            out_specs=[vmem] * 3,
            scratch_shapes=[
                pltpu.VMEM((rows, width), jnp.bfloat16),
                pltpu.VMEM((rows, width), jnp.bfloat16),
                pltpu.VMEM((width, 4 * head), jnp.bfloat16),
                pltpu.VMEM((width, 4 * head), jnp.bfloat16),
                pltpu.VMEM((4, rows, head), jnp.bfloat16),
                pltpu.VMEM((2 * rows, head), jnp.bfloat16),
                pltpu.VMEM((width,), jnp.float32),
                *[pltpu.SemaphoreType.REGULAR] * 3, dma(()), dma((chunks,)),
                *[dma((4,))] * 7,
                dma((side_chunks,)), dma((side_chunks,)), dma((2, chunks)), dma((2, chunks)), dma((2, side_chunks)), dma((2, side_chunks)),
                dma((3, chunks)), dma((3, chunks)), dma((2, chunks)), dma((2, chunks)), dma((chunks,)), dma((chunks,)), dma((1,)), dma((1,)),
            ],
            compiler_params=pltpu.CompilerParams(collective_id=0, has_side_effects=True, vmem_limit_bytes=40 * 1024 * 1024),
            name="gather",
        )(x_rows, norm_gain, w_q.reshape(width, head), w_k, w_v))
        *stored, token = pl.pallas_call(
            store_early,
            out_shape=final + [pltpu.HBM((8, 128), jnp.float32)],
            in_specs=[vmem] * 2,
            out_specs=[hbm] * 4,
            scratch_shapes=[dma((3, 6)), dma((6,))],
            compiler_params=small(),
            name="store_early",
        )(gathered, held)
        finished = pl.pallas_call(
            finish,
            out_shape=late,
            in_specs=[vmem] * 2 + [hbm],
            out_specs=vmem,
            scratch_shapes=[pltpu.SemaphoreType.REGULAR, dma((4, chunks)), dma((4, chunks)), dma((chunks,)), dma((chunks,))],
            compiler_params=small(collective_id=1, has_side_effects=True),
            name="finish",
        )(held, far_late, pltpu.with_memory_space_constraint(token, pltpu.HBM))
        outs = pl.pallas_call(
            store_late,
            out_shape=final,
            in_specs=[vmem] + [hbm] * 3,
            out_specs=[hbm] * 3,
            input_output_aliases={1: 0, 2: 1, 3: 2},
            scratch_shapes=[dma((6,))],
            compiler_params=small(),
            name="store_late",
        )(*in_vmem(finished), *stored)
        return tuple(out[:, None, :] for out in outs)

    return jax.shard_map(local_step, mesh=mesh, in_specs=(P(("dp", "tp"), None), P(None), P(None, "tp", None), P(None, "tp"), P(None, "tp")), out_specs=(P("dp", "tp", None), P("dp", "tp", None), P("dp", "tp", None)), check_vma=False)
```

```python
import functools

import jax
import jax.numpy as jnp
from jax import lax
from jax.experimental import pallas as pl
from jax.experimental.pallas import tpu as pltpu
from jax.sharding import PartitionSpec as P

EPSILON = 1e-6
CHUNK = 256
SIDE_CHUNK = 128
PIECE = 16
LEAD = 128

K, V, Q = range(3)
KV, KVQ = pl.ds(0, 2), pl.ds(0, 3)
Q_SAME, Q_OTHER = 2, 3
OWN, SIDE, MATE, MATE_SIDE, FAR, FAR_MATE = range(6)
LATE_FAR, LATE_FAR_MATE = range(2)


class Place:
    def __init__(self):
        self.me = lax.axis_index("tp")
        self.core = lax.rem(self.me, 2)
        self.row = self.me // 4
        self.mate = self.me + 1 - 2 * self.core
        self.side = self.across(self.me)
        self.far = self.me + 2 - 4 * lax.rem(self.me // 2, 2)
        self.far_mate = self.far + 1 - 2 * self.core
        self.first = FIRST[0] + (FIRST[1] - FIRST[0]) * self.core
        self.first_other = FIRST[0] + FIRST[1] - self.first

    def across(self, device):
        return device + 4 - 8 * (device // 4)


def send(src, dst, send_sem, recv_sem, to):
    return pltpu.make_async_remote_copy(src_ref=src, dst_ref=dst, send_sem=send_sem, recv_sem=recv_sem, device_id={"tp": to})


def signal(sem, to):
    pl.semaphore_signal(sem, inc=1, device_id={"tp": to})


def loop(start, stop, body):
    def step(i, carry):
        body(i)
        return carry

    lax.fori_loop(start, stop, step, 0)


def span(i, size, base=0, count=1):
    return pl.ds(pl.multiple_of(base + i * size, size), count * size)


def by_core(at, body):
    for core in range(2):
        pl.when(at.core == core)(functools.partial(body, core))


SAME, OTHER, SAME_KV, SAME_Q = range(4)
FIRST = (1, 3)


def side_message(at, rows, stage, target, send_sems, recv_sems, kind, i, count=1, size=CHUNK, slot=None):
    src, dst, block, peer = {
        SAME: (KVQ, KVQ, LATE_FAR, at.far),
        SAME_KV: (KV, KV, LATE_FAR, at.far),
        SAME_Q: (Q_SAME, Q, LATE_FAR, at.far),
        OTHER: (Q_OTHER, Q, LATE_FAR_MATE, at.far_mate),
    }[kind]
    slot = i if slot is None else slot
    return send(stage.at[src, span(i, size, 0, count), :], target.at[dst, span(i, size, block * rows, count), :],
                send_sems.at[kind, slot], recv_sems.at[kind, slot], peer)


def late_relay(at, rows, source, target, send_sems, recv_sems, i, count=1):
    return send(source.at[KV, span(i, CHUNK, LATE_FAR * rows, count), :], target.at[KV, span(i, CHUNK, LATE_FAR_MATE * rows, count), :],
                send_sems.at[i], recv_sems.at[i], at.mate)


def gather(x_hbm, gain_hbm, wq_hbm, wk_hbm, wv_hbm, early, late, far_late,
           x_own, x_side, w_own, w_far, far_own, mate_q, gain,
           mate_answer, side_answer, far_answer, load_gain, load_x, lw_sem, mw_send, mw_recv, fw_send, fw_recv, rw_send, rw_recv,
           x_send, x_recv, mo_send, mo_recv, ms_send, ms_recv, fo_send, fo_recv, fs_send, fs_recv, r_send, r_recv, lr_send, lr_recv):
    rows, width = x_hbm.shape
    head = wq_hbm.shape[1]
    part = wk_hbm.shape[1]
    chunks = rows // CHUNK
    side_chunks = rows // SIDE_CHUNK
    at = Place()
    core = at.core

    barrier = pltpu.get_barrier_semaphore()
    signal(barrier, at.far)

    @pl.when(core == 1)
    def _():
        signal(barrier, at.mate)

    @pl.when(at.row == 0)
    def _():
        signal(barrier, at.side)

    q_cols = pl.ds(pl.multiple_of(core * head, head), head)
    k_cols = pl.ds(pl.multiple_of(2 * head + core * part, part), part)
    v_cols = pl.ds(pl.multiple_of(3 * head + core * part, part), part)
    lead = width // 4
    mine = (
        (wk_hbm, pl.ds(0, lead), k_cols),
        (wk_hbm, pl.ds(lead, width - lead), k_cols),
        (wv_hbm, pl.ds(0, width), v_cols),
        (wq_hbm, pl.ds(0, width), q_cols),
    )
    load_w, mate_w, far_w, relay_w = [], [], [], []
    for i, (src, depth, cols) in enumerate(mine):
        near_part, far_part = w_own.at[depth, cols], w_far.at[depth, cols]
        load_w.append(pltpu.make_async_copy(src.at[depth, :], near_part, lw_sem.at[i]))
        mate_w.append(send(near_part, near_part, mw_send.at[i], mw_recv.at[i], at.mate))
        far_w.append(send(near_part, far_part, fw_send.at[i], fw_recv.at[i], at.far))
        relay_w.append(send(far_part, far_part, rw_send.at[i], rw_recv.at[i], at.mate))

    def load_chunk(i):
        return pltpu.make_async_copy(x_hbm.at[span(i, CHUNK), :], x_own.at[span(i, CHUNK), :], load_x.at[i])

    def side_chunk(i):
        return send(x_hbm.at[span(i, SIDE_CHUNK), :], x_side.at[span(i, SIDE_CHUNK), :], x_send.at[i], x_recv.at[i], at.side)

    for copy in load_w:
        copy.start()

    pl.semaphore_wait(barrier, 2 - core + at.row)
    for load, copy in zip(load_w, far_w):
        load.wait()
        copy.start()

    gain_copy = pltpu.make_async_copy(gain_hbm, gain, load_gain)
    gain_copy.start()
    for i in range(chunks):
        load_chunk(i).start()

    @pl.when(core == 0)
    def _():
        signal(mate_answer, at.mate)

    @pl.when(at.row == 1)
    def _():
        signal(side_answer, at.side)

    @pl.when(core == 1)
    def _():
        pl.semaphore_wait(mate_answer, 1)

    signal(far_answer, at.far)
    for copy in mate_w:
        copy.start()

    @pl.when(at.row == 0)
    def _():
        pl.semaphore_wait(side_answer, 1)

    loop(0, side_chunks, lambda i: side_chunk(i).start())

    def normalise(ref, i, size):
        def piece(p, carry):
            here = pl.ds(pl.multiple_of(i * size + p * PIECE, PIECE), PIECE)
            x_wide = ref[here, :].astype(jnp.float32)
            mean_sq = jnp.mean(x_wide * x_wide, axis=-1, keepdims=True)
            ref[here, :] = (x_wide * lax.rsqrt(mean_sq + EPSILON) * gain[...].reshape(1, width)).astype(jnp.bfloat16)
            return carry

        lax.fori_loop(0, size // PIECE, piece, 0, unroll=4)

    def product(ref, here, w, block):
        cols = slice(block * head, (block + 1) * head) if isinstance(block, int) else pl.ds(pl.multiple_of(block * head, head), head)
        return jnp.dot(ref[here, :], w[:, cols], preferred_element_type=jnp.float32).astype(jnp.bfloat16)

    def mate_copies(block, i):
        size, sends, recvs = (SIDE_CHUNK, ms_send, ms_recv) if block == SIDE else (CHUNK, mo_send, mo_recv)
        here, there = span(i, size, block * rows), span(i, size, (MATE + block) * rows)
        return (
            send(early.at[KV, here, :], early.at[KV, there, :], sends.at[0, i], recvs.at[0, i], at.mate),
            send(mate_q.at[here, :], early.at[Q, there, :], sends.at[1, i], recvs.at[1, i], at.mate),
        )

    def near_products(ref, block, i):
        size = SIDE_CHUNK if block == SIDE else CHUNK
        here, source = span(i, size, block * rows), span(i, size)
        early[K, here, :] = product(ref, source, w_own, 2)
        early[V, here, :] = product(ref, source, w_own, 3)
        early[Q, here, :] = product(ref, source, w_own, core)
        mate_q[here, :] = product(ref, source, w_own, 1 - core)
        for copy in mate_copies(block, i):
            copy.start()

    far_columns = {K: 2, V: 3, Q_SAME: core, Q_OTHER: 1 - core}

    def far_products(ref, here, stage, kinds):
        for kind in kinds:
            stage[kind, here, :] = product(ref, here, w_far, far_columns[kind])

    def own_message(j, i):
        src, dst, block, peer = ((KV, KV, FAR, at.far), (Q_SAME, Q, FAR, at.far), (Q_OTHER, Q, FAR_MATE, at.far_mate))[j]
        return send(far_own.at[src, span(i, CHUNK), :], early.at[dst, span(i, CHUNK, block * rows), :], fo_send.at[j, i], fo_recv.at[j, i], peer)

    message = functools.partial(side_message, at, rows, far_late, late, fs_send, fs_recv)

    def relay(i):
        return send(early.at[KV, span(i, CHUNK, FAR * rows), :], early.at[KV, span(i, CHUNK, FAR_MATE * rows), :], r_send.at[i], r_recv.at[i], at.mate)

    def own_norm(i):
        load_chunk(i).wait()
        normalise(x_own, i, CHUNK)

    gain_copy.wait()
    loop(0, chunks, own_norm)
    for copy in mate_w:
        copy.wait_recv()
    loop(0, chunks, lambda i: near_products(x_own, OWN, i))

    for arrived, onward in zip(far_w[:3], relay_w[:3]):
        arrived.wait_recv()
        onward.start()
    for copy in relay_w[:3]:
        copy.wait_recv()

    def far_kv_step(i):
        far_products(x_own, span(i, CHUNK), far_own, (K, V))
        own_message(0, i).start()

    loop(0, chunks, far_kv_step)
    far_w[3].wait_recv()
    relay_w[3].start()
    relay_w[3].wait_recv()
    pl.semaphore_wait(far_answer, 1)

    def far_q_step(i):
        far_products(x_own, span(i, CHUNK), far_own, (Q_SAME, Q_OTHER))
        own_message(1, i).start()
        own_message(2, i).start()

    loop(0, chunks, far_q_step)

    def side_step(i):
        side_chunk(i).wait_recv()
        normalise(x_side, i, SIDE_CHUNK)
        near_products(x_side, SIDE, i)
        far_products(x_side, span(i, SIDE_CHUNK), far_late, (Q_OTHER, K, V, Q_SAME))
        done = lax.rem(i + 1, CHUNK // SIDE_CHUNK) == 0
        n = i // (CHUNK // SIDE_CHUNK)

        @pl.when(done & (n < at.first))
        def _():
            message(OTHER, n).start()

        @pl.when(done & (n == at.first - 1))
        def _():
            by_core(at, lambda c: message(SAME, 0, FIRST[c]).start())

    loop(0, side_chunks - 1, side_step)

    def relay_step(i):
        own_message(0, i).wait_recv()
        relay(i).start()

    loop(0, chunks, relay_step)

    def drain_own(i):
        for copy in mate_copies(OWN, i):
            copy.wait_send()
            copy.wait_recv()
        for j in range(3):
            own_message(j, i).wait_send()
        for j in (1, 2):
            own_message(j, i).wait_recv()
        relay(i).wait_send()
        relay(i).wait_recv()

    loop(0, chunks, drain_own)
    for copies in (mate_w, far_w, relay_w):
        for copy in copies:
            copy.wait_send()

    side_step(side_chunks - 1)

    def drain_side(i):
        side_chunk(i).wait_send()
        for copy in mate_copies(SIDE, i):
            copy.wait_send()
            copy.wait_recv()

    loop(0, side_chunks, drain_side)
    loop(0, at.first_other, lambda i: message(OTHER, i).wait_recv())
    loop(0, at.first, lambda i: message(OTHER, i).wait_send())

    def close(c):
        same = message(SAME, 0, FIRST[c])
        same.wait_recv()
        onward = late_relay(at, rows, late, late, lr_send, lr_recv, 0, FIRST[0])
        if c == 0:
            onward.start()
            onward.wait_send()
        else:
            onward.wait_recv()
        same.wait_send()

    by_core(at, close)


def finish(held, far_late, token, late, answer, fs_send, fs_recv, r_send, r_recv):
    rows = far_late.shape[1]
    chunks = rows // CHUNK
    at = Place()
    barrier = pltpu.get_barrier_semaphore()
    signal(barrier, at.far)

    @pl.when(at.core == 0)
    def _():
        signal(barrier, at.mate)
        signal(barrier, at.far_mate)

    pl.semaphore_wait(barrier, 1 + 2 * at.core)
    message = functools.partial(side_message, at, rows, far_late, late, fs_send, fs_recv)
    relay = functools.partial(late_relay, at, rows)

    def body(c):
        first, other_first = FIRST[c], FIRST[1 - c]
        here = functools.partial(message, i=first, count=chunks - first)
        lead = FIRST[0] * CHUNK // LEAD
        others_of_core_0 = [message(OTHER, lead, 1, LEAD, 0), message(OTHER, lead + 1, (chunks - FIRST[0]) * CHUNK // LEAD - 1, LEAD, 1)]
        if c == 0:
            same = [here(SAME)]
            other = others_of_core_0
            other_arrives = [message(OTHER, other_first, chunks - other_first)]
            relays = []
            relays_arrive = [relay(held, late, r_send, r_recv, 0, other_first)]
        else:
            same = [here(SAME_KV), here(SAME_Q)]
            other = [here(OTHER)]
            other_arrives = others_of_core_0
            relays = [relay(held, late, r_send, r_recv, 0, first)]
            relays_arrive = []
        onward = relay(late, late, r_send, r_recv, first, chunks - first)
        relays_arrive.append(relay(late, late, r_send, r_recv, other_first, chunks - other_first))

        same[0].start()
        if c == 0:
            pl.semaphore_wait(answer, 2)
        else:
            signal(answer, at.mate)
            signal(answer, at.far_mate)
        for copy in other + relays:
            copy.start()
        same[0].wait_recv()
        onward.start()
        if c == 1:
            other_arrives[0].wait_recv()
            same[1].start()
        for copy in relays_arrive + other_arrives[c:] + same[1:]:
            copy.wait_recv()
        for copy in relays + [onward] + same + other:
            copy.wait_send()

    by_core(at, body)


def late_chunks(core, held):
    first, other, relayed = FIRST[core], FIRST[1 - core], core * FIRST[0]
    spans = [(o, LATE_FAR, first) for o in (K, V, Q)] + [(Q, LATE_FAR_MATE, other)] + [(o, LATE_FAR_MATE, relayed) for o in (K, V)]
    return [(o, block, 0, n) if held else (o, block, n, None) for o, block, n in spans]


def store_chunks(at, source, outs, sems, core, held):
    rows = source.shape[1] // 2
    owners = tuple(at.across(device) for device in (at.far, at.far_mate))
    copies = []
    for j, (o, block, start, count) in enumerate(late_chunks(core, held)):
        count = (rows // CHUNK - start if count is None else count) * CHUNK
        if count:
            copies.append(pltpu.make_async_copy(
                source.at[o, pl.ds(block * rows + start * CHUNK, count), :],
                outs[o].at[pl.ds(pl.multiple_of(owners[block] * rows + start * CHUNK, CHUNK), count), :],
                sems.at[j],
            ))
    return copies


def run(copies):
    for copy in copies:
        copy.start()
    for copy in copies:
        copy.wait()


def store_early(early, held, q_out, k_out, v_out, token, sems, held_sems):
    at = Place()
    owners = (at.me, at.side, at.mate, at.across(at.mate), at.far, at.far_mate)
    rows = early.shape[1] // len(owners)
    outs = (k_out, v_out, q_out)
    for core in range(2):
        @pl.when(at.core == core)
        def _():
            run([
                pltpu.make_async_copy(early.at[o, pl.ds(block * rows, rows), :], out.at[span(owner, rows), :], sems.at[o, block])
                for o, out in enumerate(outs)
                for block, owner in enumerate(owners)
            ] + store_chunks(at, held, outs, held_sems, core, True))


def store_late(late, q_in, k_in, v_in, q_out, k_out, v_out, sems):
    at = Place()
    for core in range(2):
        @pl.when(at.core == core)
        def _():
            run(store_chunks(at, late, (k_out, v_out, q_out), sems, core, False))


def in_vmem(*arrays):
    return tuple(pltpu.with_memory_space_constraint(array, pltpu.VMEM) for array in arrays)


def solution(mesh):
    group_size = mesh.shape["tp"]

    def local_step(x_rows, norm_gain, w_q, w_k, w_v):
        rows, width = x_rows.shape
        head = w_q.shape[2]
        chunks = rows // CHUNK
        dma = pltpu.SemaphoreType.DMA
        any_space = pl.BlockSpec(memory_space=pl.ANY)
        vmem = pl.BlockSpec(memory_space=pltpu.VMEM)
        hbm = pl.BlockSpec(memory_space=pltpu.HBM)

        def small(**settings):
            return pltpu.CompilerParams(vmem_limit_bytes=1024 * 1024, **settings)

        early = pltpu.VMEM((3, 6 * rows, head), jnp.bfloat16)
        late = pltpu.VMEM((3, 2 * rows, head), jnp.bfloat16)
        final = [pltpu.HBM((group_size * rows, head), jnp.bfloat16)] * 3
        side_chunks = rows // SIDE_CHUNK

        gathered, held, far_late = in_vmem(*pl.pallas_call(
            gather,
            out_shape=[early, late, pltpu.VMEM((4, rows, head), jnp.bfloat16)],
            in_specs=[any_space] * 5,
            out_specs=[vmem] * 3,
            scratch_shapes=[
                pltpu.VMEM((rows, width), jnp.bfloat16),
                pltpu.VMEM((rows, width), jnp.bfloat16),
                pltpu.VMEM((width, 4 * head), jnp.bfloat16),
                pltpu.VMEM((width, 4 * head), jnp.bfloat16),
                pltpu.VMEM((4, rows, head), jnp.bfloat16),
                pltpu.VMEM((2 * rows, head), jnp.bfloat16),
                pltpu.VMEM((width,), jnp.float32),
                *[pltpu.SemaphoreType.REGULAR] * 3, dma(()), dma((chunks,)),
                *[dma((4,))] * 7,
                dma((side_chunks,)), dma((side_chunks,)), dma((2, chunks)), dma((2, chunks)), dma((2, side_chunks)), dma((2, side_chunks)),
                dma((3, chunks)), dma((3, chunks)), dma((2, chunks)), dma((2, chunks)), dma((chunks,)), dma((chunks,)), dma((1,)), dma((1,)),
            ],
            compiler_params=pltpu.CompilerParams(collective_id=0, has_side_effects=True, vmem_limit_bytes=40 * 1024 * 1024),
            name="gather",
        )(x_rows, norm_gain, w_q.reshape(width, head), w_k, w_v))
        *stored, token = pl.pallas_call(
            store_early,
            out_shape=final + [pltpu.HBM((8, 128), jnp.float32)],
            in_specs=[vmem] * 2,
            out_specs=[hbm] * 4,
            scratch_shapes=[dma((3, 6)), dma((6,))],
            compiler_params=small(),
            name="store_early",
        )(gathered, held)
        finished = pl.pallas_call(
            finish,
            out_shape=late,
            in_specs=[vmem] * 2 + [hbm],
            out_specs=vmem,
            scratch_shapes=[pltpu.SemaphoreType.REGULAR, dma((4, chunks)), dma((4, chunks)), dma((chunks,)), dma((chunks,))],
            compiler_params=small(collective_id=1, has_side_effects=True),
            name="finish",
        )(held, far_late, pltpu.with_memory_space_constraint(token, pltpu.HBM))
        outs = pl.pallas_call(
            store_late,
            out_shape=final,
            in_specs=[vmem] + [hbm] * 3,
            out_specs=[hbm] * 3,
            input_output_aliases={1: 0, 2: 1, 3: 2},
            scratch_shapes=[dma((6,))],
            compiler_params=small(),
            name="store_late",
        )(*in_vmem(finished), *stored)
        return tuple(out[:, None, :] for out in outs)

    return jax.shard_map(local_step, mesh=mesh, in_specs=(P(("dp", "tp"), None), P(None), P(None, "tp", None), P(None, "tp"), P(None, "tp")), out_specs=(P("dp", "tp", None), P("dp", "tp", None), P("dp", "tp", None)), check_vma=False)
```

```python
import functools

import jax
import jax.numpy as jnp
from jax import lax
from jax.experimental import pallas as pl
from jax.experimental.pallas import tpu as pltpu
from jax.sharding import PartitionSpec as P

EPSILON = 1e-6
CHUNK = 256
SIDE_CHUNK = 128
PIECE = 16
DETOUR = 32

K, V, Q = range(3)
KV, KVQ = pl.ds(0, 2), pl.ds(0, 3)
Q_SAME, Q_OTHER = 2, 3
OWN, SIDE, MATE, MATE_SIDE, FAR, FAR_MATE = range(6)
LATE_FAR, LATE_FAR_MATE = range(2)


class Place:
    def __init__(self):
        self.me = lax.axis_index("tp")
        self.core = lax.rem(self.me, 2)
        self.row = self.me // 4
        self.mate = self.me + 1 - 2 * self.core
        self.side = self.across(self.me)
        self.far = self.me + 2 - 4 * lax.rem(self.me // 2, 2)
        self.far_mate = self.far + 1 - 2 * self.core
        self.first = FIRST[0] + (FIRST[1] - FIRST[0]) * self.core
        self.first_other = FIRST[0] + FIRST[1] - self.first

    def across(self, device):
        return device + 4 - 8 * (device // 4)


def send(src, dst, send_sem, recv_sem, to):
    return pltpu.make_async_remote_copy(src_ref=src, dst_ref=dst, send_sem=send_sem, recv_sem=recv_sem, device_id={"tp": to})


def signal(sem, to):
    pl.semaphore_signal(sem, inc=1, device_id={"tp": to})


def loop(start, stop, body):
    def step(i, carry):
        body(i)
        return carry

    lax.fori_loop(start, stop, step, 0)


def span(i, size, base=0, count=1):
    return pl.ds(pl.multiple_of(base + i * size, size), count * size)


def by_core(at, body):
    for core in range(2):
        pl.when(at.core == core)(functools.partial(body, core))


SAME, OTHER = range(2)
FIRST = (1, 3)


def side_message(at, rows, stage, target, send_sems, recv_sems, kind, i, count=1):
    src, dst, block, peer = ((KVQ, KVQ, LATE_FAR, at.far), (Q_OTHER, Q, LATE_FAR_MATE, at.far_mate))[kind]
    return send(stage.at[src, span(i, CHUNK, 0, count), :], target.at[dst, span(i, CHUNK, block * rows, count), :],
                send_sems.at[kind, i], recv_sems.at[kind, i], peer)


def late_relay(at, rows, source, target, send_sems, recv_sems, i, count=1):
    return send(source.at[KV, span(i, CHUNK, LATE_FAR * rows, count), :], target.at[KV, span(i, CHUNK, LATE_FAR_MATE * rows, count), :],
                send_sems.at[i], recv_sems.at[i], at.mate)


def gather(x_hbm, gain_hbm, wq_hbm, wk_hbm, wv_hbm, early, late, far_late,
           x_own, x_side, w_own, w_far, far_own, mate_q, gain, detoured,
           mate_answer, side_answer, far_answer, aside_send, aside_recv, across_send, across_recv, load_gain, load_x, lw_sem, mw_send, mw_recv, fw_send, fw_recv, rw_send, rw_recv,
           x_send, x_recv, mo_send, mo_recv, ms_send, ms_recv, fo_send, fo_recv, fs_send, fs_recv, r_send, r_recv, lr_send, lr_recv):
    rows, width = x_hbm.shape
    head = wq_hbm.shape[1]
    part = wk_hbm.shape[1]
    chunks = rows // CHUNK
    side_chunks = rows // SIDE_CHUNK
    at = Place()
    core = at.core

    barrier = pltpu.get_barrier_semaphore()
    signal(barrier, at.far)

    @pl.when(core == 1)
    def _():
        signal(barrier, at.mate)

    @pl.when(at.row == 0)
    def _():
        signal(barrier, at.side)

    q_cols = pl.ds(pl.multiple_of(core * head, head), head)
    k_cols = pl.ds(pl.multiple_of(2 * head + core * part, part), part)
    v_cols = pl.ds(pl.multiple_of(3 * head + core * part, part), part)
    lead = width // 4
    mine = (
        (wk_hbm, pl.ds(0, lead), k_cols),
        (wk_hbm, pl.ds(lead, width - lead), k_cols),
        (wv_hbm, pl.ds(0, width), v_cols),
        (wq_hbm, pl.ds(0, width - DETOUR), q_cols),
        (wq_hbm, pl.ds(width - DETOUR, DETOUR), q_cols),
    )
    load_w, mate_w, far_w, relay_w = [], [], [], []
    for i, (src, depth, cols) in enumerate(mine):
        near_part, far_part = w_own.at[depth, cols], w_far.at[depth, cols]
        load_w.append(pltpu.make_async_copy(src.at[depth, :], near_part, lw_sem.at[i]))
        mate_w.append(send(near_part, near_part, mw_send.at[i], mw_recv.at[i], at.mate))
        far_w.append(send(near_part, far_part, fw_send.at[i], fw_recv.at[i], at.far))
        relay_w.append(send(far_part, far_part, rw_send.at[i], rw_recv.at[i], at.mate))

    def load_chunk(i):
        return pltpu.make_async_copy(x_hbm.at[span(i, CHUNK), :], x_own.at[span(i, CHUNK), :], load_x.at[i])

    def side_chunk(i):
        return send(x_hbm.at[span(i, SIDE_CHUNK), :], x_side.at[span(i, SIDE_CHUNK), :], x_send.at[i], x_recv.at[i], at.side)

    for copy in load_w:
        copy.start()

    last = w_own.at[mine[4][1], q_cols]
    aside = send(last, detoured, aside_send, aside_recv, at.side)
    across = send(detoured, w_far.at[mine[4][1], q_cols], across_send, across_recv, at.across(at.far))

    pl.semaphore_wait(barrier, 2 - core + at.row)
    for load, copy in zip(load_w[:3], far_w[:3]):
        load.wait()
        copy.start()
    for load in load_w[3:]:
        load.wait()

    @pl.when(at.row == 0)
    def _():
        far_w[3].start()

    @pl.when(core == 0)
    def _():
        signal(mate_answer, at.mate)

    @pl.when(at.row == 1)
    def _():
        signal(side_answer, at.side)

    gain_copy = pltpu.make_async_copy(gain_hbm, gain, load_gain)
    gain_copy.start()
    for i in range(chunks):
        load_chunk(i).start()

    @pl.when(core == 1)
    def _():
        pl.semaphore_wait(mate_answer, 1)

    signal(far_answer, at.far)
    for copy in mate_w:
        copy.start()

    @pl.when(at.row == 0)
    def _():
        pl.semaphore_wait(side_answer, 1)
        aside.start()

    loop(0, side_chunks, lambda i: side_chunk(i).start())

    @pl.when(at.row == 1)
    def _():
        aside.wait_recv()
        across.start()
        for copy in far_w[3:]:
            copy.start()

    def normalise(ref, i, size):
        def piece(p, carry):
            here = pl.ds(pl.multiple_of(i * size + p * PIECE, PIECE), PIECE)
            x_wide = ref[here, :].astype(jnp.float32)
            mean_sq = jnp.mean(x_wide * x_wide, axis=-1, keepdims=True)
            ref[here, :] = (x_wide * lax.rsqrt(mean_sq + EPSILON) * gain[...].reshape(1, width)).astype(jnp.bfloat16)
            return carry

        lax.fori_loop(0, size // PIECE, piece, 0, unroll=4)

    def product(ref, here, w, block):
        cols = slice(block * head, (block + 1) * head) if isinstance(block, int) else pl.ds(pl.multiple_of(block * head, head), head)
        return jnp.dot(ref[here, :], w[:, cols], preferred_element_type=jnp.float32).astype(jnp.bfloat16)

    def mate_copies(block, i):
        size, sends, recvs = (SIDE_CHUNK, ms_send, ms_recv) if block == SIDE else (CHUNK, mo_send, mo_recv)
        here, there = span(i, size, block * rows), span(i, size, (MATE + block) * rows)
        return (
            send(early.at[KV, here, :], early.at[KV, there, :], sends.at[0, i], recvs.at[0, i], at.mate),
            send(mate_q.at[here, :], early.at[Q, there, :], sends.at[1, i], recvs.at[1, i], at.mate),
        )

    def near_products(ref, block, i):
        size = SIDE_CHUNK if block == SIDE else CHUNK
        here, source = span(i, size, block * rows), span(i, size)
        early[K, here, :] = product(ref, source, w_own, 2)
        early[V, here, :] = product(ref, source, w_own, 3)
        early[Q, here, :] = product(ref, source, w_own, core)
        mate_q[here, :] = product(ref, source, w_own, 1 - core)
        for copy in mate_copies(block, i):
            copy.start()

    far_columns = {K: 2, V: 3, Q_SAME: core, Q_OTHER: 1 - core}

    def far_products(ref, here, stage, kinds):
        for kind in kinds:
            stage[kind, here, :] = product(ref, here, w_far, far_columns[kind])

    def own_message(j, i):
        src, dst, block, peer = ((KV, KV, FAR, at.far), (Q_SAME, Q, FAR, at.far), (Q_OTHER, Q, FAR_MATE, at.far_mate))[j]
        return send(far_own.at[src, span(i, CHUNK), :], early.at[dst, span(i, CHUNK, block * rows), :], fo_send.at[j, i], fo_recv.at[j, i], peer)

    message = functools.partial(side_message, at, rows, far_late, late, fs_send, fs_recv)

    def relay(i):
        return send(early.at[KV, span(i, CHUNK, FAR * rows), :], early.at[KV, span(i, CHUNK, FAR_MATE * rows), :], r_send.at[i], r_recv.at[i], at.mate)

    def own_norm(i):
        load_chunk(i).wait()
        normalise(x_own, i, CHUNK)

    gain_copy.wait()
    loop(0, chunks, own_norm)
    for copy in mate_w:
        copy.wait_recv()
    loop(0, chunks, lambda i: near_products(x_own, OWN, i))

    for arrived, onward in zip(far_w[:3], relay_w[:3]):
        arrived.wait_recv()
        onward.start()
    for copy in relay_w[:3]:
        copy.wait_recv()

    def far_kv_step(i):
        far_products(x_own, span(i, CHUNK), far_own, (K, V))
        own_message(0, i).start()

    loop(0, chunks, far_kv_step)
    far_w[3].wait_recv()
    relay_w[3].start()

    @pl.when(at.row == 0)
    def _():
        across.wait_recv()

    @pl.when(at.row == 1)
    def _():
        far_w[4].wait_recv()

    relay_w[4].start()
    for copy in relay_w[3:]:
        copy.wait_recv()
    pl.semaphore_wait(far_answer, 1)

    def far_q_step(i):
        far_products(x_own, span(i, CHUNK), far_own, (Q_SAME, Q_OTHER))
        own_message(1, i).start()
        own_message(2, i).start()

    loop(0, chunks, far_q_step)

    def side_step(i):
        side_chunk(i).wait_recv()
        normalise(x_side, i, SIDE_CHUNK)
        near_products(x_side, SIDE, i)
        far_products(x_side, span(i, SIDE_CHUNK), far_late, (Q_OTHER, K, V, Q_SAME))
        done = lax.rem(i + 1, CHUNK // SIDE_CHUNK) == 0
        n = i // (CHUNK // SIDE_CHUNK)

        @pl.when(done & (n < at.first))
        def _():
            message(OTHER, n).start()

        @pl.when(done & (n == at.first - 1))
        def _():
            by_core(at, lambda c: message(SAME, 0, FIRST[c]).start())

    loop(0, side_chunks - 1, side_step)

    def relay_step(i):
        own_message(0, i).wait_recv()
        relay(i).start()

    loop(0, chunks, relay_step)

    def drain_own(i):
        for copy in mate_copies(OWN, i):
            copy.wait_send()
            copy.wait_recv()
        for j in range(3):
            own_message(j, i).wait_send()
        for j in (1, 2):
            own_message(j, i).wait_recv()
        relay(i).wait_send()
        relay(i).wait_recv()

    loop(0, chunks, drain_own)
    for copies in (mate_w, far_w[:4], relay_w):
        for copy in copies:
            copy.wait_send()

    @pl.when(at.row == 0)
    def _():
        aside.wait_send()

    @pl.when(at.row == 1)
    def _():
        across.wait_send()
        far_w[4].wait_send()

    side_step(side_chunks - 1)

    def drain_side(i):
        side_chunk(i).wait_send()
        for copy in mate_copies(SIDE, i):
            copy.wait_send()
            copy.wait_recv()

    loop(0, side_chunks, drain_side)
    loop(0, at.first_other, lambda i: message(OTHER, i).wait_recv())
    loop(0, at.first, lambda i: message(OTHER, i).wait_send())

    def close(c):
        same = message(SAME, 0, FIRST[c])
        same.wait_recv()
        onward = late_relay(at, rows, late, late, lr_send, lr_recv, 0, FIRST[0])
        if c == 0:
            onward.start()
            onward.wait_send()
        else:
            onward.wait_recv()
        same.wait_send()

    by_core(at, close)


def finish(held, far_late, token, late, answer, fs_send, fs_recv, r_send, r_recv):
    rows = far_late.shape[1]
    chunks = rows // CHUNK
    at = Place()
    barrier = pltpu.get_barrier_semaphore()
    signal(barrier, at.far)

    @pl.when(at.core == 0)
    def _():
        signal(barrier, at.mate)
        signal(barrier, at.far_mate)

    pl.semaphore_wait(barrier, 1 + 2 * at.core)
    message = functools.partial(side_message, at, rows, far_late, late, fs_send, fs_recv)
    relay = functools.partial(late_relay, at, rows)

    def body(c):
        first, other_first = FIRST[c], FIRST[1 - c]
        same, other = (message(kind, first, chunks - first) for kind in (SAME, OTHER))
        same.start()
        relays = [relay(held, late, r_send, r_recv, 0, first)] if c else []
        if c:
            signal(answer, at.mate)
            signal(answer, at.far_mate)
        else:
            pl.semaphore_wait(answer, 2)
        other.start()
        for copy in relays:
            copy.start()
        same.wait_recv()
        relays.append(relay(late, late, r_send, r_recv, first, chunks - first))
        relays[-1].start()
        if c == 0:
            relay(held, late, r_send, r_recv, 0, other_first).wait_recv()
        relay(late, late, r_send, r_recv, other_first, chunks - other_first).wait_recv()
        for copy in relays:
            copy.wait_send()
        same.wait_send()
        message(OTHER, other_first, chunks - other_first).wait_recv()
        other.wait_send()

    by_core(at, body)


def late_chunks(core, held):
    first, other, relayed = FIRST[core], FIRST[1 - core], core * FIRST[0]
    spans = [(o, LATE_FAR, first) for o in (K, V, Q)] + [(Q, LATE_FAR_MATE, other)] + [(o, LATE_FAR_MATE, relayed) for o in (K, V)]
    return [(o, block, 0, n) if held else (o, block, n, None) for o, block, n in spans]


def store_chunks(at, source, outs, sems, core, held):
    rows = source.shape[1] // 2
    owners = tuple(at.across(device) for device in (at.far, at.far_mate))
    copies = []
    for j, (o, block, start, count) in enumerate(late_chunks(core, held)):
        count = (rows // CHUNK - start if count is None else count) * CHUNK
        if count:
            copies.append(pltpu.make_async_copy(
                source.at[o, pl.ds(block * rows + start * CHUNK, count), :],
                outs[o].at[pl.ds(pl.multiple_of(owners[block] * rows + start * CHUNK, CHUNK), count), :],
                sems.at[j],
            ))
    return copies


def run(copies):
    for copy in copies:
        copy.start()
    for copy in copies:
        copy.wait()


def store_early(early, held, q_out, k_out, v_out, token, sems, held_sems):
    at = Place()
    owners = (at.me, at.side, at.mate, at.across(at.mate), at.far, at.far_mate)
    rows = early.shape[1] // len(owners)
    outs = (k_out, v_out, q_out)
    for core in range(2):
        @pl.when(at.core == core)
        def _():
            run([
                pltpu.make_async_copy(early.at[o, pl.ds(block * rows, rows), :], out.at[span(owner, rows), :], sems.at[o, block])
                for o, out in enumerate(outs)
                for block, owner in enumerate(owners)
            ] + store_chunks(at, held, outs, held_sems, core, True))


def store_late(late, q_in, k_in, v_in, q_out, k_out, v_out, sems):
    at = Place()
    for core in range(2):
        @pl.when(at.core == core)
        def _():
            run(store_chunks(at, late, (k_out, v_out, q_out), sems, core, False))


def in_vmem(*arrays):
    return tuple(pltpu.with_memory_space_constraint(array, pltpu.VMEM) for array in arrays)


def solution(mesh):
    group_size = mesh.shape["tp"]

    def local_step(x_rows, norm_gain, w_q, w_k, w_v):
        rows, width = x_rows.shape
        head = w_q.shape[2]
        chunks = rows // CHUNK
        dma = pltpu.SemaphoreType.DMA
        any_space = pl.BlockSpec(memory_space=pl.ANY)
        vmem = pl.BlockSpec(memory_space=pltpu.VMEM)
        hbm = pl.BlockSpec(memory_space=pltpu.HBM)

        def small(**settings):
            return pltpu.CompilerParams(vmem_limit_bytes=1024 * 1024, **settings)

        early = pltpu.VMEM((3, 6 * rows, head), jnp.bfloat16)
        late = pltpu.VMEM((3, 2 * rows, head), jnp.bfloat16)
        final = [pltpu.HBM((group_size * rows, head), jnp.bfloat16)] * 3
        side_chunks = rows // SIDE_CHUNK

        gathered, held, far_late = in_vmem(*pl.pallas_call(
            gather,
            out_shape=[early, late, pltpu.VMEM((4, rows, head), jnp.bfloat16)],
            in_specs=[any_space] * 5,
            out_specs=[vmem] * 3,
            scratch_shapes=[
                pltpu.VMEM((rows, width), jnp.bfloat16),
                pltpu.VMEM((rows, width), jnp.bfloat16),
                pltpu.VMEM((width, 4 * head), jnp.bfloat16),
                pltpu.VMEM((width, 4 * head), jnp.bfloat16),
                pltpu.VMEM((4, rows, head), jnp.bfloat16),
                pltpu.VMEM((2 * rows, head), jnp.bfloat16),
                pltpu.VMEM((width,), jnp.float32),
                pltpu.VMEM((DETOUR, head), jnp.bfloat16),
                *[pltpu.SemaphoreType.REGULAR] * 3, *[dma(())] * 5, dma((chunks,)),
                *[dma((5,))] * 7,
                dma((side_chunks,)), dma((side_chunks,)), dma((2, chunks)), dma((2, chunks)), dma((2, side_chunks)), dma((2, side_chunks)),
                dma((3, chunks)), dma((3, chunks)), dma((2, chunks)), dma((2, chunks)), dma((chunks,)), dma((chunks,)), dma((1,)), dma((1,)),
            ],
            compiler_params=pltpu.CompilerParams(collective_id=0, has_side_effects=True, vmem_limit_bytes=40 * 1024 * 1024),
            name="gather",
        )(x_rows, norm_gain, w_q.reshape(width, head), w_k, w_v))
        *stored, token = pl.pallas_call(
            store_early,
            out_shape=final + [pltpu.HBM((8, 128), jnp.float32)],
            in_specs=[vmem] * 2,
            out_specs=[hbm] * 4,
            scratch_shapes=[dma((3, 6)), dma((6,))],
            compiler_params=small(),
            name="store_early",
        )(gathered, held)
        finished = pl.pallas_call(
            finish,
            out_shape=late,
            in_specs=[vmem] * 2 + [hbm],
            out_specs=vmem,
            scratch_shapes=[pltpu.SemaphoreType.REGULAR, dma((2, chunks)), dma((2, chunks)), dma((chunks,)), dma((chunks,))],
            compiler_params=small(collective_id=1, has_side_effects=True),
            name="finish",
        )(held, far_late, pltpu.with_memory_space_constraint(token, pltpu.HBM))
        outs = pl.pallas_call(
            store_late,
            out_shape=final,
            in_specs=[vmem] + [hbm] * 3,
            out_specs=[hbm] * 3,
            input_output_aliases={1: 0, 2: 1, 3: 2},
            scratch_shapes=[dma((6,))],
            compiler_params=small(),
            name="store_late",
        )(*in_vmem(finished), *stored)
        return tuple(out[:, None, :] for out in outs)

    return jax.shard_map(local_step, mesh=mesh, in_specs=(P(("dp", "tp"), None), P(None), P(None, "tp", None), P(None, "tp"), P(None, "tp")), out_specs=(P("dp", "tp", None), P("dp", "tp", None), P("dp", "tp", None)), check_vma=False)
```

```python
import functools

import jax
import jax.numpy as jnp
from jax import lax
from jax.experimental import pallas as pl
from jax.experimental.pallas import tpu as pltpu
from jax.sharding import PartitionSpec as P

EPSILON = 1e-6
CHUNK = 256
SIDE_CHUNK = 128
PIECE = 16
DETOUR = 32

K, V, Q = range(3)
KV, KVQ = pl.ds(0, 2), pl.ds(0, 3)
Q_SAME, Q_OTHER = 2, 3
OWN, SIDE, MATE, MATE_SIDE, FAR, FAR_MATE = range(6)
LATE_FAR, LATE_FAR_MATE = range(2)


class Place:
    def __init__(self):
        self.me = lax.axis_index("tp")
        self.core = lax.rem(self.me, 2)
        self.row = self.me // 4
        self.mate = self.me + 1 - 2 * self.core
        self.side = self.across(self.me)
        self.far = self.me + 2 - 4 * lax.rem(self.me // 2, 2)
        self.far_mate = self.far + 1 - 2 * self.core
        self.first = FIRST[0] + (FIRST[1] - FIRST[0]) * self.core
        self.first_other = FIRST[0] + FIRST[1] - self.first

    def across(self, device):
        return device + 4 - 8 * (device // 4)


def send(src, dst, send_sem, recv_sem, to):
    return pltpu.make_async_remote_copy(src_ref=src, dst_ref=dst, send_sem=send_sem, recv_sem=recv_sem, device_id={"tp": to})


def signal(sem, to):
    pl.semaphore_signal(sem, inc=1, device_id={"tp": to})


def loop(start, stop, body):
    def step(i, carry):
        body(i)
        return carry

    lax.fori_loop(start, stop, step, 0)


def span(i, size, base=0, count=1):
    return pl.ds(pl.multiple_of(base + i * size, size), count * size)


def by_core(at, body):
    for core in range(2):
        pl.when(at.core == core)(functools.partial(body, core))


SAME, OTHER = range(2)
FIRST = (1, 3)


def side_message(at, rows, stage, target, send_sem, recv_sem, kind, i, count=1):
    src, dst, block, peer = ((KVQ, KVQ, LATE_FAR, at.far), (Q_OTHER, Q, LATE_FAR_MATE, at.far_mate))[kind]
    return send(stage.at[src, span(i, CHUNK, 0, count), :], target.at[dst, span(i, CHUNK, block * rows, count), :], send_sem, recv_sem, peer)


def late_relay(at, rows, source, target, send_sem, recv_sem, i, count=1):
    return send(source.at[KV, span(i, CHUNK, LATE_FAR * rows, count), :], target.at[KV, span(i, CHUNK, LATE_FAR_MATE * rows, count), :],
                send_sem, recv_sem, at.mate)


def gather(x_hbm, gain_hbm, wq_hbm, wk_hbm, wv_hbm, early, late, far_late,
           x_own, x_side, w_own, w_far, far_own, mate_q, gain, detoured,
           mate_answer, side_answer, far_answer, aside_send, aside_recv, across_send, across_recv, load_gain, load_x, lw_sem, mw_send, mw_recv, fw_send, fw_recv, rw_send, rw_recv,
           x_send, x_recv, mo_send, mo_recv, ms_send, ms_recv, fo_send, fo_recv, fs_send, fs_recv, r_send, r_recv, lr_send, lr_recv):
    rows, width = x_hbm.shape
    head = wq_hbm.shape[1]
    part = wk_hbm.shape[1]
    chunks = rows // CHUNK
    side_chunks = rows // SIDE_CHUNK
    at = Place()
    core = at.core

    barrier = pltpu.get_barrier_semaphore()
    signal(barrier, at.far)

    @pl.when(core == 1)
    def _():
        signal(barrier, at.mate)

    @pl.when(at.row == 0)
    def _():
        signal(barrier, at.side)

    q_cols = pl.ds(pl.multiple_of(core * head, head), head)
    k_cols = pl.ds(pl.multiple_of(2 * head + core * part, part), part)
    v_cols = pl.ds(pl.multiple_of(3 * head + core * part, part), part)
    lead = 6 * PIECE
    mine = (
        (wk_hbm, pl.ds(0, lead), k_cols),
        (wk_hbm, pl.ds(lead, width - lead), k_cols),
        (wv_hbm, pl.ds(0, width), v_cols),
        (wq_hbm, pl.ds(0, width - DETOUR), q_cols),
        (wq_hbm, pl.ds(width - DETOUR, DETOUR), q_cols),
    )
    load_w, mate_w, far_w, relay_w = [], [], [], []
    for i, (src, depth, cols) in enumerate(mine):
        near_part, far_part = w_own.at[depth, cols], w_far.at[depth, cols]
        load_w.append(pltpu.make_async_copy(src.at[depth, :], near_part, lw_sem.at[i]))
        mate_w.append(send(near_part, near_part, mw_send.at[i], mw_recv.at[i], at.mate))
        far_w.append(send(near_part, far_part, fw_send.at[i], fw_recv.at[i], at.far))
        relay_w.append(send(far_part, far_part, rw_send.at[i], rw_recv.at[i], at.mate))

    def load_chunk(i):
        return pltpu.make_async_copy(x_hbm.at[span(i, CHUNK), :], x_own.at[span(i, CHUNK), :], load_x.at[i])

    def side_chunk(i):
        return send(x_hbm.at[span(i, SIDE_CHUNK), :], x_side.at[span(i, SIDE_CHUNK), :], x_send.at[i], x_recv.at[i], at.side)

    for copy in load_w:
        copy.start()

    last = w_own.at[mine[4][1], q_cols]
    aside = send(last, detoured, aside_send, aside_recv, at.side)
    across = send(detoured, w_far.at[mine[4][1], q_cols], across_send, across_recv, at.across(at.far))

    pl.semaphore_wait(barrier, 2 - core + at.row)
    for load, copy in zip(load_w[:3], far_w[:3]):
        load.wait()
        copy.start()
    for load in load_w[3:]:
        load.wait()

    @pl.when(at.row == 0)
    def _():
        far_w[3].start()

    @pl.when(core == 0)
    def _():
        signal(mate_answer, at.mate)

    @pl.when(at.row == 1)
    def _():
        signal(side_answer, at.side)

    gain_copy = pltpu.make_async_copy(gain_hbm, gain, load_gain)
    gain_copy.start()
    for i in range(chunks):
        load_chunk(i).start()

    @pl.when(core == 1)
    def _():
        pl.semaphore_wait(mate_answer, 1)

    signal(far_answer, at.far)
    for copy in mate_w:
        copy.start()

    @pl.when(at.row == 0)
    def _():
        pl.semaphore_wait(side_answer, 1)
        aside.start()

    loop(0, side_chunks, lambda i: side_chunk(i).start())

    @pl.when(at.row == 1)
    def _():
        aside.wait_recv()
        across.start()
        for copy in far_w[3:]:
            copy.start()

    def normalise(ref, i, size):
        def piece(p, carry):
            here = pl.ds(pl.multiple_of(i * size + p * PIECE, PIECE), PIECE)
            x_wide = ref[here, :].astype(jnp.float32)
            mean_sq = jnp.mean(x_wide * x_wide, axis=-1, keepdims=True)
            ref[here, :] = (x_wide * lax.rsqrt(mean_sq + EPSILON) * gain[...].reshape(1, width)).astype(jnp.bfloat16)
            return carry

        lax.fori_loop(0, size // PIECE, piece, 0, unroll=4)

    def product(ref, here, w, block):
        cols = slice(block * head, (block + 1) * head) if isinstance(block, int) else pl.ds(pl.multiple_of(block * head, head), head)
        return jnp.dot(ref[here, :], w[:, cols], preferred_element_type=jnp.float32).astype(jnp.bfloat16)

    def mate_copies(block, i):
        size, sends, recvs = (SIDE_CHUNK, ms_send, ms_recv) if block == SIDE else (CHUNK, mo_send, mo_recv)
        here, there = span(i, size, block * rows), span(i, size, (MATE + block) * rows)
        return (
            send(early.at[KV, here, :], early.at[KV, there, :], sends.at[0, i], recvs.at[0, i], at.mate),
            send(mate_q.at[here, :], early.at[Q, there, :], sends.at[1, i], recvs.at[1, i], at.mate),
        )

    def near_products(ref, block, i):
        size = SIDE_CHUNK if block == SIDE else CHUNK
        here, source = span(i, size, block * rows), span(i, size)
        early[K, here, :] = product(ref, source, w_own, 2)
        early[V, here, :] = product(ref, source, w_own, 3)
        early[Q, here, :] = product(ref, source, w_own, core)
        mate_q[here, :] = product(ref, source, w_own, 1 - core)
        for copy in mate_copies(block, i):
            copy.start()

    far_columns = {K: 2, V: 3, Q_SAME: core, Q_OTHER: 1 - core}

    def far_products(ref, here, stage, kinds):
        for kind in kinds:
            stage[kind, here, :] = product(ref, here, w_far, far_columns[kind])

    def own_message(j, i):
        src, dst, block, peer = ((KV, KV, FAR, at.far), (Q_SAME, Q, FAR, at.far), (Q_OTHER, Q, FAR_MATE, at.far_mate))[j]
        return send(far_own.at[src, span(i, CHUNK), :], early.at[dst, span(i, CHUNK, block * rows), :], fo_send.at[j, i], fo_recv.at[j, i], peer)

    def message(kind, i, count=1):
        return side_message(at, rows, far_late, late, fs_send.at[kind, i], fs_recv.at[kind, i], kind, i, count)

    def relay(i):
        return send(early.at[KV, span(i, CHUNK, FAR * rows), :], early.at[KV, span(i, CHUNK, FAR_MATE * rows), :], r_send.at[i], r_recv.at[i], at.mate)

    def own_norm(i):
        load_chunk(i).wait()
        normalise(x_own, i, CHUNK)

    for copy in mate_w:
        copy.wait_recv()
    gain_copy.wait()
    loop(0, chunks, own_norm)
    loop(0, chunks, lambda i: near_products(x_own, OWN, i))

    for arrived, onward in zip(far_w[:3], relay_w[:3]):
        arrived.wait_recv()
        onward.start()
    for copy in relay_w[:3]:
        copy.wait_recv()

    def far_kv_step(i):
        far_products(x_own, span(i, CHUNK), far_own, (K, V))
        own_message(0, i).start()

    loop(0, chunks, far_kv_step)
    far_w[3].wait_recv()
    relay_w[3].start()

    @pl.when(at.row == 0)
    def _():
        across.wait_recv()

    @pl.when(at.row == 1)
    def _():
        far_w[4].wait_recv()

    relay_w[4].start()
    for copy in relay_w[3:]:
        copy.wait_recv()
    pl.semaphore_wait(far_answer, 1)

    def far_q_step(i):
        far_products(x_own, span(i, CHUNK), far_own, (Q_SAME, Q_OTHER))
        own_message(1, i).start()
        own_message(2, i).start()

    loop(0, chunks, far_q_step)

    def side_step(i):
        side_chunk(i).wait_recv()
        normalise(x_side, i, SIDE_CHUNK)
        near_products(x_side, SIDE, i)
        far_products(x_side, span(i, SIDE_CHUNK), far_late, (Q_OTHER, K, V, Q_SAME))
        done = lax.rem(i + 1, CHUNK // SIDE_CHUNK) == 0
        n = i // (CHUNK // SIDE_CHUNK)

        @pl.when(done & (n < at.first))
        def _():
            message(OTHER, n).start()

        @pl.when(done & (n == at.first - 1))
        def _():
            by_core(at, lambda c: message(SAME, 0, FIRST[c]).start())

    loop(0, side_chunks - 1, side_step)

    def relay_step(i):
        own_message(0, i).wait_recv()
        relay(i).start()

    loop(0, chunks, relay_step)

    def drain_own(i):
        for copy in mate_copies(OWN, i):
            copy.wait_send()
            copy.wait_recv()
        for j in range(3):
            own_message(j, i).wait_send()
        for j in (1, 2):
            own_message(j, i).wait_recv()
        relay(i).wait_send()
        relay(i).wait_recv()

    loop(0, chunks, drain_own)
    for copies in (mate_w, far_w[:4], relay_w):
        for copy in copies:
            copy.wait_send()

    @pl.when(at.row == 0)
    def _():
        aside.wait_send()

    @pl.when(at.row == 1)
    def _():
        across.wait_send()
        far_w[4].wait_send()

    side_step(side_chunks - 1)

    def drain_side(i):
        side_chunk(i).wait_send()
        for copy in mate_copies(SIDE, i):
            copy.wait_send()
            copy.wait_recv()

    loop(0, side_chunks, drain_side)
    loop(0, at.first_other, lambda i: message(OTHER, i).wait_recv())
    loop(0, at.first, lambda i: message(OTHER, i).wait_send())

    def close(c):
        same = message(SAME, 0, FIRST[c])
        same.wait_recv()
        onward = late_relay(at, rows, late, late, lr_send, lr_recv, 0, FIRST[0])
        if c == 0:
            onward.start()
            onward.wait_send()
        else:
            onward.wait_recv()
        same.wait_send()

    by_core(at, close)


def finish(held, far_late, token, late, answer, send_sem, same_recv, other_recv, relay_recv):
    rows = far_late.shape[1]
    chunks = rows // CHUNK
    at = Place()
    barrier = pltpu.get_barrier_semaphore()
    signal(barrier, at.far)

    @pl.when(at.core == 0)
    def _():
        signal(barrier, at.mate)
        signal(barrier, at.far_mate)

    pl.semaphore_wait(barrier, 1 + 2 * at.core)
    def message(kind, i, count):
        return side_message(at, rows, far_late, late, send_sem, (same_recv, other_recv)[kind], kind, i, count)

    def relay(source, i, count):
        return late_relay(at, rows, source, late, send_sem, relay_recv, i, count)

    def body(c):
        first, other_first = FIRST[c], FIRST[1 - c]
        same, other = (message(kind, first, chunks - first) for kind in (SAME, OTHER))
        same.start()
        if c:
            signal(answer, at.mate)
            signal(answer, at.far_mate)
        else:
            pl.semaphore_wait(answer, 2)
        other.start()
        if c:
            relay(held, 0, first).start()
        same.wait_recv()
        relay(late, first, chunks - first).start()
        arrived = chunks if c == 0 else chunks - other_first
        relay(late, 0, arrived).wait_recv()
        message(OTHER, other_first, chunks - other_first).wait_recv()
        sent = 4 * (chunks - first) + 2 * (chunks if c else chunks - first)
        everything = late.at[KVQ, span(0, CHUNK, 0, sent // 3), :]
        pltpu.make_async_copy(everything, everything, send_sem).wait()

    by_core(at, body)


def late_chunks(core, held):
    first, other, relayed = FIRST[core], FIRST[1 - core], core * FIRST[0]
    spans = [(o, LATE_FAR, first) for o in (K, V, Q)] + [(Q, LATE_FAR_MATE, other)] + [(o, LATE_FAR_MATE, relayed) for o in (K, V)]
    return [(o, block, 0, n) if held else (o, block, n, None) for o, block, n in spans]


def store_chunks(at, source, outs, sem, core, held):
    rows = source.shape[1] // 2
    owners = tuple(at.across(device) for device in (at.far, at.far_mate))
    copies = []
    for o, block, start, count in late_chunks(core, held):
        count = (rows // CHUNK - start if count is None else count) * CHUNK
        if count:
            copies.append(pltpu.make_async_copy(
                source.at[o, pl.ds(block * rows + start * CHUNK, count), :],
                outs[o].at[pl.ds(pl.multiple_of(owners[block] * rows + start * CHUNK, CHUNK), count), :],
                sem,
            ))
    return copies


def run(copies):
    for copy in copies:
        copy.start()
    for copy in copies:
        copy.wait()


def store_early(early, held, q_out, k_out, v_out, token, sem):
    at = Place()
    owners = (at.me, at.side, at.mate, at.across(at.mate), at.far, at.far_mate)
    rows = early.shape[1] // len(owners)
    outs = (k_out, v_out, q_out)
    for core in range(2):
        @pl.when(at.core == core)
        def _():
            run([
                pltpu.make_async_copy(early.at[o, pl.ds(block * rows, rows), :], out.at[span(owner, rows), :], sem)
                for o, out in enumerate(outs)
                for block, owner in enumerate(owners)
            ] + store_chunks(at, held, outs, sem, core, True))


def store_late(late, q_in, k_in, v_in, q_out, k_out, v_out, sem):
    at = Place()
    for core in range(2):
        @pl.when(at.core == core)
        def _():
            run(store_chunks(at, late, (k_out, v_out, q_out), sem, core, False))


def in_vmem(*arrays):
    return tuple(pltpu.with_memory_space_constraint(array, pltpu.VMEM) for array in arrays)


def solution(mesh):
    group_size = mesh.shape["tp"]

    def local_step(x_rows, norm_gain, w_q, w_k, w_v):
        rows, width = x_rows.shape
        head = w_q.shape[2]
        chunks = rows // CHUNK
        dma = pltpu.SemaphoreType.DMA
        any_space = pl.BlockSpec(memory_space=pl.ANY)
        vmem = pl.BlockSpec(memory_space=pltpu.VMEM)
        hbm = pl.BlockSpec(memory_space=pltpu.HBM)

        def small(**settings):
            return pltpu.CompilerParams(vmem_limit_bytes=1024 * 1024, **settings)

        early = pltpu.VMEM((3, 6 * rows, head), jnp.bfloat16)
        late = pltpu.VMEM((3, 2 * rows, head), jnp.bfloat16)
        final = [pltpu.HBM((group_size * rows, head), jnp.bfloat16)] * 3
        side_chunks = rows // SIDE_CHUNK

        gathered, held, far_late = in_vmem(*pl.pallas_call(
            gather,
            out_shape=[early, late, pltpu.VMEM((4, rows, head), jnp.bfloat16)],
            in_specs=[any_space] * 5,
            out_specs=[vmem] * 3,
            scratch_shapes=[
                pltpu.VMEM((rows, width), jnp.bfloat16),
                pltpu.VMEM((rows, width), jnp.bfloat16),
                pltpu.VMEM((width, 4 * head), jnp.bfloat16),
                pltpu.VMEM((width, 4 * head), jnp.bfloat16),
                pltpu.VMEM((4, rows, head), jnp.bfloat16),
                pltpu.VMEM((2 * rows, head), jnp.bfloat16),
                pltpu.VMEM((width,), jnp.float32),
                pltpu.VMEM((DETOUR, head), jnp.bfloat16),
                *[pltpu.SemaphoreType.REGULAR] * 3, *[dma(())] * 5, dma((chunks,)),
                *[dma((5,))] * 7,
                dma((side_chunks,)), dma((side_chunks,)), dma((2, chunks)), dma((2, chunks)), dma((2, side_chunks)), dma((2, side_chunks)),
                dma((3, chunks)), dma((3, chunks)), dma((2, chunks)), dma((2, chunks)), dma((chunks,)), dma((chunks,)), dma(()), dma(()),
            ],
            compiler_params=pltpu.CompilerParams(collective_id=0, has_side_effects=True, vmem_limit_bytes=40 * 1024 * 1024),
            name="gather",
        )(x_rows, norm_gain, w_q.reshape(width, head), w_k, w_v))
        *stored, token = pl.pallas_call(
            store_early,
            out_shape=final + [pltpu.HBM((8, 128), jnp.float32)],
            in_specs=[vmem] * 2,
            out_specs=[hbm] * 4,
            scratch_shapes=[dma(())],
            compiler_params=small(),
            name="store_early",
        )(gathered, held)
        finished = pl.pallas_call(
            finish,
            out_shape=late,
            in_specs=[vmem] * 2 + [hbm],
            out_specs=vmem,
            scratch_shapes=[pltpu.SemaphoreType.REGULAR] + [dma(())] * 4,
            compiler_params=small(collective_id=1, has_side_effects=True),
            name="finish",
        )(held, far_late, pltpu.with_memory_space_constraint(token, pltpu.HBM))
        outs = pl.pallas_call(
            store_late,
            out_shape=final,
            in_specs=[vmem] + [hbm] * 3,
            out_specs=[hbm] * 3,
            input_output_aliases={1: 0, 2: 1, 3: 2},
            scratch_shapes=[dma(())],
            compiler_params=small(),
            name="store_late",
        )(*in_vmem(finished), *stored)
        return tuple(out[:, None, :] for out in outs)

    return jax.shard_map(local_step, mesh=mesh, in_specs=(P(("dp", "tp"), None), P(None), P(None, "tp", None), P(None, "tp"), P(None, "tp")), out_specs=(P("dp", "tp", None), P("dp", "tp", None), P("dp", "tp", None)), check_vma=False)
```

```python
import functools

import jax
import jax.numpy as jnp
from jax import lax
from jax.experimental import pallas as pl
from jax.experimental.pallas import tpu as pltpu
from jax.sharding import PartitionSpec as P

EPSILON = 1e-6
CHUNK = 256
SIDE_CHUNK = 128
PIECE = 16
DETOUR = 32

K, V, Q = range(3)
KV, KVQ = pl.ds(0, 2), pl.ds(0, 3)
Q_SAME, Q_OTHER = 2, 3
OWN, SIDE, MATE, MATE_SIDE, FAR, FAR_MATE = range(6)
LATE_FAR, LATE_FAR_MATE = range(2)


class Place:
    def __init__(self):
        self.me = lax.axis_index("tp")
        self.core = lax.rem(self.me, 2)
        self.row = self.me // 4
        self.column = lax.rem(self.me // 2, 2)
        self.mate = self.me + 1 - 2 * self.core
        self.side = self.across(self.me)
        self.far = self.me + 2 - 4 * lax.rem(self.me // 2, 2)
        self.far_mate = self.far + 1 - 2 * self.core
        self.first = FIRST[0] + (FIRST[1] - FIRST[0]) * self.core
        self.first_other = FIRST[0] + FIRST[1] - self.first

    def across(self, device):
        return device + 4 - 8 * (device // 4)


def send(src, dst, send_sem, recv_sem, to):
    return pltpu.make_async_remote_copy(src_ref=src, dst_ref=dst, send_sem=send_sem, recv_sem=recv_sem, device_id={"tp": to})


def signal(sem, to):
    pl.semaphore_signal(sem, inc=1, device_id={"tp": to})


def loop(start, stop, body):
    def step(i, carry):
        body(i)
        return carry

    lax.fori_loop(start, stop, step, 0)


def span(i, size, base=0, count=1):
    return pl.ds(pl.multiple_of(base + i * size, size), count * size)


def by_core(at, body):
    for core in range(2):
        pl.when(at.core == core)(functools.partial(body, core))


SAME, OTHER = range(2)
FIRST = (1, 3)


def side_message(at, rows, stage, target, send_sem, recv_sem, kind, i, count=1):
    src, dst, block, peer = ((KVQ, KVQ, LATE_FAR, at.far), (Q_OTHER, Q, LATE_FAR_MATE, at.far_mate))[kind]
    return send(stage.at[src, span(i, CHUNK, 0, count), :], target.at[dst, span(i, CHUNK, block * rows, count), :], send_sem, recv_sem, peer)


def late_relay(at, rows, source, target, send_sem, recv_sem, i, count=1):
    return send(source.at[KV, span(i, CHUNK, LATE_FAR * rows, count), :], target.at[KV, span(i, CHUNK, LATE_FAR_MATE * rows, count), :],
                send_sem, recv_sem, at.mate)


def gather(x_hbm, gain_hbm, wq_hbm, wk_hbm, wv_hbm, early, late, far_late,
           x_own, x_side, w_own, w_far, far_own, mate_q, gain, detoured,
           mate_answer, side_answer, far_answer, aside_send, aside_recv, across_send, across_recv, load_gain, load_x, lw_sem, mw_send, mw_recv, fw_send, fw_recv, rw_send, rw_recv,
           x_send, x_recv, mo_send, mo_recv, ms_send, ms_recv, fo_send, fo_recv, fs_send, fs_recv, r_send, r_recv, lr_send, lr_recv):
    rows, width = x_hbm.shape
    head = wq_hbm.shape[1]
    part = wk_hbm.shape[1]
    chunks = rows // CHUNK
    side_chunks = rows // SIDE_CHUNK
    at = Place()
    core = at.core

    barrier = pltpu.get_barrier_semaphore()
    signal(barrier, at.far)

    @pl.when(core == 1)
    def _():
        signal(barrier, at.mate)

    @pl.when(at.row == 0)
    def _():
        signal(barrier, at.side)

    q_cols = pl.ds(pl.multiple_of(core * head, head), head)
    k_cols = pl.ds(pl.multiple_of(2 * head + core * part, part), part)
    v_cols = pl.ds(pl.multiple_of(3 * head + core * part, part), part)
    lead = width // 4
    mine = (
        (wk_hbm, pl.ds(0, lead), k_cols),
        (wk_hbm, pl.ds(lead, width - lead), k_cols),
        (wv_hbm, pl.ds(0, width), v_cols),
        (wq_hbm, pl.ds(0, width - DETOUR), q_cols),
        (wq_hbm, pl.ds(width - DETOUR, DETOUR), q_cols),
    )
    load_w, mate_w, far_w, relay_w = [], [], [], []
    for i, (src, depth, cols) in enumerate(mine):
        near_part, far_part = w_own.at[depth, cols], w_far.at[depth, cols]
        load_w.append(pltpu.make_async_copy(src.at[depth, :], near_part, lw_sem.at[i]))
        mate_w.append(send(near_part, near_part, mw_send.at[i], mw_recv.at[i], at.mate))
        far_w.append(send(near_part, far_part, fw_send.at[i], fw_recv.at[i], at.far))
        relay_w.append(send(far_part, far_part, rw_send.at[i], rw_recv.at[i], at.mate))

    def load_chunk(i):
        return pltpu.make_async_copy(x_hbm.at[span(i, CHUNK), :], x_own.at[span(i, CHUNK), :], load_x.at[i])

    def side_chunk(i):
        return send(x_hbm.at[span(i, SIDE_CHUNK), :], x_side.at[span(i, SIDE_CHUNK), :], x_send.at[i], x_recv.at[i], at.side)

    for copy in load_w:
        copy.start()

    last = w_own.at[mine[4][1], q_cols]
    aside = send(last, detoured, aside_send, aside_recv, at.side)
    across = send(detoured, w_far.at[mine[4][1], q_cols], across_send, across_recv, at.across(at.far))

    pl.semaphore_wait(barrier, 2 - core + at.row)

    @pl.when(at.column == 1)
    def _():
        send(wk_hbm.at[mine[0][1], :], w_far.at[mine[0][1], k_cols], fw_send.at[0], fw_recv.at[0], at.far).start()

    load_w[0].wait()

    @pl.when(at.column == 0)
    def _():
        far_w[0].start()

    for load, copy in zip(load_w[1:3], far_w[1:3]):
        load.wait()
        copy.start()
    for load in load_w[3:]:
        load.wait()

    @pl.when(at.row == 0)
    def _():
        far_w[3].start()

    @pl.when(core == 0)
    def _():
        signal(mate_answer, at.mate)

    @pl.when(at.row == 1)
    def _():
        signal(side_answer, at.side)

    gain_copy = pltpu.make_async_copy(gain_hbm, gain, load_gain)
    gain_copy.start()
    for i in range(chunks):
        load_chunk(i).start()

    @pl.when(core == 1)
    def _():
        pl.semaphore_wait(mate_answer, 1)

    signal(far_answer, at.far)
    for copy in mate_w:
        copy.start()

    @pl.when(at.row == 0)
    def _():
        pl.semaphore_wait(side_answer, 1)
        aside.start()

    loop(0, side_chunks, lambda i: side_chunk(i).start())

    @pl.when(at.row == 1)
    def _():
        aside.wait_recv()
        across.start()
        for copy in far_w[3:]:
            copy.start()

    def normalise(ref, i, size):
        def piece(p, carry):
            here = pl.ds(pl.multiple_of(i * size + p * PIECE, PIECE), PIECE)
            x_wide = ref[here, :].astype(jnp.float32)
            mean_sq = jnp.mean(x_wide * x_wide, axis=-1, keepdims=True)
            ref[here, :] = (x_wide * lax.rsqrt(mean_sq + EPSILON) * gain[...].reshape(1, width)).astype(jnp.bfloat16)
            return carry

        lax.fori_loop(0, size // PIECE, piece, 0, unroll=4)

    def product(ref, here, w, block):
        cols = slice(block * head, (block + 1) * head) if isinstance(block, int) else pl.ds(pl.multiple_of(block * head, head), head)
        return jnp.dot(ref[here, :], w[:, cols], preferred_element_type=jnp.float32).astype(jnp.bfloat16)

    def mate_copies(block, i):
        size, sends, recvs = (SIDE_CHUNK, ms_send, ms_recv) if block == SIDE else (CHUNK, mo_send, mo_recv)
        here, there = span(i, size, block * rows), span(i, size, (MATE + block) * rows)
        return (
            send(early.at[KV, here, :], early.at[KV, there, :], sends.at[0, i], recvs.at[0, i], at.mate),
            send(mate_q.at[here, :], early.at[Q, there, :], sends.at[1, i], recvs.at[1, i], at.mate),
        )

    def near_products(ref, block, i):
        size = SIDE_CHUNK if block == SIDE else CHUNK
        here, source = span(i, size, block * rows), span(i, size)
        early[K, here, :] = product(ref, source, w_own, 2)
        early[V, here, :] = product(ref, source, w_own, 3)
        early[Q, here, :] = product(ref, source, w_own, core)
        mate_q[here, :] = product(ref, source, w_own, 1 - core)
        for copy in mate_copies(block, i):
            copy.start()

    far_columns = {K: 2, V: 3, Q_SAME: core, Q_OTHER: 1 - core}

    def far_products(ref, here, stage, kinds):
        for kind in kinds:
            stage[kind, here, :] = product(ref, here, w_far, far_columns[kind])

    def own_message(j, i):
        src, dst, block, peer = ((KV, KV, FAR, at.far), (Q_SAME, Q, FAR, at.far), (Q_OTHER, Q, FAR_MATE, at.far_mate))[j]
        return send(far_own.at[src, span(i, CHUNK), :], early.at[dst, span(i, CHUNK, block * rows), :], fo_send.at[j, i], fo_recv.at[j, i], peer)

    def message(kind, i, count=1):
        return side_message(at, rows, far_late, late, fs_send.at[kind, i], fs_recv.at[kind, i], kind, i, count)

    def relay(i):
        return send(early.at[KV, span(i, CHUNK, FAR * rows), :], early.at[KV, span(i, CHUNK, FAR_MATE * rows), :], r_send.at[i], r_recv.at[i], at.mate)

    def own_norm(i):
        load_chunk(i).wait()
        normalise(x_own, i, CHUNK)

    for copy in mate_w:
        copy.wait_recv()
    gain_copy.wait()
    loop(0, chunks, own_norm)
    loop(0, chunks, lambda i: near_products(x_own, OWN, i))

    for arrived, onward in zip(far_w[:3], relay_w[:3]):
        arrived.wait_recv()
        onward.start()
    for copy in relay_w[:3]:
        copy.wait_recv()

    def far_kv_step(i):
        far_products(x_own, span(i, CHUNK), far_own, (K, V))
        own_message(0, i).start()

    loop(0, chunks, far_kv_step)
    far_w[3].wait_recv()
    relay_w[3].start()

    @pl.when(at.row == 0)
    def _():
        across.wait_recv()

    @pl.when(at.row == 1)
    def _():
        far_w[4].wait_recv()

    relay_w[4].start()
    for copy in relay_w[3:]:
        copy.wait_recv()
    pl.semaphore_wait(far_answer, 1)

    def far_q_step(i):
        far_products(x_own, span(i, CHUNK), far_own, (Q_SAME, Q_OTHER))
        own_message(1, i).start()
        own_message(2, i).start()

    loop(0, chunks, far_q_step)

    def side_step(i):
        side_chunk(i).wait_recv()
        normalise(x_side, i, SIDE_CHUNK)
        near_products(x_side, SIDE, i)
        far_products(x_side, span(i, SIDE_CHUNK), far_late, (Q_OTHER, K, V, Q_SAME))
        done = lax.rem(i + 1, CHUNK // SIDE_CHUNK) == 0
        n = i // (CHUNK // SIDE_CHUNK)

        @pl.when(done & (n < at.first))
        def _():
            message(OTHER, n).start()

        @pl.when(done & (n == at.first - 1))
        def _():
            by_core(at, lambda c: message(SAME, 0, FIRST[c]).start())

    loop(0, side_chunks - 1, side_step)

    def relay_step(i):
        own_message(0, i).wait_recv()
        relay(i).start()

    loop(0, chunks, relay_step)

    def drain_own(i):
        for copy in mate_copies(OWN, i):
            copy.wait_send()
            copy.wait_recv()
        for j in range(3):
            own_message(j, i).wait_send()
        for j in (1, 2):
            own_message(j, i).wait_recv()
        relay(i).wait_send()
        relay(i).wait_recv()

    loop(0, chunks, drain_own)
    for copies in (mate_w, far_w[:4], relay_w):
        for copy in copies:
            copy.wait_send()

    @pl.when(at.row == 0)
    def _():
        aside.wait_send()

    @pl.when(at.row == 1)
    def _():
        across.wait_send()
        far_w[4].wait_send()

    side_step(side_chunks - 1)

    def drain_side(i):
        side_chunk(i).wait_send()
        for copy in mate_copies(SIDE, i):
            copy.wait_send()
            copy.wait_recv()

    loop(0, side_chunks, drain_side)
    loop(0, at.first_other, lambda i: message(OTHER, i).wait_recv())
    loop(0, at.first, lambda i: message(OTHER, i).wait_send())

    def close(c):
        same = message(SAME, 0, FIRST[c])
        same.wait_recv()
        onward = late_relay(at, rows, late, late, lr_send, lr_recv, 0, FIRST[0])
        if c == 0:
            onward.start()
            onward.wait_send()
        else:
            onward.wait_recv()
        same.wait_send()

    by_core(at, close)


def finish(held, far_late, token, late, answer, send_sem, same_recv, other_recv, relay_recv):
    rows = far_late.shape[1]
    chunks = rows // CHUNK
    at = Place()
    barrier = pltpu.get_barrier_semaphore()
    signal(barrier, at.far)

    @pl.when(at.core == 0)
    def _():
        signal(barrier, at.mate)
        signal(barrier, at.far_mate)

    pl.semaphore_wait(barrier, 1 + 2 * at.core)
    def message(kind, i, count):
        return side_message(at, rows, far_late, late, send_sem, (same_recv, other_recv)[kind], kind, i, count)

    def relay(source, i, count):
        return late_relay(at, rows, source, late, send_sem, relay_recv, i, count)

    def body(c):
        first, other_first = FIRST[c], FIRST[1 - c]
        same, other = (message(kind, first, chunks - first) for kind in (SAME, OTHER))
        same.start()
        if c:
            signal(answer, at.mate)
            signal(answer, at.far_mate)
        else:
            pl.semaphore_wait(answer, 2)
        other.start()
        if c:
            relay(held, 0, first).start()
        same.wait_recv()
        relay(late, first, chunks - first).start()
        arrived = chunks if c == 0 else chunks - other_first
        relay(late, 0, arrived).wait_recv()
        message(OTHER, other_first, chunks - other_first).wait_recv()
        sent = 4 * (chunks - first) + 2 * (chunks if c else chunks - first)
        everything = late.at[KVQ, span(0, CHUNK, 0, sent // 3), :]
        pltpu.make_async_copy(everything, everything, send_sem).wait()

    by_core(at, body)


def late_chunks(core, held):
    first, other, relayed = FIRST[core], FIRST[1 - core], core * FIRST[0]
    spans = [(o, LATE_FAR, first) for o in (K, V, Q)] + [(Q, LATE_FAR_MATE, other)] + [(o, LATE_FAR_MATE, relayed) for o in (K, V)]
    return [(o, block, 0, n) if held else (o, block, n, None) for o, block, n in spans]


def store_chunks(at, source, outs, sem, core, held):
    rows = source.shape[1] // 2
    owners = tuple(at.across(device) for device in (at.far, at.far_mate))
    copies = []
    for o, block, start, count in late_chunks(core, held):
        count = (rows // CHUNK - start if count is None else count) * CHUNK
        if count:
            copies.append(pltpu.make_async_copy(
                source.at[o, pl.ds(block * rows + start * CHUNK, count), :],
                outs[o].at[pl.ds(pl.multiple_of(owners[block] * rows + start * CHUNK, CHUNK), count), :],
                sem,
            ))
    return copies


def run(copies):
    for copy in copies:
        copy.start()
    for copy in copies:
        copy.wait()


def store_early(early, held, q_out, k_out, v_out, token, sem):
    at = Place()
    owners = (at.me, at.side, at.mate, at.across(at.mate), at.far, at.far_mate)
    rows = early.shape[1] // len(owners)
    outs = (k_out, v_out, q_out)
    for core in range(2):
        @pl.when(at.core == core)
        def _():
            run([
                pltpu.make_async_copy(early.at[o, pl.ds(block * rows, rows), :], out.at[span(owner, rows), :], sem)
                for o, out in enumerate(outs)
                for block, owner in enumerate(owners)
            ] + store_chunks(at, held, outs, sem, core, True))


def store_late(late, q_in, k_in, v_in, q_out, k_out, v_out, sem):
    at = Place()
    for core in range(2):
        @pl.when(at.core == core)
        def _():
            run(store_chunks(at, late, (k_out, v_out, q_out), sem, core, False))


def in_vmem(*arrays):
    return tuple(pltpu.with_memory_space_constraint(array, pltpu.VMEM) for array in arrays)


def solution(mesh):
    group_size = mesh.shape["tp"]

    def local_step(x_rows, norm_gain, w_q, w_k, w_v):
        rows, width = x_rows.shape
        head = w_q.shape[2]
        chunks = rows // CHUNK
        dma = pltpu.SemaphoreType.DMA
        any_space = pl.BlockSpec(memory_space=pl.ANY)
        vmem = pl.BlockSpec(memory_space=pltpu.VMEM)
        hbm = pl.BlockSpec(memory_space=pltpu.HBM)

        def small(**settings):
            return pltpu.CompilerParams(vmem_limit_bytes=1024 * 1024, **settings)

        early = pltpu.VMEM((3, 6 * rows, head), jnp.bfloat16)
        late = pltpu.VMEM((3, 2 * rows, head), jnp.bfloat16)
        final = [pltpu.HBM((group_size * rows, head), jnp.bfloat16)] * 3
        side_chunks = rows // SIDE_CHUNK

        gathered, held, far_late = in_vmem(*pl.pallas_call(
            gather,
            out_shape=[early, late, pltpu.VMEM((4, rows, head), jnp.bfloat16)],
            in_specs=[any_space] * 5,
            out_specs=[vmem] * 3,
            scratch_shapes=[
                pltpu.VMEM((rows, width), jnp.bfloat16),
                pltpu.VMEM((rows, width), jnp.bfloat16),
                pltpu.VMEM((width, 4 * head), jnp.bfloat16),
                pltpu.VMEM((width, 4 * head), jnp.bfloat16),
                pltpu.VMEM((4, rows, head), jnp.bfloat16),
                pltpu.VMEM((2 * rows, head), jnp.bfloat16),
                pltpu.VMEM((width,), jnp.float32),
                pltpu.VMEM((DETOUR, head), jnp.bfloat16),
                *[pltpu.SemaphoreType.REGULAR] * 3, *[dma(())] * 5, dma((chunks,)),
                *[dma((5,))] * 7,
                dma((side_chunks,)), dma((side_chunks,)), dma((2, chunks)), dma((2, chunks)), dma((2, side_chunks)), dma((2, side_chunks)),
                dma((3, chunks)), dma((3, chunks)), dma((2, chunks)), dma((2, chunks)), dma((chunks,)), dma((chunks,)), dma(()), dma(()),
            ],
            compiler_params=pltpu.CompilerParams(collective_id=0, has_side_effects=True, vmem_limit_bytes=40 * 1024 * 1024),
            name="gather",
        )(x_rows, norm_gain, w_q.reshape(width, head), w_k, w_v))
        *stored, token = pl.pallas_call(
            store_early,
            out_shape=final + [pltpu.HBM((8, 128), jnp.float32)],
            in_specs=[vmem] * 2,
            out_specs=[hbm] * 4,
            scratch_shapes=[dma(())],
            compiler_params=small(),
            name="store_early",
        )(gathered, held)
        finished = pl.pallas_call(
            finish,
            out_shape=late,
            in_specs=[vmem] * 2 + [hbm],
            out_specs=vmem,
            scratch_shapes=[pltpu.SemaphoreType.REGULAR] + [dma(())] * 4,
            compiler_params=small(collective_id=1, has_side_effects=True),
            name="finish",
        )(held, far_late, pltpu.with_memory_space_constraint(token, pltpu.HBM))
        outs = pl.pallas_call(
            store_late,
            out_shape=final,
            in_specs=[vmem] + [hbm] * 3,
            out_specs=[hbm] * 3,
            input_output_aliases={1: 0, 2: 1, 3: 2},
            scratch_shapes=[dma(())],
            compiler_params=small(),
            name="store_late",
        )(*in_vmem(finished), *stored)
        return tuple(out[:, None, :] for out in outs)

    return jax.shard_map(local_step, mesh=mesh, in_specs=(P(("dp", "tp"), None), P(None), P(None, "tp", None), P(None, "tp"), P(None, "tp")), out_specs=(P("dp", "tp", None), P("dp", "tp", None), P("dp", "tp", None)), check_vma=False)
```

```python
import functools

import jax
import jax.numpy as jnp
from jax import lax
from jax.experimental import pallas as pl
from jax.experimental.pallas import tpu as pltpu
from jax.sharding import PartitionSpec as P

EPSILON = 1e-6
CHUNK = 256
SIDE_CHUNK = 128
PIECE = 16
DETOUR = 32

K, V, Q = range(3)
KV, KVQ = pl.ds(0, 2), pl.ds(0, 3)
Q_SAME, Q_OTHER = 2, 3
OWN, SIDE, MATE, MATE_SIDE, FAR, FAR_MATE = range(6)
LATE_FAR, LATE_FAR_MATE = range(2)


class Place:
    def __init__(self):
        self.me = lax.axis_index("tp")
        self.core = lax.rem(self.me, 2)
        self.row = self.me // 4
        self.column = lax.rem(self.me // 2, 2)
        self.mate = self.me + 1 - 2 * self.core
        self.side = self.across(self.me)
        self.far = self.me + 2 - 4 * lax.rem(self.me // 2, 2)
        self.far_mate = self.far + 1 - 2 * self.core
        self.first = FIRST[0] + (FIRST[1] - FIRST[0]) * self.core
        self.first_other = FIRST[0] + FIRST[1] - self.first

    def across(self, device):
        return device + 4 - 8 * (device // 4)


def send(src, dst, send_sem, recv_sem, to):
    return pltpu.make_async_remote_copy(src_ref=src, dst_ref=dst, send_sem=send_sem, recv_sem=recv_sem, device_id={"tp": to})


def signal(sem, to):
    pl.semaphore_signal(sem, inc=1, device_id={"tp": to})


def loop(start, stop, body):
    def step(i, carry):
        body(i)
        return carry

    lax.fori_loop(start, stop, step, 0)


def span(i, size, base=0, count=1):
    return pl.ds(pl.multiple_of(base + i * size, size), count * size)


def by_core(at, body):
    for core in range(2):
        pl.when(at.core == core)(functools.partial(body, core))


SAME, OTHER, SAME_KV, SAME_Q = range(4)
FIRST = (1, 3)


def side_message(at, rows, stage, target, send_sem, recv_sem, kind, i, count=1):
    src, dst, block, peer = {
        SAME: (KVQ, KVQ, LATE_FAR, at.far),
        SAME_KV: (KV, KV, LATE_FAR, at.far),
        SAME_Q: (Q_SAME, Q, LATE_FAR, at.far),
        OTHER: (Q_OTHER, Q, LATE_FAR_MATE, at.far_mate),
    }[kind]
    return send(stage.at[src, span(i, CHUNK, 0, count), :], target.at[dst, span(i, CHUNK, block * rows, count), :], send_sem, recv_sem, peer)


def late_relay(at, rows, source, target, send_sem, recv_sem, i, count=1):
    return send(source.at[KV, span(i, CHUNK, LATE_FAR * rows, count), :], target.at[KV, span(i, CHUNK, LATE_FAR_MATE * rows, count), :],
                send_sem, recv_sem, at.mate)


def gather(x_hbm, gain_hbm, wq_hbm, wk_hbm, wv_hbm, early, late, far_late,
           x_own, x_side, w_own, w_far, far_own, mate_q, gain, detoured,
           mate_answer, side_answer, far_answer, aside_send, aside_recv, across_send, across_recv, load_gain, load_x, lw_sem, mw_send, mw_recv, fw_send, fw_recv, rw_send, rw_recv,
           x_send, x_recv, mo_send, mo_recv, ms_send, ms_recv, fo_send, fo_recv, fs_send, fs_recv, r_send, r_recv, lr_send, lr_recv):
    rows, width = x_hbm.shape
    head = wq_hbm.shape[1]
    part = wk_hbm.shape[1]
    chunks = rows // CHUNK
    side_chunks = rows // SIDE_CHUNK
    at = Place()
    core = at.core

    barrier = pltpu.get_barrier_semaphore()
    signal(barrier, at.far)

    @pl.when(core == 1)
    def _():
        signal(barrier, at.mate)

    @pl.when(at.row == 0)
    def _():
        signal(barrier, at.side)

    q_cols = pl.ds(pl.multiple_of(core * head, head), head)
    k_cols = pl.ds(pl.multiple_of(2 * head + core * part, part), part)
    v_cols = pl.ds(pl.multiple_of(3 * head + core * part, part), part)
    lead = width // 4
    mine = (
        (wk_hbm, pl.ds(0, lead), k_cols),
        (wk_hbm, pl.ds(lead, width - lead), k_cols),
        (wv_hbm, pl.ds(0, width), v_cols),
        (wq_hbm, pl.ds(0, width - DETOUR), q_cols),
        (wq_hbm, pl.ds(width - DETOUR, DETOUR), q_cols),
    )
    load_w, mate_w, far_w, relay_w = [], [], [], []
    for i, (src, depth, cols) in enumerate(mine):
        near_part, far_part = w_own.at[depth, cols], w_far.at[depth, cols]
        load_w.append(pltpu.make_async_copy(src.at[depth, :], near_part, lw_sem.at[i]))
        mate_w.append(send(near_part, near_part, mw_send.at[i], mw_recv.at[i], at.mate))
        far_w.append(send(near_part, far_part, fw_send.at[i], fw_recv.at[i], at.far))
        relay_w.append(send(far_part, far_part, rw_send.at[i], rw_recv.at[i], at.mate))

    def load_chunk(i):
        return pltpu.make_async_copy(x_hbm.at[span(i, CHUNK), :], x_own.at[span(i, CHUNK), :], load_x.at[i])

    def side_chunk(i):
        return send(x_hbm.at[span(i, SIDE_CHUNK), :], x_side.at[span(i, SIDE_CHUNK), :], x_send.at[i], x_recv.at[i], at.side)

    for copy in load_w:
        copy.start()

    last = w_own.at[mine[4][1], q_cols]
    aside = send(last, detoured, aside_send, aside_recv, at.side)
    across = send(detoured, w_far.at[mine[4][1], q_cols], across_send, across_recv, at.across(at.far))

    pl.semaphore_wait(barrier, 2 - core + at.row)

    @pl.when(at.column == 1)
    def _():
        send(wk_hbm.at[mine[0][1], :], w_far.at[mine[0][1], k_cols], fw_send.at[0], fw_recv.at[0], at.far).start()

    load_w[0].wait()

    @pl.when(at.column == 0)
    def _():
        far_w[0].start()

    for load, copy in zip(load_w[1:3], far_w[1:3]):
        load.wait()
        copy.start()
    for load in load_w[3:]:
        load.wait()

    @pl.when(at.row == 0)
    def _():
        far_w[3].start()

    @pl.when(core == 0)
    def _():
        signal(mate_answer, at.mate)

    @pl.when(at.row == 1)
    def _():
        signal(side_answer, at.side)

    gain_copy = pltpu.make_async_copy(gain_hbm, gain, load_gain)
    gain_copy.start()
    for i in range(chunks):
        load_chunk(i).start()

    @pl.when(core == 1)
    def _():
        pl.semaphore_wait(mate_answer, 1)

    signal(far_answer, at.far)
    for copy in mate_w:
        copy.start()

    @pl.when(at.row == 0)
    def _():
        pl.semaphore_wait(side_answer, 1)
        aside.start()

    loop(0, side_chunks, lambda i: side_chunk(i).start())

    @pl.when(at.row == 1)
    def _():
        aside.wait_recv()
        across.start()
        for copy in far_w[3:]:
            copy.start()

    def normalise(ref, i, size):
        def piece(p, carry):
            here = pl.ds(pl.multiple_of(i * size + p * PIECE, PIECE), PIECE)
            x_wide = ref[here, :].astype(jnp.float32)
            mean_sq = jnp.mean(x_wide * x_wide, axis=-1, keepdims=True)
            ref[here, :] = (x_wide * lax.rsqrt(mean_sq + EPSILON) * gain[...].reshape(1, width)).astype(jnp.bfloat16)
            return carry

        lax.fori_loop(0, size // PIECE, piece, 0, unroll=4)

    def product(ref, here, w, block):
        cols = slice(block * head, (block + 1) * head) if isinstance(block, int) else pl.ds(pl.multiple_of(block * head, head), head)
        return jnp.dot(ref[here, :], w[:, cols], preferred_element_type=jnp.float32).astype(jnp.bfloat16)

    def mate_copies(block, i):
        size, sends, recvs = (SIDE_CHUNK, ms_send, ms_recv) if block == SIDE else (CHUNK, mo_send, mo_recv)
        here, there = span(i, size, block * rows), span(i, size, (MATE + block) * rows)
        return (
            send(early.at[KV, here, :], early.at[KV, there, :], sends.at[0, i], recvs.at[0, i], at.mate),
            send(mate_q.at[here, :], early.at[Q, there, :], sends.at[1, i], recvs.at[1, i], at.mate),
        )

    def near_products(ref, block, i):
        size = SIDE_CHUNK if block == SIDE else CHUNK
        here, source = span(i, size, block * rows), span(i, size)
        early[K, here, :] = product(ref, source, w_own, 2)
        early[V, here, :] = product(ref, source, w_own, 3)
        early[Q, here, :] = product(ref, source, w_own, core)
        mate_q[here, :] = product(ref, source, w_own, 1 - core)
        for copy in mate_copies(block, i):
            copy.start()

    far_columns = {K: 2, V: 3, Q_SAME: core, Q_OTHER: 1 - core}

    def far_products(ref, here, stage, kinds):
        for kind in kinds:
            stage[kind, here, :] = product(ref, here, w_far, far_columns[kind])

    def own_message(j, i):
        src, dst, block, peer = ((KV, KV, FAR, at.far), (Q_SAME, Q, FAR, at.far), (Q_OTHER, Q, FAR_MATE, at.far_mate))[j]
        return send(far_own.at[src, span(i, CHUNK), :], early.at[dst, span(i, CHUNK, block * rows), :], fo_send.at[j, i], fo_recv.at[j, i], peer)

    def message(kind, i, count=1):
        return side_message(at, rows, far_late, late, fs_send.at[kind, i], fs_recv.at[kind, i], kind, i, count)

    def relay(i):
        return send(early.at[KV, span(i, CHUNK, FAR * rows), :], early.at[KV, span(i, CHUNK, FAR_MATE * rows), :], r_send.at[i], r_recv.at[i], at.mate)

    def own_norm(i):
        load_chunk(i).wait()
        normalise(x_own, i, CHUNK)

    for copy in mate_w:
        copy.wait_recv()
    gain_copy.wait()
    loop(0, chunks, own_norm)
    loop(0, chunks, lambda i: near_products(x_own, OWN, i))

    for arrived, onward in zip(far_w[:3], relay_w[:3]):
        arrived.wait_recv()
        onward.start()
    for copy in relay_w[:3]:
        copy.wait_recv()

    def far_kv_step(i):
        far_products(x_own, span(i, CHUNK), far_own, (K, V))
        own_message(0, i).start()

    loop(0, chunks, far_kv_step)
    far_w[3].wait_recv()
    relay_w[3].start()

    @pl.when(at.row == 0)
    def _():
        across.wait_recv()

    @pl.when(at.row == 1)
    def _():
        far_w[4].wait_recv()

    relay_w[4].start()
    for copy in relay_w[3:]:
        copy.wait_recv()
    pl.semaphore_wait(far_answer, 1)

    def far_q_step(i):
        far_products(x_own, span(i, CHUNK), far_own, (Q_SAME, Q_OTHER))
        own_message(1, i).start()
        own_message(2, i).start()

    loop(0, chunks, far_q_step)

    def side_step(i):
        side_chunk(i).wait_recv()
        normalise(x_side, i, SIDE_CHUNK)
        near_products(x_side, SIDE, i)
        far_products(x_side, span(i, SIDE_CHUNK), far_late, (Q_OTHER, K, V, Q_SAME))
        done = lax.rem(i + 1, CHUNK // SIDE_CHUNK) == 0
        n = i // (CHUNK // SIDE_CHUNK)

        @pl.when(done & (n < at.first))
        def _():
            message(OTHER, n).start()

        @pl.when(done & (n == at.first - 1))
        def _():
            by_core(at, lambda c: message(SAME, 0, FIRST[c]).start())

    loop(0, side_chunks - 1, side_step)

    def relay_step(i):
        own_message(0, i).wait_recv()
        relay(i).start()

    loop(0, chunks, relay_step)

    def drain_own(i):
        for copy in mate_copies(OWN, i):
            copy.wait_send()
            copy.wait_recv()
        for j in range(3):
            own_message(j, i).wait_send()
        for j in (1, 2):
            own_message(j, i).wait_recv()
        relay(i).wait_send()
        relay(i).wait_recv()

    loop(0, chunks, drain_own)
    for copies in (mate_w, far_w[:4], relay_w):
        for copy in copies:
            copy.wait_send()

    @pl.when(at.row == 0)
    def _():
        aside.wait_send()

    @pl.when(at.row == 1)
    def _():
        across.wait_send()
        far_w[4].wait_send()

    side_step(side_chunks - 1)

    def drain_side(i):
        side_chunk(i).wait_send()
        for copy in mate_copies(SIDE, i):
            copy.wait_send()
            copy.wait_recv()

    loop(0, side_chunks, drain_side)
    loop(0, at.first_other, lambda i: message(OTHER, i).wait_recv())
    loop(0, at.first, lambda i: message(OTHER, i).wait_send())

    def close(c):
        same = message(SAME, 0, FIRST[c])
        same.wait_recv()
        onward = late_relay(at, rows, late, late, lr_send, lr_recv, 0, FIRST[0])
        if c == 0:
            onward.start()
            onward.wait_send()
        else:
            onward.wait_recv()
        same.wait_send()

    by_core(at, close)


def finish(held, far_late, token, late, answer, send_sem, same_recv, lead_recv, rest_recv, relay_recv):
    rows = far_late.shape[1]
    chunks = rows // CHUNK
    at = Place()
    barrier = pltpu.get_barrier_semaphore()
    signal(barrier, at.far)

    @pl.when(at.core == 0)
    def _():
        signal(barrier, at.mate)
        signal(barrier, at.far_mate)

    pl.semaphore_wait(barrier, 1 + 2 * at.core)
    def message(kind, recv_sem, i, count):
        return side_message(at, rows, far_late, late, send_sem, recv_sem, kind, i, count)

    def relay(source, i, count):
        return late_relay(at, rows, source, late, send_sem, relay_recv, i, count)

    def chunks_of_all(count):
        ref = late.at[KVQ, span(0, CHUNK, 0, count), :]
        return ref, ref

    def body(c):
        first, other_first = FIRST[c], FIRST[1 - c]
        mine, others = chunks - first, chunks - other_first
        if c == 0:
            same = message(SAME, same_recv, first, mine)
            same.start()
            pl.semaphore_wait(answer, 2)
            message(OTHER, lead_recv, first, 1).start()
            message(OTHER, rest_recv, first + 1, mine - 1).start()
        else:
            same = message(SAME_KV, same_recv, first, mine)
            same.start()
            signal(answer, at.mate)
            signal(answer, at.far_mate)
            message(OTHER, rest_recv, first, mine).start()
            relay(held, 0, first).start()
        same.wait_recv()
        relay(late, first, mine).start()
        if c == 1:
            message(OTHER, lead_recv, other_first, 1).wait_recv()
            message(SAME_Q, rest_recv, first, mine).start()
        relay(late, 0, chunks if c == 0 else others).wait_recv()
        if c == 0:
            message(OTHER, rest_recv, other_first, others).wait_recv()
        else:
            pltpu.make_async_copy(*chunks_of_all((others - 1 + mine) // 3), rest_recv).wait()
        sent = 4 * mine + 2 * (mine if c == 0 else chunks)
        pltpu.make_async_copy(*chunks_of_all(sent // 3), send_sem).wait()

    by_core(at, body)


def late_chunks(core, held):
    first, other, relayed = FIRST[core], FIRST[1 - core], core * FIRST[0]
    spans = [(o, LATE_FAR, first) for o in (K, V, Q)] + [(Q, LATE_FAR_MATE, other)] + [(o, LATE_FAR_MATE, relayed) for o in (K, V)]
    return [(o, block, 0, n) if held else (o, block, n, None) for o, block, n in spans]


def store_chunks(at, source, outs, sem, core, held):
    rows = source.shape[1] // 2
    owners = tuple(at.across(device) for device in (at.far, at.far_mate))
    copies = []
    for o, block, start, count in late_chunks(core, held):
        count = (rows // CHUNK - start if count is None else count) * CHUNK
        if count:
            copies.append(pltpu.make_async_copy(
                source.at[o, pl.ds(block * rows + start * CHUNK, count), :],
                outs[o].at[pl.ds(pl.multiple_of(owners[block] * rows + start * CHUNK, CHUNK), count), :],
                sem,
            ))
    return copies


def run(copies):
    for copy in copies:
        copy.start()
    for copy in copies:
        copy.wait()


def store_early(early, held, q_out, k_out, v_out, token, sem):
    at = Place()
    owners = (at.me, at.side, at.mate, at.across(at.mate), at.far, at.far_mate)
    rows = early.shape[1] // len(owners)
    outs = (k_out, v_out, q_out)
    for core in range(2):
        @pl.when(at.core == core)
        def _():
            run([
                pltpu.make_async_copy(early.at[o, pl.ds(block * rows, rows), :], out.at[span(owner, rows), :], sem)
                for o, out in enumerate(outs)
                for block, owner in enumerate(owners)
            ] + store_chunks(at, held, outs, sem, core, True))


def store_late(late, q_in, k_in, v_in, q_out, k_out, v_out, sem):
    at = Place()
    for core in range(2):
        @pl.when(at.core == core)
        def _():
            run(store_chunks(at, late, (k_out, v_out, q_out), sem, core, False))


def in_vmem(*arrays):
    return tuple(pltpu.with_memory_space_constraint(array, pltpu.VMEM) for array in arrays)


def solution(mesh):
    group_size = mesh.shape["tp"]

    def local_step(x_rows, norm_gain, w_q, w_k, w_v):
        rows, width = x_rows.shape
        head = w_q.shape[2]
        chunks = rows // CHUNK
        dma = pltpu.SemaphoreType.DMA
        any_space = pl.BlockSpec(memory_space=pl.ANY)
        vmem = pl.BlockSpec(memory_space=pltpu.VMEM)
        hbm = pl.BlockSpec(memory_space=pltpu.HBM)

        def small(**settings):
            return pltpu.CompilerParams(vmem_limit_bytes=1024 * 1024, **settings)

        early = pltpu.VMEM((3, 6 * rows, head), jnp.bfloat16)
        late = pltpu.VMEM((3, 2 * rows, head), jnp.bfloat16)
        final = [pltpu.HBM((group_size * rows, head), jnp.bfloat16)] * 3
        side_chunks = rows // SIDE_CHUNK

        gathered, held, far_late = in_vmem(*pl.pallas_call(
            gather,
            out_shape=[early, late, pltpu.VMEM((4, rows, head), jnp.bfloat16)],
            in_specs=[any_space] * 5,
            out_specs=[vmem] * 3,
            scratch_shapes=[
                pltpu.VMEM((rows, width), jnp.bfloat16),
                pltpu.VMEM((rows, width), jnp.bfloat16),
                pltpu.VMEM((width, 4 * head), jnp.bfloat16),
                pltpu.VMEM((width, 4 * head), jnp.bfloat16),
                pltpu.VMEM((4, rows, head), jnp.bfloat16),
                pltpu.VMEM((2 * rows, head), jnp.bfloat16),
                pltpu.VMEM((width,), jnp.float32),
                pltpu.VMEM((DETOUR, head), jnp.bfloat16),
                *[pltpu.SemaphoreType.REGULAR] * 3, *[dma(())] * 5, dma((chunks,)),
                *[dma((5,))] * 7,
                dma((side_chunks,)), dma((side_chunks,)), dma((2, chunks)), dma((2, chunks)), dma((2, side_chunks)), dma((2, side_chunks)),
                dma((3, chunks)), dma((3, chunks)), dma((2, chunks)), dma((2, chunks)), dma((chunks,)), dma((chunks,)), dma(()), dma(()),
            ],
            compiler_params=pltpu.CompilerParams(collective_id=0, has_side_effects=True, vmem_limit_bytes=40 * 1024 * 1024),
            name="gather",
        )(x_rows, norm_gain, w_q.reshape(width, head), w_k, w_v))
        *stored, token = pl.pallas_call(
            store_early,
            out_shape=final + [pltpu.HBM((8, 128), jnp.float32)],
            in_specs=[vmem] * 2,
            out_specs=[hbm] * 4,
            scratch_shapes=[dma(())],
            compiler_params=small(),
            name="store_early",
        )(gathered, held)
        finished = pl.pallas_call(
            finish,
            out_shape=late,
            in_specs=[vmem] * 2 + [hbm],
            out_specs=vmem,
            scratch_shapes=[pltpu.SemaphoreType.REGULAR] + [dma(())] * 5,
            compiler_params=small(collective_id=1, has_side_effects=True),
            name="finish",
        )(held, far_late, pltpu.with_memory_space_constraint(token, pltpu.HBM))
        outs = pl.pallas_call(
            store_late,
            out_shape=final,
            in_specs=[vmem] + [hbm] * 3,
            out_specs=[hbm] * 3,
            input_output_aliases={1: 0, 2: 1, 3: 2},
            scratch_shapes=[dma(())],
            compiler_params=small(),
            name="store_late",
        )(*in_vmem(finished), *stored)
        return tuple(out[:, None, :] for out in outs)

    return jax.shard_map(local_step, mesh=mesh, in_specs=(P(("dp", "tp"), None), P(None), P(None, "tp", None), P(None, "tp"), P(None, "tp")), out_specs=(P("dp", "tp", None), P("dp", "tp", None), P("dp", "tp", None)), check_vma=False)
```

```python
import functools

import jax
import jax.numpy as jnp
from jax import lax
from jax.experimental import pallas as pl
from jax.experimental.pallas import tpu as pltpu
from jax.sharding import PartitionSpec as P

EPSILON = 1e-6
CHUNK = 256
SIDE_CHUNK = 128
PIECE = 16
DETOUR = 48

K, V, Q = range(3)
KV, KVQ = pl.ds(0, 2), pl.ds(0, 3)
Q_SAME, Q_OTHER = 2, 3
OWN, SIDE, MATE, MATE_SIDE, FAR, FAR_MATE = range(6)
LATE_FAR, LATE_FAR_MATE = range(2)


class Place:
    def __init__(self):
        self.me = lax.axis_index("tp")
        self.core = lax.rem(self.me, 2)
        self.row = self.me // 4
        self.column = lax.rem(self.me // 2, 2)
        self.mate = self.me + 1 - 2 * self.core
        self.side = self.across(self.me)
        self.far = self.me + 2 - 4 * lax.rem(self.me // 2, 2)
        self.far_mate = self.far + 1 - 2 * self.core
        self.first = FIRST[0] + (FIRST[1] - FIRST[0]) * self.core
        self.first_other = FIRST[0] + FIRST[1] - self.first

    def across(self, device):
        return device + 4 - 8 * (device // 4)


def send(src, dst, send_sem, recv_sem, to):
    return pltpu.make_async_remote_copy(src_ref=src, dst_ref=dst, send_sem=send_sem, recv_sem=recv_sem, device_id={"tp": to})


def signal(sem, to):
    pl.semaphore_signal(sem, inc=1, device_id={"tp": to})


def loop(start, stop, body):
    def step(i, carry):
        body(i)
        return carry

    lax.fori_loop(start, stop, step, 0)


def span(i, size, base=0, count=1):
    return pl.ds(pl.multiple_of(base + i * size, size), count * size)


def by_core(at, body):
    for core in range(2):
        pl.when(at.core == core)(functools.partial(body, core))


SAME, OTHER = range(2)
FIRST = (1, 3)


def side_message(at, rows, stage, target, send_sem, recv_sem, kind, i, count=1):
    src, dst, block, peer = ((KVQ, KVQ, LATE_FAR, at.far), (Q_OTHER, Q, LATE_FAR_MATE, at.far_mate))[kind]
    return send(stage.at[src, span(i, CHUNK, 0, count), :], target.at[dst, span(i, CHUNK, block * rows, count), :], send_sem, recv_sem, peer)


def late_relay(at, rows, source, target, send_sem, recv_sem, i, count=1):
    return send(source.at[KV, span(i, CHUNK, LATE_FAR * rows, count), :], target.at[KV, span(i, CHUNK, LATE_FAR_MATE * rows, count), :],
                send_sem, recv_sem, at.mate)


def gather(x_hbm, gain_hbm, wq_hbm, wk_hbm, wv_hbm, early, late, far_late,
           x_own, x_side, w_own, w_far, far_own, mate_q, gain, detoured,
           mate_answer, side_answer, far_answer, aside_send, aside_recv, across_send, across_recv, load_gain, load_x, lw_sem, mw_send, mw_recv, fw_send, fw_recv, rw_send, rw_recv,
           x_send, x_recv, mo_send, mo_recv, ms_send, ms_recv, fo_send, fo_recv, fs_send, fs_recv, r_send, r_recv, lr_send, lr_recv):
    rows, width = x_hbm.shape
    head = wq_hbm.shape[1]
    part = wk_hbm.shape[1]
    chunks = rows // CHUNK
    side_chunks = rows // SIDE_CHUNK
    at = Place()
    core = at.core

    barrier = pltpu.get_barrier_semaphore()
    signal(barrier, at.far)

    @pl.when(core == 1)
    def _():
        signal(barrier, at.mate)

    @pl.when(at.row == 0)
    def _():
        signal(barrier, at.side)

    q_cols = pl.ds(pl.multiple_of(core * head, head), head)
    k_cols = pl.ds(pl.multiple_of(2 * head + core * part, part), part)
    v_cols = pl.ds(pl.multiple_of(3 * head + core * part, part), part)
    lead = width // 4
    mine = (
        (wk_hbm, pl.ds(0, lead), k_cols),
        (wk_hbm, pl.ds(lead, width - lead), k_cols),
        (wv_hbm, pl.ds(0, width), v_cols),
        (wq_hbm, pl.ds(0, width - DETOUR), q_cols),
        (wq_hbm, pl.ds(width - DETOUR, DETOUR), q_cols),
    )
    load_w, mate_w, far_w, relay_w = [], [], [], []
    for i, (src, depth, cols) in enumerate(mine):
        near_part, far_part = w_own.at[depth, cols], w_far.at[depth, cols]
        load_w.append(pltpu.make_async_copy(src.at[depth, :], near_part, lw_sem.at[i]))
        mate_w.append(send(near_part, near_part, mw_send.at[i], mw_recv.at[i], at.mate))
        far_w.append(send(near_part, far_part, fw_send.at[i], fw_recv.at[i], at.far))
        relay_w.append(send(far_part, far_part, rw_send.at[i], rw_recv.at[i], at.mate))

    def load_chunk(i):
        return pltpu.make_async_copy(x_hbm.at[span(i, CHUNK), :], x_own.at[span(i, CHUNK), :], load_x.at[i])

    def side_chunk(i):
        return send(x_hbm.at[span(i, SIDE_CHUNK), :], x_side.at[span(i, SIDE_CHUNK), :], x_send.at[i], x_recv.at[i], at.side)

    for copy in load_w:
        copy.start()

    last = w_own.at[mine[4][1], q_cols]
    aside = send(last, detoured, aside_send, aside_recv, at.side)
    across = send(detoured, w_far.at[mine[4][1], q_cols], across_send, across_recv, at.across(at.far))

    pl.semaphore_wait(barrier, 2 - core + at.row)

    @pl.when(at.column == 1)
    def _():
        send(wk_hbm.at[mine[0][1], :], w_far.at[mine[0][1], k_cols], fw_send.at[0], fw_recv.at[0], at.far).start()

    load_w[0].wait()

    @pl.when(at.column == 0)
    def _():
        far_w[0].start()

    for load, copy in zip(load_w[1:3], far_w[1:3]):
        load.wait()
        copy.start()
    for load in load_w[3:]:
        load.wait()

    @pl.when(at.row == 0)
    def _():
        far_w[3].start()

    @pl.when(core == 0)
    def _():
        signal(mate_answer, at.mate)

    @pl.when(at.row == 1)
    def _():
        signal(side_answer, at.side)

    gain_copy = pltpu.make_async_copy(gain_hbm, gain, load_gain)
    gain_copy.start()
    for i in range(chunks):
        load_chunk(i).start()

    @pl.when(core == 1)
    def _():
        pl.semaphore_wait(mate_answer, 1)

    signal(far_answer, at.far)
    for copy in mate_w:
        copy.start()

    @pl.when(at.row == 0)
    def _():
        pl.semaphore_wait(side_answer, 1)
        aside.start()

    loop(0, side_chunks, lambda i: side_chunk(i).start())

    @pl.when(at.row == 1)
    def _():
        aside.wait_recv()
        across.start()
        for copy in far_w[3:]:
            copy.start()

    def normalise(ref, i, size):
        def piece(p, carry):
            here = pl.ds(pl.multiple_of(i * size + p * PIECE, PIECE), PIECE)
            x_wide = ref[here, :].astype(jnp.float32)
            mean_sq = jnp.mean(x_wide * x_wide, axis=-1, keepdims=True)
            ref[here, :] = (x_wide * lax.rsqrt(mean_sq + EPSILON) * gain[...].reshape(1, width)).astype(jnp.bfloat16)
            return carry

        lax.fori_loop(0, size // PIECE, piece, 0, unroll=4)

    def product(ref, here, w, block):
        cols = slice(block * head, (block + 1) * head) if isinstance(block, int) else pl.ds(pl.multiple_of(block * head, head), head)
        return jnp.dot(ref[here, :], w[:, cols], preferred_element_type=jnp.float32).astype(jnp.bfloat16)

    def mate_copies(block, i):
        size, sends, recvs = (SIDE_CHUNK, ms_send, ms_recv) if block == SIDE else (CHUNK, mo_send, mo_recv)
        here, there = span(i, size, block * rows), span(i, size, (MATE + block) * rows)
        return (
            send(early.at[KV, here, :], early.at[KV, there, :], sends.at[0, i], recvs.at[0, i], at.mate),
            send(mate_q.at[here, :], early.at[Q, there, :], sends.at[1, i], recvs.at[1, i], at.mate),
        )

    def near_products(ref, block, i):
        size = SIDE_CHUNK if block == SIDE else CHUNK
        here, source = span(i, size, block * rows), span(i, size)
        early[K, here, :] = product(ref, source, w_own, 2)
        early[V, here, :] = product(ref, source, w_own, 3)
        early[Q, here, :] = product(ref, source, w_own, core)
        mate_q[here, :] = product(ref, source, w_own, 1 - core)
        for copy in mate_copies(block, i):
            copy.start()

    far_columns = {K: 2, V: 3, Q_SAME: core, Q_OTHER: 1 - core}

    def far_products(ref, here, stage, kinds):
        for kind in kinds:
            stage[kind, here, :] = product(ref, here, w_far, far_columns[kind])

    def own_message(j, i):
        src, dst, block, peer = ((KV, KV, FAR, at.far), (Q_SAME, Q, FAR, at.far), (Q_OTHER, Q, FAR_MATE, at.far_mate))[j]
        return send(far_own.at[src, span(i, CHUNK), :], early.at[dst, span(i, CHUNK, block * rows), :], fo_send.at[j, i], fo_recv.at[j, i], peer)

    def message(kind, i, count=1):
        return side_message(at, rows, far_late, late, fs_send.at[kind, i], fs_recv.at[kind, i], kind, i, count)

    def relay(i):
        return send(early.at[KV, span(i, CHUNK, FAR * rows), :], early.at[KV, span(i, CHUNK, FAR_MATE * rows), :], r_send.at[i], r_recv.at[i], at.mate)

    def own_norm(i):
        load_chunk(i).wait()
        normalise(x_own, i, CHUNK)

    for copy in mate_w:
        copy.wait_recv()
    gain_copy.wait()
    loop(0, chunks, own_norm)
    loop(0, chunks, lambda i: near_products(x_own, OWN, i))

    for arrived, onward in zip(far_w[:3], relay_w[:3]):
        arrived.wait_recv()
        onward.start()
    for copy in relay_w[:3]:
        copy.wait_recv()

    def far_kv_step(i):
        far_products(x_own, span(i, CHUNK), far_own, (K, V))
        own_message(0, i).start()

    loop(0, chunks, far_kv_step)
    far_w[3].wait_recv()
    relay_w[3].start()

    @pl.when(at.row == 0)
    def _():
        across.wait_recv()

    @pl.when(at.row == 1)
    def _():
        far_w[4].wait_recv()

    relay_w[4].start()
    for copy in relay_w[3:]:
        copy.wait_recv()
    pl.semaphore_wait(far_answer, 1)

    def far_q_step(i):
        far_products(x_own, span(i, CHUNK), far_own, (Q_SAME, Q_OTHER))
        own_message(1, i).start()
        own_message(2, i).start()

    loop(0, chunks, far_q_step)

    def side_step(i):
        side_chunk(i).wait_recv()
        normalise(x_side, i, SIDE_CHUNK)
        near_products(x_side, SIDE, i)
        far_products(x_side, span(i, SIDE_CHUNK), far_late, (Q_OTHER, K, V, Q_SAME))
        done = lax.rem(i + 1, CHUNK // SIDE_CHUNK) == 0
        n = i // (CHUNK // SIDE_CHUNK)

        @pl.when(done & (n < at.first))
        def _():
            message(OTHER, n).start()

        @pl.when(done & (n == at.first - 1))
        def _():
            by_core(at, lambda c: message(SAME, 0, FIRST[c]).start())

    loop(0, side_chunks - 1, side_step)

    def relay_step(i):
        own_message(0, i).wait_recv()
        relay(i).start()

    loop(0, chunks, relay_step)

    def drain_own(i):
        for copy in mate_copies(OWN, i):
            copy.wait_send()
            copy.wait_recv()
        for j in range(3):
            own_message(j, i).wait_send()
        for j in (1, 2):
            own_message(j, i).wait_recv()
        relay(i).wait_send()
        relay(i).wait_recv()

    loop(0, chunks, drain_own)
    for copies in (mate_w, far_w[:4], relay_w):
        for copy in copies:
            copy.wait_send()

    @pl.when(at.row == 0)
    def _():
        aside.wait_send()

    @pl.when(at.row == 1)
    def _():
        across.wait_send()
        far_w[4].wait_send()

    side_step(side_chunks - 1)

    def drain_side(i):
        side_chunk(i).wait_send()
        for copy in mate_copies(SIDE, i):
            copy.wait_send()
            copy.wait_recv()

    loop(0, side_chunks, drain_side)
    loop(0, at.first_other, lambda i: message(OTHER, i).wait_recv())
    loop(0, at.first, lambda i: message(OTHER, i).wait_send())

    def close(c):
        same = message(SAME, 0, FIRST[c])
        same.wait_recv()
        onward = late_relay(at, rows, late, late, lr_send, lr_recv, 0, FIRST[0])
        if c == 0:
            onward.start()
            onward.wait_send()
        else:
            onward.wait_recv()
        same.wait_send()

    by_core(at, close)


def finish(held, far_late, token, late, answer, send_sem, same_recv, other_recv, relay_recv):
    rows = far_late.shape[1]
    chunks = rows // CHUNK
    at = Place()
    barrier = pltpu.get_barrier_semaphore()
    signal(barrier, at.far)

    @pl.when(at.core == 0)
    def _():
        signal(barrier, at.mate)
        signal(barrier, at.far_mate)

    pl.semaphore_wait(barrier, 1 + 2 * at.core)
    def message(kind, i, count):
        return side_message(at, rows, far_late, late, send_sem, (same_recv, other_recv)[kind], kind, i, count)

    def relay(source, i, count):
        return late_relay(at, rows, source, late, send_sem, relay_recv, i, count)

    def body(c):
        first, other_first = FIRST[c], FIRST[1 - c]
        same, other = (message(kind, first, chunks - first) for kind in (SAME, OTHER))
        same.start()
        if c:
            signal(answer, at.mate)
            signal(answer, at.far_mate)
        else:
            pl.semaphore_wait(answer, 2)
        other.start()
        if c:
            relay(held, 0, first).start()
        same.wait_recv()
        relay(late, first, chunks - first).start()
        arrived = chunks if c == 0 else chunks - other_first
        relay(late, 0, arrived).wait_recv()
        message(OTHER, other_first, chunks - other_first).wait_recv()
        sent = 4 * (chunks - first) + 2 * (chunks if c else chunks - first)
        everything = late.at[KVQ, span(0, CHUNK, 0, sent // 3), :]
        pltpu.make_async_copy(everything, everything, send_sem).wait()

    by_core(at, body)


def late_chunks(core, held):
    first, other, relayed = FIRST[core], FIRST[1 - core], core * FIRST[0]
    spans = [(o, LATE_FAR, first) for o in (K, V, Q)] + [(Q, LATE_FAR_MATE, other)] + [(o, LATE_FAR_MATE, relayed) for o in (K, V)]
    return [(o, block, 0, n) if held else (o, block, n, None) for o, block, n in spans]


def store_chunks(at, source, outs, sem, core, held):
    rows = source.shape[1] // 2
    owners = tuple(at.across(device) for device in (at.far, at.far_mate))
    copies = []
    for o, block, start, count in late_chunks(core, held):
        count = (rows // CHUNK - start if count is None else count) * CHUNK
        if count:
            copies.append(pltpu.make_async_copy(
                source.at[o, pl.ds(block * rows + start * CHUNK, count), :],
                outs[o].at[pl.ds(pl.multiple_of(owners[block] * rows + start * CHUNK, CHUNK), count), :],
                sem,
            ))
    return copies


def run(copies):
    for copy in copies:
        copy.start()
    for copy in copies:
        copy.wait()


def store_early(early, held, q_out, k_out, v_out, token, sem):
    at = Place()
    owners = (at.me, at.side, at.mate, at.across(at.mate), at.far, at.far_mate)
    rows = early.shape[1] // len(owners)
    outs = (k_out, v_out, q_out)
    for core in range(2):
        @pl.when(at.core == core)
        def _():
            run([
                pltpu.make_async_copy(early.at[o, pl.ds(block * rows, rows), :], out.at[span(owner, rows), :], sem)
                for o, out in enumerate(outs)
                for block, owner in enumerate(owners)
            ] + store_chunks(at, held, outs, sem, core, True))


def store_late(late, q_in, k_in, v_in, q_out, k_out, v_out, sem):
    at = Place()
    for core in range(2):
        @pl.when(at.core == core)
        def _():
            run(store_chunks(at, late, (k_out, v_out, q_out), sem, core, False))


def in_vmem(*arrays):
    return tuple(pltpu.with_memory_space_constraint(array, pltpu.VMEM) for array in arrays)


def solution(mesh):
    group_size = mesh.shape["tp"]

    def local_step(x_rows, norm_gain, w_q, w_k, w_v):
        rows, width = x_rows.shape
        head = w_q.shape[2]
        chunks = rows // CHUNK
        dma = pltpu.SemaphoreType.DMA
        any_space = pl.BlockSpec(memory_space=pl.ANY)
        vmem = pl.BlockSpec(memory_space=pltpu.VMEM)
        hbm = pl.BlockSpec(memory_space=pltpu.HBM)

        def small(**settings):
            return pltpu.CompilerParams(vmem_limit_bytes=1024 * 1024, **settings)

        early = pltpu.VMEM((3, 6 * rows, head), jnp.bfloat16)
        late = pltpu.VMEM((3, 2 * rows, head), jnp.bfloat16)
        final = [pltpu.HBM((group_size * rows, head), jnp.bfloat16)] * 3
        side_chunks = rows // SIDE_CHUNK

        gathered, held, far_late = in_vmem(*pl.pallas_call(
            gather,
            out_shape=[early, late, pltpu.VMEM((4, rows, head), jnp.bfloat16)],
            in_specs=[any_space] * 5,
            out_specs=[vmem] * 3,
            scratch_shapes=[
                pltpu.VMEM((rows, width), jnp.bfloat16),
                pltpu.VMEM((rows, width), jnp.bfloat16),
                pltpu.VMEM((width, 4 * head), jnp.bfloat16),
                pltpu.VMEM((width, 4 * head), jnp.bfloat16),
                pltpu.VMEM((4, rows, head), jnp.bfloat16),
                pltpu.VMEM((2 * rows, head), jnp.bfloat16),
                pltpu.VMEM((width,), jnp.float32),
                pltpu.VMEM((DETOUR, head), jnp.bfloat16),
                *[pltpu.SemaphoreType.REGULAR] * 3, *[dma(())] * 5, dma((chunks,)),
                *[dma((5,))] * 7,
                dma((side_chunks,)), dma((side_chunks,)), dma((2, chunks)), dma((2, chunks)), dma((2, side_chunks)), dma((2, side_chunks)),
                dma((3, chunks)), dma((3, chunks)), dma((2, chunks)), dma((2, chunks)), dma((chunks,)), dma((chunks,)), dma(()), dma(()),
            ],
            compiler_params=pltpu.CompilerParams(collective_id=0, has_side_effects=True, vmem_limit_bytes=40 * 1024 * 1024),
            name="gather",
        )(x_rows, norm_gain, w_q.reshape(width, head), w_k, w_v))
        *stored, token = pl.pallas_call(
            store_early,
            out_shape=final + [pltpu.HBM((8, 128), jnp.float32)],
            in_specs=[vmem] * 2,
            out_specs=[hbm] * 4,
            scratch_shapes=[dma(())],
            compiler_params=small(),
            name="store_early",
        )(gathered, held)
        finished = pl.pallas_call(
            finish,
            out_shape=late,
            in_specs=[vmem] * 2 + [hbm],
            out_specs=vmem,
            scratch_shapes=[pltpu.SemaphoreType.REGULAR] + [dma(())] * 4,
            compiler_params=small(collective_id=1, has_side_effects=True),
            name="finish",
        )(held, far_late, pltpu.with_memory_space_constraint(token, pltpu.HBM))
        outs = pl.pallas_call(
            store_late,
            out_shape=final,
            in_specs=[vmem] + [hbm] * 3,
            out_specs=[hbm] * 3,
            input_output_aliases={1: 0, 2: 1, 3: 2},
            scratch_shapes=[dma(())],
            compiler_params=small(),
            name="store_late",
        )(*in_vmem(finished), *stored)
        return tuple(out[:, None, :] for out in outs)

    return jax.shard_map(local_step, mesh=mesh, in_specs=(P(("dp", "tp"), None), P(None), P(None, "tp", None), P(None, "tp"), P(None, "tp")), out_specs=(P("dp", "tp", None), P("dp", "tp", None), P("dp", "tp", None)), check_vma=False)
```

```python
import functools

import jax
import jax.numpy as jnp
from jax import lax
from jax.experimental import pallas as pl
from jax.experimental.pallas import tpu as pltpu
from jax.sharding import PartitionSpec as P

EPSILON = 1e-6
CHUNK = 256
SIDE_CHUNK = 128
PIECE = 16
DETOUR = 48

K, V, Q = range(3)
KV, KVQ = pl.ds(0, 2), pl.ds(0, 3)
Q_SAME, Q_OTHER = 2, 3
OWN, SIDE, MATE, MATE_SIDE, FAR, FAR_MATE = range(6)
LATE_FAR, LATE_FAR_MATE = range(2)


class Place:
    def __init__(self):
        self.me = lax.axis_index("tp")
        self.core = lax.rem(self.me, 2)
        self.row = self.me // 4
        self.column = lax.rem(self.me // 2, 2)
        self.mate = self.me + 1 - 2 * self.core
        self.side = self.across(self.me)
        self.far = self.me + 2 - 4 * lax.rem(self.me // 2, 2)
        self.far_mate = self.far + 1 - 2 * self.core
        self.first = FIRST[0] + (FIRST[1] - FIRST[0]) * self.core
        self.first_other = FIRST[0] + FIRST[1] - self.first

    def across(self, device):
        return device + 4 - 8 * (device // 4)


def send(src, dst, send_sem, recv_sem, to):
    return pltpu.make_async_remote_copy(src_ref=src, dst_ref=dst, send_sem=send_sem, recv_sem=recv_sem, device_id={"tp": to})


def signal(sem, to):
    pl.semaphore_signal(sem, inc=1, device_id={"tp": to})


def loop(start, stop, body):
    def step(i, carry):
        body(i)
        return carry

    lax.fori_loop(start, stop, step, 0)


def span(i, size, base=0, count=1):
    return pl.ds(pl.multiple_of(base + i * size, size), count * size)


def by_core(at, body):
    for core in range(2):
        pl.when(at.core == core)(functools.partial(body, core))


SAME, OTHER = range(2)
FIRST = (1, 3)


def side_message(at, rows, stage, target, send_sem, recv_sem, kind, i, count=1):
    src, dst, block, peer = ((KVQ, KVQ, LATE_FAR, at.far), (Q_OTHER, Q, LATE_FAR_MATE, at.far_mate))[kind]
    return send(stage.at[src, span(i, CHUNK, 0, count), :], target.at[dst, span(i, CHUNK, block * rows, count), :], send_sem, recv_sem, peer)


def late_relay(at, rows, source, target, send_sem, recv_sem, i, count=1):
    return send(source.at[KV, span(i, CHUNK, LATE_FAR * rows, count), :], target.at[KV, span(i, CHUNK, LATE_FAR_MATE * rows, count), :],
                send_sem, recv_sem, at.mate)


def gather(x_hbm, gain_hbm, wq_hbm, wk_hbm, wv_hbm, early, late, far_late,
           x_own, x_side, w_own, w_far, far_own, mate_q, gain, detoured,
           mate_answer, side_answer, far_answer, aside_send, aside_recv, across_send, across_recv, load_gain, load_x, lw_sem, mw_send, mw_recv, fw_send, fw_recv, rw_send, rw_recv,
           x_send, x_recv, mo_send, mo_recv, ms_send, ms_recv, fo_send, fo_recv, fs_send, fs_recv, r_send, r_recv, lr_send, lr_recv):
    rows, width = x_hbm.shape
    head = wq_hbm.shape[1]
    part = wk_hbm.shape[1]
    chunks = rows // CHUNK
    side_chunks = rows // SIDE_CHUNK
    at = Place()
    core = at.core

    barrier = pltpu.get_barrier_semaphore()
    signal(barrier, at.far)

    @pl.when(core == 1)
    def _():
        signal(barrier, at.mate)

    @pl.when(at.row == 0)
    def _():
        signal(barrier, at.side)

    q_cols = pl.ds(pl.multiple_of(core * head, head), head)
    k_cols = pl.ds(pl.multiple_of(2 * head + core * part, part), part)
    v_cols = pl.ds(pl.multiple_of(3 * head + core * part, part), part)
    lead = width // 4
    mine = (
        (wk_hbm, pl.ds(0, lead), k_cols),
        (wk_hbm, pl.ds(lead, width - lead), k_cols),
        (wv_hbm, pl.ds(0, width), v_cols),
        (wq_hbm, pl.ds(0, width - DETOUR), q_cols),
        (wq_hbm, pl.ds(width - DETOUR, DETOUR), q_cols),
    )
    load_w, mate_w, far_w, relay_w = [], [], [], []
    for i, (src, depth, cols) in enumerate(mine):
        near_part, far_part = w_own.at[depth, cols], w_far.at[depth, cols]
        load_w.append(pltpu.make_async_copy(src.at[depth, :], near_part, lw_sem.at[i]))
        mate_w.append(send(near_part, near_part, mw_send.at[i], mw_recv.at[i], at.mate))
        far_w.append(send(near_part, far_part, fw_send.at[i], fw_recv.at[i], at.far))
        relay_w.append(send(far_part, far_part, rw_send.at[i], rw_recv.at[i], at.mate))

    def load_chunk(i):
        return pltpu.make_async_copy(x_hbm.at[span(i, CHUNK), :], x_own.at[span(i, CHUNK), :], load_x.at[i])

    def side_chunk(i):
        return send(x_hbm.at[span(i, SIDE_CHUNK), :], x_side.at[span(i, SIDE_CHUNK), :], x_send.at[i], x_recv.at[i], at.side)

    for copy in load_w:
        copy.start()

    last = w_own.at[mine[4][1], q_cols]
    aside = send(last, detoured, aside_send, aside_recv, at.side)
    across = send(detoured, w_far.at[mine[4][1], q_cols], across_send, across_recv, at.across(at.far))

    pl.semaphore_wait(barrier, 2 - core + at.row)

    @pl.when(at.column == 1)
    def _():
        send(wk_hbm.at[mine[0][1], :], w_far.at[mine[0][1], k_cols], fw_send.at[0], fw_recv.at[0], at.far).start()

    @pl.when(at.column == 0)
    def _():
        load_w[0].wait()
        far_w[0].start()

    @pl.when(core == 0)
    def _():
        signal(mate_answer, at.mate)

    @pl.when(at.row == 1)
    def _():
        signal(side_answer, at.side)

    @pl.when(core == 1)
    def _():
        pl.semaphore_wait(mate_answer, 1)

    signal(far_answer, at.far)

    @pl.when(at.row == 0)
    def _():
        pl.semaphore_wait(side_answer, 1)

    @pl.when(at.column == 1)
    def _():
        load_w[0].wait()

    for load, copy in zip(load_w[1:3], far_w[1:3]):
        load.wait()
        copy.start()
    for load in load_w[3:]:
        load.wait()

    @pl.when(at.row == 0)
    def _():
        far_w[3].start()
        aside.start()

    for copy in mate_w:
        copy.start()

    gain_copy = pltpu.make_async_copy(gain_hbm, gain, load_gain)
    gain_copy.start()
    for i in range(chunks):
        load_chunk(i).start()

    loop(0, side_chunks, lambda i: side_chunk(i).start())

    @pl.when(at.row == 1)
    def _():
        aside.wait_recv()
        across.start()
        for copy in far_w[3:]:
            copy.start()

    def normalise(ref, i, size):
        def piece(p, carry):
            here = pl.ds(pl.multiple_of(i * size + p * PIECE, PIECE), PIECE)
            x_wide = ref[here, :].astype(jnp.float32)
            mean_sq = jnp.mean(x_wide * x_wide, axis=-1, keepdims=True)
            ref[here, :] = (x_wide * lax.rsqrt(mean_sq + EPSILON) * gain[...].reshape(1, width)).astype(jnp.bfloat16)
            return carry

        lax.fori_loop(0, size // PIECE, piece, 0, unroll=4)

    def product(ref, here, w, block):
        cols = slice(block * head, (block + 1) * head) if isinstance(block, int) else pl.ds(pl.multiple_of(block * head, head), head)
        return jnp.dot(ref[here, :], w[:, cols], preferred_element_type=jnp.float32).astype(jnp.bfloat16)

    def mate_copies(block, i):
        size, sends, recvs = (SIDE_CHUNK, ms_send, ms_recv) if block == SIDE else (CHUNK, mo_send, mo_recv)
        here, there = span(i, size, block * rows), span(i, size, (MATE + block) * rows)
        return (
            send(early.at[KV, here, :], early.at[KV, there, :], sends.at[0, i], recvs.at[0, i], at.mate),
            send(mate_q.at[here, :], early.at[Q, there, :], sends.at[1, i], recvs.at[1, i], at.mate),
        )

    def near_products(ref, block, i):
        size = SIDE_CHUNK if block == SIDE else CHUNK
        here, source = span(i, size, block * rows), span(i, size)
        early[K, here, :] = product(ref, source, w_own, 2)
        early[V, here, :] = product(ref, source, w_own, 3)
        early[Q, here, :] = product(ref, source, w_own, core)
        mate_q[here, :] = product(ref, source, w_own, 1 - core)
        for copy in mate_copies(block, i):
            copy.start()

    far_columns = {K: 2, V: 3, Q_SAME: core, Q_OTHER: 1 - core}

    def far_products(ref, here, stage, kinds):
        for kind in kinds:
            stage[kind, here, :] = product(ref, here, w_far, far_columns[kind])

    def own_message(j, i):
        src, dst, block, peer = ((KV, KV, FAR, at.far), (Q_SAME, Q, FAR, at.far), (Q_OTHER, Q, FAR_MATE, at.far_mate))[j]
        return send(far_own.at[src, span(i, CHUNK), :], early.at[dst, span(i, CHUNK, block * rows), :], fo_send.at[j, i], fo_recv.at[j, i], peer)

    def message(kind, i, count=1):
        return side_message(at, rows, far_late, late, fs_send.at[kind, i], fs_recv.at[kind, i], kind, i, count)

    def relay(i):
        return send(early.at[KV, span(i, CHUNK, FAR * rows), :], early.at[KV, span(i, CHUNK, FAR_MATE * rows), :], r_send.at[i], r_recv.at[i], at.mate)

    def own_norm(i):
        load_chunk(i).wait()
        normalise(x_own, i, CHUNK)

    for copy in mate_w:
        copy.wait_recv()
    gain_copy.wait()
    loop(0, chunks, own_norm)
    loop(0, chunks, lambda i: near_products(x_own, OWN, i))

    for arrived, onward in zip(far_w[:3], relay_w[:3]):
        arrived.wait_recv()
        onward.start()
    for copy in relay_w[:3]:
        copy.wait_recv()

    def far_kv_step(i):
        far_products(x_own, span(i, CHUNK), far_own, (K, V))
        own_message(0, i).start()

    loop(0, chunks, far_kv_step)
    far_w[3].wait_recv()
    relay_w[3].start()

    @pl.when(at.row == 0)
    def _():
        across.wait_recv()

    @pl.when(at.row == 1)
    def _():
        far_w[4].wait_recv()

    relay_w[4].start()
    for copy in relay_w[3:]:
        copy.wait_recv()
    pl.semaphore_wait(far_answer, 1)

    def far_q_step(i):
        far_products(x_own, span(i, CHUNK), far_own, (Q_SAME, Q_OTHER))
        own_message(1, i).start()
        own_message(2, i).start()

    loop(0, chunks, far_q_step)

    def side_step(i):
        side_chunk(i).wait_recv()
        normalise(x_side, i, SIDE_CHUNK)
        near_products(x_side, SIDE, i)
        far_products(x_side, span(i, SIDE_CHUNK), far_late, (Q_OTHER, K, V, Q_SAME))
        done = lax.rem(i + 1, CHUNK // SIDE_CHUNK) == 0
        n = i // (CHUNK // SIDE_CHUNK)

        @pl.when(done & (n < at.first))
        def _():
            message(OTHER, n).start()

        @pl.when(done & (n == at.first - 1))
        def _():
            by_core(at, lambda c: message(SAME, 0, FIRST[c]).start())

    loop(0, side_chunks - 1, side_step)

    def relay_step(i):
        own_message(0, i).wait_recv()
        relay(i).start()

    loop(0, chunks, relay_step)

    def drain_own(i):
        for copy in mate_copies(OWN, i):
            copy.wait_send()
            copy.wait_recv()
        for j in range(3):
            own_message(j, i).wait_send()
        for j in (1, 2):
            own_message(j, i).wait_recv()
        relay(i).wait_send()
        relay(i).wait_recv()

    loop(0, chunks, drain_own)
    for copies in (mate_w, far_w[:4], relay_w):
        for copy in copies:
            copy.wait_send()

    @pl.when(at.row == 0)
    def _():
        aside.wait_send()

    @pl.when(at.row == 1)
    def _():
        across.wait_send()
        far_w[4].wait_send()

    side_step(side_chunks - 1)

    def drain_side(i):
        side_chunk(i).wait_send()
        for copy in mate_copies(SIDE, i):
            copy.wait_send()
            copy.wait_recv()

    loop(0, side_chunks, drain_side)
    loop(0, at.first_other, lambda i: message(OTHER, i).wait_recv())
    loop(0, at.first, lambda i: message(OTHER, i).wait_send())

    def close(c):
        same = message(SAME, 0, FIRST[c])
        same.wait_recv()
        onward = late_relay(at, rows, late, late, lr_send, lr_recv, 0, FIRST[0])
        if c == 0:
            onward.start()
            onward.wait_send()
        else:
            onward.wait_recv()
        same.wait_send()

    by_core(at, close)


def finish(held, far_late, token, late, answer, send_sem, same_recv, other_recv, relay_recv):
    rows = far_late.shape[1]
    chunks = rows // CHUNK
    at = Place()
    barrier = pltpu.get_barrier_semaphore()
    signal(barrier, at.far)

    @pl.when(at.core == 0)
    def _():
        signal(barrier, at.mate)
        signal(barrier, at.far_mate)

    pl.semaphore_wait(barrier, 1 + 2 * at.core)
    def message(kind, i, count):
        return side_message(at, rows, far_late, late, send_sem, (same_recv, other_recv)[kind], kind, i, count)

    def relay(source, i, count):
        return late_relay(at, rows, source, late, send_sem, relay_recv, i, count)

    def body(c):
        first, other_first = FIRST[c], FIRST[1 - c]
        same, other = (message(kind, first, chunks - first) for kind in (SAME, OTHER))
        same.start()
        if c:
            signal(answer, at.mate)
            signal(answer, at.far_mate)
        else:
            pl.semaphore_wait(answer, 2)
        other.start()
        if c:
            relay(held, 0, first).start()
        same.wait_recv()
        relay(late, first, chunks - first).start()
        arrived = chunks if c == 0 else chunks - other_first
        relay(late, 0, arrived).wait_recv()
        message(OTHER, other_first, chunks - other_first).wait_recv()
        sent = 4 * (chunks - first) + 2 * (chunks if c else chunks - first)
        everything = late.at[KVQ, span(0, CHUNK, 0, sent // 3), :]
        pltpu.make_async_copy(everything, everything, send_sem).wait()

    by_core(at, body)


def late_chunks(core, held):
    first, other, relayed = FIRST[core], FIRST[1 - core], core * FIRST[0]
    spans = [(o, LATE_FAR, first) for o in (K, V, Q)] + [(Q, LATE_FAR_MATE, other)] + [(o, LATE_FAR_MATE, relayed) for o in (K, V)]
    return [(o, block, 0, n) if held else (o, block, n, None) for o, block, n in spans]


def store_chunks(at, source, outs, sem, core, held):
    rows = source.shape[1] // 2
    owners = tuple(at.across(device) for device in (at.far, at.far_mate))
    copies = []
    for o, block, start, count in late_chunks(core, held):
        count = (rows // CHUNK - start if count is None else count) * CHUNK
        if count:
            copies.append(pltpu.make_async_copy(
                source.at[o, pl.ds(block * rows + start * CHUNK, count), :],
                outs[o].at[pl.ds(pl.multiple_of(owners[block] * rows + start * CHUNK, CHUNK), count), :],
                sem,
            ))
    return copies


def run(copies):
    for copy in copies:
        copy.start()
    for copy in copies:
        copy.wait()


def store_early(early, held, q_out, k_out, v_out, token, sem):
    at = Place()
    owners = (at.me, at.side, at.mate, at.across(at.mate), at.far, at.far_mate)
    rows = early.shape[1] // len(owners)
    outs = (k_out, v_out, q_out)
    for core in range(2):
        @pl.when(at.core == core)
        def _():
            run([
                pltpu.make_async_copy(early.at[o, pl.ds(block * rows, rows), :], out.at[span(owner, rows), :], sem)
                for o, out in enumerate(outs)
                for block, owner in enumerate(owners)
            ] + store_chunks(at, held, outs, sem, core, True))


def store_late(late, q_in, k_in, v_in, q_out, k_out, v_out, sem):
    at = Place()
    for core in range(2):
        @pl.when(at.core == core)
        def _():
            run(store_chunks(at, late, (k_out, v_out, q_out), sem, core, False))


def in_vmem(*arrays):
    return tuple(pltpu.with_memory_space_constraint(array, pltpu.VMEM) for array in arrays)


def solution(mesh):
    group_size = mesh.shape["tp"]

    def local_step(x_rows, norm_gain, w_q, w_k, w_v):
        rows, width = x_rows.shape
        head = w_q.shape[2]
        chunks = rows // CHUNK
        dma = pltpu.SemaphoreType.DMA
        any_space = pl.BlockSpec(memory_space=pl.ANY)
        vmem = pl.BlockSpec(memory_space=pltpu.VMEM)
        hbm = pl.BlockSpec(memory_space=pltpu.HBM)

        def small(**settings):
            return pltpu.CompilerParams(vmem_limit_bytes=1024 * 1024, **settings)

        early = pltpu.VMEM((3, 6 * rows, head), jnp.bfloat16)
        late = pltpu.VMEM((3, 2 * rows, head), jnp.bfloat16)
        final = [pltpu.HBM((group_size * rows, head), jnp.bfloat16)] * 3
        side_chunks = rows // SIDE_CHUNK

        gathered, held, far_late = in_vmem(*pl.pallas_call(
            gather,
            out_shape=[early, late, pltpu.VMEM((4, rows, head), jnp.bfloat16)],
            in_specs=[any_space] * 5,
            out_specs=[vmem] * 3,
            scratch_shapes=[
                pltpu.VMEM((rows, width), jnp.bfloat16),
                pltpu.VMEM((rows, width), jnp.bfloat16),
                pltpu.VMEM((width, 4 * head), jnp.bfloat16),
                pltpu.VMEM((width, 4 * head), jnp.bfloat16),
                pltpu.VMEM((4, rows, head), jnp.bfloat16),
                pltpu.VMEM((2 * rows, head), jnp.bfloat16),
                pltpu.VMEM((width,), jnp.float32),
                pltpu.VMEM((DETOUR, head), jnp.bfloat16),
                *[pltpu.SemaphoreType.REGULAR] * 3, *[dma(())] * 5, dma((chunks,)),
                *[dma((5,))] * 7,
                dma((side_chunks,)), dma((side_chunks,)), dma((2, chunks)), dma((2, chunks)), dma((2, side_chunks)), dma((2, side_chunks)),
                dma((3, chunks)), dma((3, chunks)), dma((2, chunks)), dma((2, chunks)), dma((chunks,)), dma((chunks,)), dma(()), dma(()),
            ],
            compiler_params=pltpu.CompilerParams(collective_id=0, has_side_effects=True, vmem_limit_bytes=40 * 1024 * 1024),
            name="gather",
        )(x_rows, norm_gain, w_q.reshape(width, head), w_k, w_v))
        *stored, token = pl.pallas_call(
            store_early,
            out_shape=final + [pltpu.HBM((8, 128), jnp.float32)],
            in_specs=[vmem] * 2,
            out_specs=[hbm] * 4,
            scratch_shapes=[dma(())],
            compiler_params=small(),
            name="store_early",
        )(gathered, held)
        finished = pl.pallas_call(
            finish,
            out_shape=late,
            in_specs=[vmem] * 2 + [hbm],
            out_specs=vmem,
            scratch_shapes=[pltpu.SemaphoreType.REGULAR] + [dma(())] * 4,
            compiler_params=small(collective_id=1, has_side_effects=True),
            name="finish",
        )(held, far_late, pltpu.with_memory_space_constraint(token, pltpu.HBM))
        outs = pl.pallas_call(
            store_late,
            out_shape=final,
            in_specs=[vmem] + [hbm] * 3,
            out_specs=[hbm] * 3,
            input_output_aliases={1: 0, 2: 1, 3: 2},
            scratch_shapes=[dma(())],
            compiler_params=small(),
            name="store_late",
        )(*in_vmem(finished), *stored)
        return tuple(out[:, None, :] for out in outs)

    return jax.shard_map(local_step, mesh=mesh, in_specs=(P(("dp", "tp"), None), P(None), P(None, "tp", None), P(None, "tp"), P(None, "tp")), out_specs=(P("dp", "tp", None), P("dp", "tp", None), P("dp", "tp", None)), check_vma=False)
```

```python
import functools

import jax
import jax.numpy as jnp
from jax import lax
from jax.experimental import pallas as pl
from jax.experimental.pallas import tpu as pltpu
from jax.sharding import PartitionSpec as P

EPSILON = 1e-6
CHUNK = 256
SIDE_CHUNK = 128
PIECE = 16
DETOUR = 64

K, V, Q = range(3)
KV, KVQ = pl.ds(0, 2), pl.ds(0, 3)
Q_SAME, Q_OTHER = 2, 3
OWN, SIDE, MATE, MATE_SIDE, FAR, FAR_MATE = range(6)
LATE_FAR, LATE_FAR_MATE = range(2)


class Place:
    def __init__(self):
        self.me = lax.axis_index("tp")
        self.core = lax.rem(self.me, 2)
        self.row = self.me // 4
        self.column = lax.rem(self.me // 2, 2)
        self.mate = self.me + 1 - 2 * self.core
        self.side = self.across(self.me)
        self.far = self.me + 2 - 4 * lax.rem(self.me // 2, 2)
        self.far_mate = self.far + 1 - 2 * self.core
        self.turn = 1 - self.core
        self.first = FIRST[0] + (FIRST[1] - FIRST[0]) * self.turn
        self.first_other = FIRST[0] + FIRST[1] - self.first

    def across(self, device):
        return device + 4 - 8 * (device // 4)


def send(src, dst, send_sem, recv_sem, to):
    return pltpu.make_async_remote_copy(src_ref=src, dst_ref=dst, send_sem=send_sem, recv_sem=recv_sem, device_id={"tp": to})


def signal(sem, to):
    pl.semaphore_signal(sem, inc=1, device_id={"tp": to})


def loop(start, stop, body):
    def step(i, carry):
        body(i)
        return carry

    lax.fori_loop(start, stop, step, 0)


def span(i, size, base=0, count=1):
    return pl.ds(pl.multiple_of(base + i * size, size), count * size)


def by_turn(at, body):
    for turn in range(2):
        pl.when(at.turn == turn)(functools.partial(body, turn))


SAME, OTHER = range(2)
FIRST = (1, 3)


def side_message(at, rows, stage, target, send_sem, recv_sem, kind, i, count=1):
    src, dst, block, peer = ((KVQ, KVQ, LATE_FAR, at.far), (Q_OTHER, Q, LATE_FAR_MATE, at.far_mate))[kind]
    return send(stage.at[src, span(i, CHUNK, 0, count), :], target.at[dst, span(i, CHUNK, block * rows, count), :], send_sem, recv_sem, peer)


def late_relay(at, rows, source, target, send_sem, recv_sem, i, count=1):
    return send(source.at[KV, span(i, CHUNK, LATE_FAR * rows, count), :], target.at[KV, span(i, CHUNK, LATE_FAR_MATE * rows, count), :],
                send_sem, recv_sem, at.mate)


def gather(x_hbm, gain_hbm, wq_hbm, wk_hbm, wv_hbm, early, late, far_late,
           x_own, x_side, w_own, w_far, far_own, mate_q, gain, detoured,
           mate_answer, side_answer, far_answer, aside_send, aside_recv, across_send, across_recv, load_gain, load_x, lw_sem, mw_send, mw_recv, fw_send, fw_recv, rw_send, rw_recv,
           x_send, x_recv, mo_send, mo_recv, ms_send, ms_recv, fo_send, fo_recv, fs_send, fs_recv, r_send, r_recv, lr_send, lr_recv):
    rows, width = x_hbm.shape
    head = wq_hbm.shape[1]
    part = wk_hbm.shape[1]
    chunks = rows // CHUNK
    side_chunks = rows // SIDE_CHUNK
    at = Place()
    core = at.core

    barrier = pltpu.get_barrier_semaphore()
    signal(barrier, at.far)

    @pl.when(core == 1)
    def _():
        signal(barrier, at.mate)

    @pl.when(at.row == 0)
    def _():
        signal(barrier, at.side)

    q_cols = pl.ds(pl.multiple_of(core * head, head), head)
    k_cols = pl.ds(pl.multiple_of(2 * head + core * part, part), part)
    v_cols = pl.ds(pl.multiple_of(3 * head + core * part, part), part)
    lead = width // 4
    mine = (
        (wk_hbm, pl.ds(0, lead), k_cols),
        (wk_hbm, pl.ds(lead, width - lead), k_cols),
        (wv_hbm, pl.ds(0, width), v_cols),
        (wq_hbm, pl.ds(0, width - DETOUR), q_cols),
        (wq_hbm, pl.ds(width - DETOUR, DETOUR), q_cols),
    )
    load_w, mate_w, far_w, relay_w = [], [], [], []
    for i, (src, depth, cols) in enumerate(mine):
        near_part, far_part = w_own.at[depth, cols], w_far.at[depth, cols]
        load_w.append(pltpu.make_async_copy(src.at[depth, :], near_part, lw_sem.at[i]))
        mate_w.append(send(near_part, near_part, mw_send.at[i], mw_recv.at[i], at.mate))
        far_w.append(send(near_part, far_part, fw_send.at[i], fw_recv.at[i], at.far))
        relay_w.append(send(far_part, far_part, rw_send.at[i], rw_recv.at[i], at.mate))

    def load_chunk(i):
        return pltpu.make_async_copy(x_hbm.at[span(i, CHUNK), :], x_own.at[span(i, CHUNK), :], load_x.at[i])

    def side_chunk(i):
        return send(x_hbm.at[span(i, SIDE_CHUNK), :], x_side.at[span(i, SIDE_CHUNK), :], x_send.at[i], x_recv.at[i], at.side)

    for copy in load_w:
        copy.start()

    last = w_own.at[mine[4][1], q_cols]
    aside = send(last, detoured, aside_send, aside_recv, at.side)
    across = send(detoured, w_far.at[mine[4][1], q_cols], across_send, across_recv, at.across(at.far))

    pl.semaphore_wait(barrier, 2 - core + at.row)

    @pl.when(at.column == 1)
    def _():
        send(wk_hbm.at[mine[0][1], :], w_far.at[mine[0][1], k_cols], fw_send.at[0], fw_recv.at[0], at.far).start()

    @pl.when(at.column == 0)
    def _():
        load_w[0].wait()
        far_w[0].start()

    @pl.when(core == 0)
    def _():
        signal(mate_answer, at.mate)

    @pl.when(at.row == 1)
    def _():
        signal(side_answer, at.side)

    @pl.when(core == 1)
    def _():
        pl.semaphore_wait(mate_answer, 1)

    signal(far_answer, at.far)

    @pl.when(at.row == 0)
    def _():
        pl.semaphore_wait(side_answer, 1)

    @pl.when(at.column == 1)
    def _():
        load_w[0].wait()

    for load, copy in zip(load_w[1:3], far_w[1:3]):
        load.wait()
        copy.start()
    for load in load_w[3:]:
        load.wait()

    @pl.when(at.row == 0)
    def _():
        far_w[3].start()
        aside.start()

    for copy in mate_w:
        copy.start()

    gain_copy = pltpu.make_async_copy(gain_hbm, gain, load_gain)
    gain_copy.start()
    for i in range(chunks):
        load_chunk(i).start()

    loop(0, side_chunks, lambda i: side_chunk(i).start())

    @pl.when(at.row == 1)
    def _():
        aside.wait_recv()
        across.start()
        for copy in far_w[3:]:
            copy.start()

    def normalise(ref, i, size):
        def piece(p, carry):
            here = pl.ds(pl.multiple_of(i * size + p * PIECE, PIECE), PIECE)
            x_wide = ref[here, :].astype(jnp.float32)
            mean_sq = jnp.mean(x_wide * x_wide, axis=-1, keepdims=True)
            ref[here, :] = (x_wide * lax.rsqrt(mean_sq + EPSILON) * gain[...].reshape(1, width)).astype(jnp.bfloat16)
            return carry

        lax.fori_loop(0, size // PIECE, piece, 0, unroll=4)

    def product(ref, here, w, block):
        cols = slice(block * head, (block + 1) * head) if isinstance(block, int) else pl.ds(pl.multiple_of(block * head, head), head)
        return jnp.dot(ref[here, :], w[:, cols], preferred_element_type=jnp.float32).astype(jnp.bfloat16)

    def mate_copies(block, i):
        size, sends, recvs = (SIDE_CHUNK, ms_send, ms_recv) if block == SIDE else (CHUNK, mo_send, mo_recv)
        here, there = span(i, size, block * rows), span(i, size, (MATE + block) * rows)
        return (
            send(early.at[KV, here, :], early.at[KV, there, :], sends.at[0, i], recvs.at[0, i], at.mate),
            send(mate_q.at[here, :], early.at[Q, there, :], sends.at[1, i], recvs.at[1, i], at.mate),
        )

    def near_products(ref, block, i):
        size = SIDE_CHUNK if block == SIDE else CHUNK
        here, source = span(i, size, block * rows), span(i, size)
        early[K, here, :] = product(ref, source, w_own, 2)
        early[V, here, :] = product(ref, source, w_own, 3)
        early[Q, here, :] = product(ref, source, w_own, core)
        mate_q[here, :] = product(ref, source, w_own, 1 - core)
        for copy in mate_copies(block, i):
            copy.start()

    far_columns = {K: 2, V: 3, Q_SAME: core, Q_OTHER: 1 - core}

    def far_products(ref, here, stage, kinds):
        for kind in kinds:
            stage[kind, here, :] = product(ref, here, w_far, far_columns[kind])

    def own_message(j, i):
        src, dst, block, peer = ((KV, KV, FAR, at.far), (Q_SAME, Q, FAR, at.far), (Q_OTHER, Q, FAR_MATE, at.far_mate))[j]
        return send(far_own.at[src, span(i, CHUNK), :], early.at[dst, span(i, CHUNK, block * rows), :], fo_send.at[j, i], fo_recv.at[j, i], peer)

    def message(kind, i, count=1):
        return side_message(at, rows, far_late, late, fs_send.at[kind, i], fs_recv.at[kind, i], kind, i, count)

    def relay(i):
        return send(early.at[KV, span(i, CHUNK, FAR * rows), :], early.at[KV, span(i, CHUNK, FAR_MATE * rows), :], r_send.at[i], r_recv.at[i], at.mate)

    def own_norm(i):
        load_chunk(i).wait()
        normalise(x_own, i, CHUNK)

    for copy in mate_w:
        copy.wait_recv()
    gain_copy.wait()
    loop(0, chunks, own_norm)
    loop(0, chunks, lambda i: near_products(x_own, OWN, i))

    for arrived, onward in zip(far_w[:3], relay_w[:3]):
        arrived.wait_recv()
        onward.start()
    for copy in relay_w[:3]:
        copy.wait_recv()

    def far_kv_step(i):
        far_products(x_own, span(i, CHUNK), far_own, (K, V))
        own_message(0, i).start()

    loop(0, chunks, far_kv_step)
    far_w[3].wait_recv()
    relay_w[3].start()

    @pl.when(at.row == 0)
    def _():
        across.wait_recv()

    @pl.when(at.row == 1)
    def _():
        far_w[4].wait_recv()

    relay_w[4].start()
    for copy in relay_w[3:]:
        copy.wait_recv()
    pl.semaphore_wait(far_answer, 1)

    def far_q_step(i):
        far_products(x_own, span(i, CHUNK), far_own, (Q_SAME, Q_OTHER))
        own_message(1, i).start()
        own_message(2, i).start()

    loop(0, chunks, far_q_step)

    def side_step(i):
        side_chunk(i).wait_recv()
        normalise(x_side, i, SIDE_CHUNK)
        near_products(x_side, SIDE, i)
        far_products(x_side, span(i, SIDE_CHUNK), far_late, (Q_OTHER, K, V, Q_SAME))
        done = lax.rem(i + 1, CHUNK // SIDE_CHUNK) == 0
        n = i // (CHUNK // SIDE_CHUNK)

        @pl.when(done & (n < at.first))
        def _():
            message(OTHER, n).start()

        @pl.when(done & (n == at.first - 1))
        def _():
            by_turn(at, lambda c: message(SAME, 0, FIRST[c]).start())

    loop(0, side_chunks - 1, side_step)

    def relay_step(i):
        own_message(0, i).wait_recv()
        relay(i).start()

    loop(0, chunks, relay_step)

    def drain_own(i):
        for copy in mate_copies(OWN, i):
            copy.wait_send()
            copy.wait_recv()
        for j in range(3):
            own_message(j, i).wait_send()
        for j in (1, 2):
            own_message(j, i).wait_recv()
        relay(i).wait_send()
        relay(i).wait_recv()

    loop(0, chunks, drain_own)
    for copies in (mate_w, far_w[:4], relay_w):
        for copy in copies:
            copy.wait_send()

    @pl.when(at.row == 0)
    def _():
        aside.wait_send()

    @pl.when(at.row == 1)
    def _():
        across.wait_send()
        far_w[4].wait_send()

    side_step(side_chunks - 1)

    def drain_side(i):
        side_chunk(i).wait_send()
        for copy in mate_copies(SIDE, i):
            copy.wait_send()
            copy.wait_recv()

    loop(0, side_chunks, drain_side)
    loop(0, at.first_other, lambda i: message(OTHER, i).wait_recv())
    loop(0, at.first, lambda i: message(OTHER, i).wait_send())

    def close(c):
        same = message(SAME, 0, FIRST[c])
        same.wait_recv()
        onward = late_relay(at, rows, late, late, lr_send, lr_recv, 0, FIRST[0])
        if c == 0:
            onward.start()
            onward.wait_send()
        else:
            onward.wait_recv()
        same.wait_send()

    by_turn(at, close)


def finish(held, far_late, token, late, answer, send_sem, same_recv, other_recv, relay_recv):
    rows = far_late.shape[1]
    chunks = rows // CHUNK
    at = Place()
    barrier = pltpu.get_barrier_semaphore()
    signal(barrier, at.far)

    @pl.when(at.turn == 0)
    def _():
        signal(barrier, at.mate)
        signal(barrier, at.far_mate)

    pl.semaphore_wait(barrier, 1 + 2 * at.turn)
    def message(kind, i, count):
        return side_message(at, rows, far_late, late, send_sem, (same_recv, other_recv)[kind], kind, i, count)

    def relay(source, i, count):
        return late_relay(at, rows, source, late, send_sem, relay_recv, i, count)

    def body(c):
        first, other_first = FIRST[c], FIRST[1 - c]
        same, other = (message(kind, first, chunks - first) for kind in (SAME, OTHER))
        same.start()
        if c:
            signal(answer, at.mate)
            signal(answer, at.far_mate)
        else:
            pl.semaphore_wait(answer, 2)
        other.start()
        if c:
            relay(held, 0, first).start()
        same.wait_recv()
        relay(late, first, chunks - first).start()
        arrived = chunks if c == 0 else chunks - other_first
        relay(late, 0, arrived).wait_recv()
        message(OTHER, other_first, chunks - other_first).wait_recv()
        sent = 4 * (chunks - first) + 2 * (chunks if c else chunks - first)
        everything = late.at[KVQ, span(0, CHUNK, 0, sent // 3), :]
        pltpu.make_async_copy(everything, everything, send_sem).wait()

    by_turn(at, body)


def late_chunks(core, held):
    first, other, relayed = FIRST[core], FIRST[1 - core], core * FIRST[0]
    spans = [(o, LATE_FAR, first) for o in (K, V, Q)] + [(Q, LATE_FAR_MATE, other)] + [(o, LATE_FAR_MATE, relayed) for o in (K, V)]
    return [(o, block, 0, n) if held else (o, block, n, None) for o, block, n in spans]


def store_chunks(at, source, outs, sem, core, held):
    rows = source.shape[1] // 2
    owners = tuple(at.across(device) for device in (at.far, at.far_mate))
    copies = []
    for o, block, start, count in late_chunks(core, held):
        count = (rows // CHUNK - start if count is None else count) * CHUNK
        if count:
            copies.append(pltpu.make_async_copy(
                source.at[o, pl.ds(block * rows + start * CHUNK, count), :],
                outs[o].at[pl.ds(pl.multiple_of(owners[block] * rows + start * CHUNK, CHUNK), count), :],
                sem,
            ))
    return copies


def run(copies):
    for copy in copies:
        copy.start()
    for copy in copies:
        copy.wait()


def store_early(early, held, q_out, k_out, v_out, token, sem):
    at = Place()
    owners = (at.me, at.side, at.mate, at.across(at.mate), at.far, at.far_mate)
    rows = early.shape[1] // len(owners)
    outs = (k_out, v_out, q_out)
    for core in range(2):
        @pl.when(at.turn == core)
        def _():
            run([
                pltpu.make_async_copy(early.at[o, pl.ds(block * rows, rows), :], out.at[span(owner, rows), :], sem)
                for o, out in enumerate(outs)
                for block, owner in enumerate(owners)
            ] + store_chunks(at, held, outs, sem, core, True))


def store_late(late, q_in, k_in, v_in, q_out, k_out, v_out, sem):
    at = Place()
    for core in range(2):
        @pl.when(at.turn == core)
        def _():
            run(store_chunks(at, late, (k_out, v_out, q_out), sem, core, False))


def in_vmem(*arrays):
    return tuple(pltpu.with_memory_space_constraint(array, pltpu.VMEM) for array in arrays)


def solution(mesh):
    group_size = mesh.shape["tp"]

    def local_step(x_rows, norm_gain, w_q, w_k, w_v):
        rows, width = x_rows.shape
        head = w_q.shape[2]
        chunks = rows // CHUNK
        dma = pltpu.SemaphoreType.DMA
        any_space = pl.BlockSpec(memory_space=pl.ANY)
        vmem = pl.BlockSpec(memory_space=pltpu.VMEM)
        hbm = pl.BlockSpec(memory_space=pltpu.HBM)

        def small(**settings):
            return pltpu.CompilerParams(vmem_limit_bytes=1024 * 1024, **settings)

        early = pltpu.VMEM((3, 6 * rows, head), jnp.bfloat16)
        late = pltpu.VMEM((3, 2 * rows, head), jnp.bfloat16)
        final = [pltpu.HBM((group_size * rows, head), jnp.bfloat16)] * 3
        side_chunks = rows // SIDE_CHUNK

        gathered, held, far_late = in_vmem(*pl.pallas_call(
            gather,
            out_shape=[early, late, pltpu.VMEM((4, rows, head), jnp.bfloat16)],
            in_specs=[any_space] * 5,
            out_specs=[vmem] * 3,
            scratch_shapes=[
                pltpu.VMEM((rows, width), jnp.bfloat16),
                pltpu.VMEM((rows, width), jnp.bfloat16),
                pltpu.VMEM((width, 4 * head), jnp.bfloat16),
                pltpu.VMEM((width, 4 * head), jnp.bfloat16),
                pltpu.VMEM((4, rows, head), jnp.bfloat16),
                pltpu.VMEM((2 * rows, head), jnp.bfloat16),
                pltpu.VMEM((width,), jnp.float32),
                pltpu.VMEM((DETOUR, head), jnp.bfloat16),
                *[pltpu.SemaphoreType.REGULAR] * 3, *[dma(())] * 5, dma((chunks,)),
                *[dma((5,))] * 7,
                dma((side_chunks,)), dma((side_chunks,)), dma((2, chunks)), dma((2, chunks)), dma((2, side_chunks)), dma((2, side_chunks)),
                dma((3, chunks)), dma((3, chunks)), dma((2, chunks)), dma((2, chunks)), dma((chunks,)), dma((chunks,)), dma(()), dma(()),
            ],
            compiler_params=pltpu.CompilerParams(collective_id=0, has_side_effects=True, vmem_limit_bytes=40 * 1024 * 1024),
            name="gather",
        )(x_rows, norm_gain, w_q.reshape(width, head), w_k, w_v))
        *stored, token = pl.pallas_call(
            store_early,
            out_shape=final + [pltpu.HBM((8, 128), jnp.float32)],
            in_specs=[vmem] * 2,
            out_specs=[hbm] * 4,
            scratch_shapes=[dma(())],
            compiler_params=small(),
            name="store_early",
        )(gathered, held)
        finished = pl.pallas_call(
            finish,
            out_shape=late,
            in_specs=[vmem] * 2 + [hbm],
            out_specs=vmem,
            scratch_shapes=[pltpu.SemaphoreType.REGULAR] + [dma(())] * 4,
            compiler_params=small(collective_id=1, has_side_effects=True),
            name="finish",
        )(held, far_late, pltpu.with_memory_space_constraint(token, pltpu.HBM))
        outs = pl.pallas_call(
            store_late,
            out_shape=final,
            in_specs=[vmem] + [hbm] * 3,
            out_specs=[hbm] * 3,
            input_output_aliases={1: 0, 2: 1, 3: 2},
            scratch_shapes=[dma(())],
            compiler_params=small(),
            name="store_late",
        )(*in_vmem(finished), *stored)
        return tuple(out[:, None, :] for out in outs)

    return jax.shard_map(local_step, mesh=mesh, in_specs=(P(("dp", "tp"), None), P(None), P(None, "tp", None), P(None, "tp"), P(None, "tp")), out_specs=(P("dp", "tp", None), P("dp", "tp", None), P("dp", "tp", None)), check_vma=False)
```
